128 devices in a mesh: rep: 64 (over z, y, x), data: 2 (over core).
Axes of the slice: x: 4, y: 4, z: 4, core: 2. Of those that a mesh axis runs over, the one named last changes fastest.
Arguments:
- img_feat: bfloat16 [393216, 768], P(('rep', 'data'))
- txt_feat: bfloat16 [393216, 512], P(('rep', 'data'))
- w_img: bfloat16 [768, 512], replicated
- w_txt: bfloat16 [512, 512], replicated
- log_temp: float32 [], replicated
- logit_bias: float32 [], replicated
Outputs:
- output 1: float32 [], replicated
- output 2: float32 [], replicated
- output 3: float32 [], replicated
- output 4: float32 [768, 512], replicated
- output 5: float32 [512, 512], replicated
All inputs are finite; a program needn't handle non-finite values.
Results may differ from the reference program's by a relative error of at most 0.001.
Values are sent between devices in bfloat16 or wider.
A program may use at most 1 GiB of HBM per device.

```python
import math
import jax
import jax.numpy as jnp
from jax import lax

FI = 768
FT = 512
D = 512
BLOCK_ROWS = 3072
BLOCKS = 2
GROUPS = 64
LATENT = 16
GROUP_ROWS = BLOCK_ROWS * BLOCKS
TOTAL_ROWS = GROUP_ROWS * GROUPS


def draw_features(mean_key, shift_key, mix_key, noise_key, latent, width):
    feat_mean = jax.random.normal(mean_key, (width,), jnp.float32)
    block_shift = jnp.repeat(jax.random.normal(shift_key, (BLOCKS * GROUPS, width), jnp.float32), BLOCK_ROWS, axis=0)
    latent_mix = jax.random.normal(mix_key, (LATENT, width), jnp.float32) * LATENT ** -0.5
    noise_rows = jax.random.normal(noise_key, (TOTAL_ROWS, width), jnp.float32)
    features = feat_mean[None, :] + 0.6 * block_shift + 0.8 * jnp.dot(latent, latent_mix) + 0.5 * noise_rows
    return features.astype(jnp.bfloat16)


def setup_inputs(seed: int = 0) -> dict:
    root_key = jax.random.key(seed)
    sub_keys = jax.random.split(root_key, 13)
    latent = jax.random.normal(sub_keys[0], (TOTAL_ROWS, LATENT), jnp.float32)
    img_feat = draw_features(sub_keys[1], sub_keys[2], sub_keys[3], sub_keys[4], latent, FI)
    txt_feat = draw_features(sub_keys[5], sub_keys[6], sub_keys[7], sub_keys[8], latent, FT)
    w_img = (jax.random.normal(sub_keys[9], (FI, D), jnp.float32) * FI ** -0.5).astype(jnp.bfloat16)
    w_txt = (jax.random.normal(sub_keys[10], (FT, D), jnp.float32) * FT ** -0.5).astype(jnp.bfloat16)
    log_temp = (math.log(5.0) + 0.3 * jax.random.normal(sub_keys[11], (), jnp.float32)).astype(jnp.float32)
    logit_bias = (0.5 * jax.random.normal(sub_keys[12], (), jnp.float32) - math.log(GROUP_ROWS)).astype(jnp.float32)
    return {"img_feat": img_feat, "txt_feat": txt_feat, "w_img": w_img, "w_txt": w_txt, "log_temp": log_temp, "logit_bias": logit_bias}


def normalize_rows(raw_emb):
    inv_norm = lax.rsqrt(jnp.sum(raw_emb * raw_emb, axis=1, keepdims=True))
    return raw_emb * inv_norm, inv_norm


def backward_norm(grad_unit, unit_emb, inv_norm):
    proj = jnp.sum(unit_emb * grad_unit, axis=1, keepdims=True)
    return (inv_norm * (grad_unit - unit_emb * proj)).astype(jnp.bfloat16)


def group_terms(img_grp, txt_grp, temp_scale, logit_bias):
    img_blocks = img_grp.reshape(BLOCKS, BLOCK_ROWS, D)
    col_ids = jnp.arange(GROUP_ROWS)[None, :]

    def block_step(loop_state, block_in):
        txt_acc, scal_acc = loop_state
        img_blk, blk_idx = block_in
        row_ids = blk_idx * BLOCK_ROWS + jnp.arange(BLOCK_ROWS)[:, None]
        sign_mat = jnp.where(row_ids == col_ids, 1.0, -1.0)
        tile_dots = jnp.dot(img_blk, txt_grp.T, preferred_element_type=jnp.float32)
        logits = temp_scale * tile_dots + logit_bias
        margin = sign_mat * logits
        grad_z = -sign_mat * jax.nn.sigmoid(-margin) / TOTAL_ROWS
        scal_part = jnp.stack([jnp.sum(jax.nn.softplus(-margin)), temp_scale * jnp.sum(grad_z * tile_dots), jnp.sum(grad_z)])
        h_mat = (temp_scale * grad_z).astype(jnp.bfloat16)
        img_grad = jnp.dot(h_mat, txt_grp, preferred_element_type=jnp.float32)
        txt_acc = txt_acc + jnp.dot(h_mat.T, img_blk, preferred_element_type=jnp.float32)
        return (txt_acc, scal_acc + scal_part), img_grad

    init_state = (jnp.zeros((GROUP_ROWS, D), jnp.float32), jnp.zeros((3,), jnp.float32))
    final_state, img_grads = lax.scan(block_step, init_state, (img_blocks, jnp.arange(BLOCKS)))
    return img_grads.reshape(GROUP_ROWS, D), final_state[0], final_state[1]


def reference(img_feat, txt_feat, w_img, w_txt, log_temp, logit_bias):
    temp_scale = jnp.exp(log_temp)
    unit_img, inv_img = normalize_rows(jnp.dot(img_feat, w_img, preferred_element_type=jnp.float32))
    unit_txt, inv_txt = normalize_rows(jnp.dot(txt_feat, w_txt, preferred_element_type=jnp.float32))
    emb_img = unit_img.astype(jnp.bfloat16).reshape(GROUPS, GROUP_ROWS, D)
    emb_txt = unit_txt.astype(jnp.bfloat16).reshape(GROUPS, GROUP_ROWS, D)

    def per_group(group_embs):
        return group_terms(group_embs[0], group_embs[1], temp_scale, logit_bias)

    img_grad, txt_grad, scal_sums = lax.map(per_group, (emb_img, emb_txt))
    raw_img_grad = backward_norm(img_grad.reshape(TOTAL_ROWS, D), unit_img, inv_img)
    raw_txt_grad = backward_norm(txt_grad.reshape(TOTAL_ROWS, D), unit_txt, inv_txt)
    dw_img = jnp.dot(img_feat.T, raw_img_grad, preferred_element_type=jnp.float32)
    dw_txt = jnp.dot(txt_feat.T, raw_txt_grad, preferred_element_type=jnp.float32)
    scal_total = jnp.sum(scal_sums, axis=0)
    return scal_total[0] / TOTAL_ROWS, scal_total[1], scal_total[2], dw_img, dw_txt
```

```python
import functools

import jax
import jax.numpy as jnp
from jax import lax
from jax.experimental import pallas as pl
from jax.experimental.pallas import tpu as pltpu
from jax.sharding import PartitionSpec as P

LOG2E = 1.4426950408889634
LN2 = 0.6931471805599453
NT = (((1,), (1,)), ((), ()))
TN = (((0,), (0,)), ((), ()))
MESH = pl.DeviceIdType.MESH
F32 = jnp.float32
BF16 = jnp.bfloat16
MIB = 1024 * 1024

BM = 512
BN = 512
CR, CC = 16, 256
HALF = 2688
PART = HALF // 3
QUART = PART // 4
SIXT = QUART // 4


def inv_norm(raw):
    return lax.rsqrt(jnp.sum(raw * raw, axis=1, keepdims=True))


def params(vmem, **kw):
    return pltpu.CompilerParams(dimension_semantics=("arbitrary",), vmem_limit_bytes=vmem * MIB, **kw)


def cost(flops, nbytes):
    return pl.CostEstimate(flops=int(flops), bytes_accessed=int(nbytes), transcendentals=0)


def head_body(x_ref, w_ref, raw_ref, emb_ref, *maybe_t):
    raw = jnp.dot(x_ref[...], w_ref[...], preferred_element_type=F32)
    raw_ref[...] = raw
    emb = (raw * inv_norm(raw)).astype(BF16)
    emb_ref[...] = emb
    if maybe_t:
        maybe_t[0][...] = emb.T


def head(x, w, transposed, name):
    rows, feat = x.shape
    dim = w.shape[1]
    out_shape = [jax.ShapeDtypeStruct((rows, dim), F32), jax.ShapeDtypeStruct((rows, dim), BF16)]
    out_specs = [pl.BlockSpec((BM, dim), lambda i: (i, 0)), pl.BlockSpec((BM, dim), lambda i: (i, 0))]
    if transposed:
        out_shape.append(jax.ShapeDtypeStruct((dim, rows), BF16))
        out_specs.append(pl.BlockSpec((dim, BM), lambda i: (0, i)))
    return pl.pallas_call(
        head_body,
        grid=(rows // BM,),
        in_specs=[pl.BlockSpec((BM, feat), lambda i: (i, 0)), pl.BlockSpec((feat, dim), lambda i: (0, 0))],
        out_specs=out_specs,
        out_shape=out_shape,
        compiler_params=params(24),
        cost_estimate=cost(2 * rows * feat * dim, rows * (2 * feat + 8 * dim)),
        name=name,
    )(x, w)


def pair_terms(sc_ref, img_ref, imgt_ref, txt_ref, di_ref, dt_ref, acc, s_scr, h_scr, total_rows, home, di_init):
    step = pl.program_id(0)
    blocks = txt_ref.shape[0]
    s = sc_ref[0]
    a, b, hs = s * LOG2E, sc_ref[1] * LOG2E, s / total_rows
    img, imgt = img_ref[...], imgt_ref[...]

    def block_of(k):
        return lax.rem(step + k, blocks) if home else k

    def logits(k):
        s_scr[k % 2] = lax.dot_general(img, txt_ref[block_of(k)], NT, preferred_element_type=F32)

    def terms(k):
        zero = jnp.zeros((CR, CC), F32)
        top, prod, g_sum, gs_sum = zero, zero, zero, zero
        for r in range(0, BM, CR):
            for c in range(0, BN, CC):
                dots = s_scr[k % 2, r:r + CR, c:c + CC]
                z = dots * a + b
                pos = jnp.maximum(z, 0.0)
                t = jnp.exp2(-jnp.abs(z))
                rcp = 1.0 / (1.0 + t)
                sig = jnp.where(z >= 0, rcp, t * rcp)
                if home and k == 0 and r < c + CC and c < r + CR:
                    eye = (lax.broadcasted_iota(jnp.int32, (CR, CC), 0) + r) == (lax.broadcasted_iota(jnp.int32, (CR, CC), 1) + c)
                    sig = jnp.where(eye, -jnp.where(z >= 0, t * rcp, rcp), sig)
                    pos = jnp.where(eye, jnp.maximum(-z, 0.0), pos)
                top = top + pos
                prod = (prod + t) + prod * t
                g_sum = g_sum + sig
                gs_sum = gs_sum + sig * dots
                h_scr[k % 2, r:r + CR, c:c + CC] = (sig * hs).astype(BF16)
        acc[0] += LN2 * top + jnp.log1p(prod)
        acc[1] += gs_sum
        acc[2] += g_sum

    def grads(k):
        h = h_scr[k % 2]
        part = jnp.dot(h, txt_ref[block_of(k)], preferred_element_type=F32)
        if k == 0:
            di_ref[...] = part if di_init is None else di_init[...] + part
        else:
            di_ref[...] += part
        dt_ref[block_of(k)] += jnp.dot(imgt, h, preferred_element_type=F32)

    logits(0)
    for k in range(blocks):
        if k + 1 < blocks:
            logits(k + 1)
        terms(k)
        grads(k)


def away_body(sc_ref, img_ref, imgt_ref, txt_ref, di_ref, dt_ref, sums_ref, s_scr, h_scr, *, total_rows):
    @pl.when(pl.program_id(0) == 0)
    def _():
        sums_ref[...] = jnp.zeros_like(sums_ref)
        dt_ref[...] = jnp.zeros_like(dt_ref)

    pair_terms(sc_ref, img_ref, imgt_ref, txt_ref, di_ref, dt_ref, sums_ref, s_scr, h_scr, total_rows, False, None)


def home_body(sc_ref, img_ref, imgt_ref, txt_ref, raw_ref, x_ref, away_ref, sums_in, dt_ref, dw_ref, sums_ref, s_scr, h_scr, di_ref, *, total_rows):
    @pl.when(pl.program_id(0) == 0)
    def _():
        sums_ref[...] = sums_in[...]
        dt_ref[...] = jnp.zeros_like(dt_ref)
        dw_ref[...] = jnp.zeros_like(dw_ref)

    pair_terms(sc_ref, img_ref, imgt_ref, txt_ref, di_ref, dt_ref, sums_ref, s_scr, h_scr, total_rows, True, away_ref)
    dw_ref[...] += lax.dot_general(x_ref[...], raw_grad(raw_ref[...], di_ref[...]), TN, preferred_element_type=F32)


def raw_grad(raw, grad_unit):
    inv = inv_norm(raw)
    unit = raw * inv
    proj = jnp.sum(unit * grad_unit, axis=1, keepdims=True)
    return (inv * (grad_unit - unit * proj)).astype(BF16)


def tile_scratch():
    return [pltpu.VMEM((2, BM, BN), F32), pltpu.VMEM((2, BM, BN), BF16)]


def whole(shape, **kw):
    return pl.BlockSpec(shape, lambda i: (0,) * len(shape), **kw)


def away_tile(scal, img, imgt, txt, total_rows):
    rows, dim = img.shape
    blocks = txt.shape[0]
    once = dict(pipeline_mode=pl.Buffered(1))
    return pl.pallas_call(
        functools.partial(away_body, total_rows=total_rows),
        grid=(rows // BM,),
        in_specs=[
            pl.BlockSpec(memory_space=pltpu.SMEM),
            pl.BlockSpec((BM, dim), lambda i: (i, 0)),
            pl.BlockSpec((dim, BM), lambda i: (0, i)),
            whole((blocks, BN, dim), **once),
        ],
        out_specs=[pl.BlockSpec((BM, dim), lambda i: (i, 0)), whole((blocks, dim, BN), **once), whole((3, CR, CC))],
        out_shape=[
            jax.ShapeDtypeStruct((rows, dim), F32),
            jax.ShapeDtypeStruct((blocks, dim, BN), F32),
            jax.ShapeDtypeStruct((3, CR, CC), F32),
        ],
        scratch_shapes=tile_scratch(),
        compiler_params=params(40),
        cost_estimate=cost(6 * rows * rows * dim, 30 * rows * dim),
        name="away_tile",
    )(scal, img, imgt, txt)


def home_tile(scal, img, imgt, txt, raw, x, away, sums, total_rows):
    rows, dim = img.shape
    feat = x.shape[1]
    blocks = txt.shape[0]
    once = dict(pipeline_mode=pl.Buffered(1))
    return pl.pallas_call(
        functools.partial(home_body, total_rows=total_rows),
        grid=(rows // BM,),
        in_specs=[
            pl.BlockSpec(memory_space=pltpu.SMEM),
            pl.BlockSpec((BM, dim), lambda i: (i, 0)),
            pl.BlockSpec((dim, BM), lambda i: (0, i)),
            whole((blocks, BN, dim), **once),
            pl.BlockSpec((BM, dim), lambda i: (i, 0)),
            pl.BlockSpec((BM, feat), lambda i: (i, 0)),
            pl.BlockSpec((BM, dim), lambda i: (i, 0)),
            whole((3, CR, CC)),
        ],
        out_specs=[whole((blocks, dim, BN), **once), whole((feat, dim), **once), whole((3, CR, CC))],
        out_shape=[
            jax.ShapeDtypeStruct((blocks, dim, BN), F32),
            jax.ShapeDtypeStruct((feat, dim), F32),
            jax.ShapeDtypeStruct((3, CR, CC), F32),
        ],
        scratch_shapes=tile_scratch() + [pltpu.VMEM((BM, dim), F32)],
        compiler_params=params(48),
        cost_estimate=cost(6 * rows * rows * dim, 40 * rows * dim),
        name="home_tile",
    )(scal, img, imgt, txt, raw, x, away, sums)


def text_body(sc_ref, own_ref, got_ref, raw_ref, x_ref, dwi_ref, sums_ref, out_ref, dw_ref, *, total_rows):
    step = pl.program_id(0)

    @pl.when(step == 0)
    def _():
        dw_ref[...] = jnp.zeros_like(dw_ref)

    grad = (own_ref[0] + got_ref[0]).T
    dw_ref[...] += lax.dot_general(x_ref[...], raw_grad(raw_ref[...], grad), TN, preferred_element_type=F32)

    @pl.when(step == pl.num_programs(0) - 1)
    def _():
        feat_i, feat_t = dwi_ref.shape[0], dw_ref.shape[0]
        flat = []
        for l in range(4):
            flat.append((dwi_ref, l, feat_i))
        for l in range(4):
            flat.append((dw_ref, l, feat_t))
        pos = 0
        size = 2 * feat_i + 2 * feat_t
        for ref, l, n in flat:
            done = 0
            while done < n:
                half, at = divmod(pos, size)
                take = min(n - done, size - at)
                out_ref[half, at:at + take, :] = ref[done:done + take, 128 * l:128 * (l + 1)]
                done += take
                pos += take
        out_ref[:, size:, :] = jnp.zeros((2, HALF - size, 128), F32)
        s = sc_ref[0]
        row = lax.broadcasted_iota(jnp.int32, (8, 128), 0)
        loss = jnp.sum(sums_ref[0]) / total_rows
        temp = jnp.sum(sums_ref[1]) * (s / total_rows)
        bias = jnp.sum(sums_ref[2]) / total_rows
        out_ref[0, size:size + 8, :] = jnp.where(row == 0, loss, jnp.where(row == 1, temp, bias))


def text_back(scal, own, got, raw, x, dwi, sums, total_rows):
    rows, dim = raw.shape
    feat = x.shape[1]
    return pl.pallas_call(
        functools.partial(text_body, total_rows=total_rows),
        grid=(rows // BN,),
        in_specs=[
            pl.BlockSpec(memory_space=pltpu.SMEM),
            pl.BlockSpec((1, dim, BN), lambda i: (i, 0, 0)),
            pl.BlockSpec((1, dim, BN), lambda i: (i, 0, 0)),
            pl.BlockSpec((BN, dim), lambda i: (i, 0)),
            pl.BlockSpec((BN, feat), lambda i: (i, 0)),
            whole(dwi.shape),
            whole((3, CR, CC)),
        ],
        out_specs=whole((2, HALF, 128)),
        out_shape=jax.ShapeDtypeStruct((2, HALF, 128), F32),
        scratch_shapes=[pltpu.VMEM((feat, dim), F32)],
        compiler_params=params(32),
        cost_estimate=cost(2 * rows * feat * dim, rows * (2 * feat + 12 * dim)),
        name="text_back",
    )(scal, own, got, raw, x, dwi, sums)


def allsum_body(a_ref, o_ref, d2d, r1, r2, r3, dsem, s1, v1, s2, v2, s3, v3, s4, v4, s5, v5):
    rep, core = lax.axis_index("rep"), lax.axis_index("data")
    coord = [lax.rem(rep, 4), lax.rem(lax.div(rep, 4), 4), lax.div(rep, 16)]
    stride = [1, 4, 16]

    def peer(dim, off):
        return (rep + (lax.rem(coord[dim] + off, 4) - coord[dim]) * stride[dim], core)

    sib = (rep, 1 - core)
    bar = pltpu.get_barrier_semaphore()
    pl.semaphore_signal(bar, inc=1, device_id=sib, device_id_type=MESH)
    for dim in range(3):
        for off in (1, 2, 3):
            pl.semaphore_signal(bar, inc=1, device_id=peer(dim, off), device_id_type=MESH)
    pl.semaphore_wait(bar, 10)

    started = []

    def send(src, dst, ssem, rsem, dev):
        copy = pltpu.make_async_remote_copy(src_ref=src, dst_ref=dst, send_sem=ssem, recv_sem=rsem, device_id=dev, device_id_type=MESH)
        copy.start()
        started.append(copy)
        return copy

    out = o_ref.at[core]
    dims = [(p, (p + 1) % 3, (p + 2) % 3) for p in range(3)]
    offs = (2, 1, 3)

    c0 = []
    for p in range(3):
        rows = pl.ds(PART * p, PART)
        c0.append(send(a_ref.at[1 - core, rows], d2d.at[rows], dsem.at[0, p], dsem.at[1, p], sib))
    c1 = []
    for p in range(3):
        c0[p].wait_recv()
        rows = pl.ds(PART * p, PART)
        d2d[rows, :] = d2d[rows, :] + a_ref[core, rows, :]
        d = dims[p][0]
        c1.append([
            send(d2d.at[pl.ds(PART * p + lax.rem(coord[d] + o, 4) * QUART, QUART)], r1.at[p, o - 1], s1.at[p, o - 1], v1.at[p, o - 1], peer(d, o))
            for o in offs
        ])
    c2, base1 = [], []
    for p in range(3):
        for copy in c1[p]:
            copy.wait_recv()
        base = PART * p + coord[dims[p][0]] * QUART
        base1.append(base)
        mine = pl.ds(base, QUART)
        d2d[mine, :] = ((d2d[mine, :] + r1[p, 0]) + r1[p, 1]) + r1[p, 2]
        d = dims[p][1]
        c2.append([
            send(d2d.at[pl.ds(base + lax.rem(coord[d] + o, 4) * SIXT, SIXT)], r2.at[p, o - 1], s2.at[p, o - 1], v2.at[p, o - 1], peer(d, o))
            for o in offs
        ])
    c3, base2 = [], []
    for p in range(3):
        for copy in c2[p]:
            copy.wait_recv()
        base = base1[p] + coord[dims[p][1]] * SIXT
        base2.append(base)
        d = dims[p][2]
        k = coord[d]
        r3[p, k] = ((d2d[pl.ds(base, SIXT), :] + r2[p, 0]) + r2[p, 1]) + r2[p, 2]
        c3.append([send(r3.at[p, k], r3.at[p, k], s3.at[p, o - 1], v3.at[p, o - 1], peer(d, o)) for o in offs])
    c4 = []
    for p in range(3):
        for copy in c3[p]:
            copy.wait_recv()
        mine = pl.ds(base2[p], SIXT)
        o_ref[core, mine, :] = ((r3[p, 0] + r3[p, 1]) + r3[p, 2]) + r3[p, 3]
        c4.append([send(out.at[mine], out.at[mine], s4.at[p, o - 1], v4.at[p, o - 1], peer(dims[p][1], o)) for o in offs])
    c5, c6 = [], []
    for p in range(3):
        for copy in c4[p]:
            copy.wait_recv()
        mine = pl.ds(base1[p], QUART)
        c5.append([send(out.at[mine], out.at[mine], s5.at[p, o - 1], v5.at[p, o - 1], peer(dims[p][0], o)) for o in offs])
        c6.append(send(out.at[mine], out.at[mine], dsem.at[2, p], dsem.at[3, p], sib))
    for p in range(3):
        for i, o in enumerate(offs):
            c5[p][i].wait_recv()
            src = pl.ds(PART * p + lax.rem(coord[dims[p][0]] + 4 - o, 4) * QUART, QUART)
            c6.append(send(out.at[src], out.at[src], dsem.at[4 + 2 * i, p], dsem.at[5 + 2 * i, p], sib))
    for copy in c6:
        copy.wait_recv()
    for copy in started:
        copy.wait_send()


def allsum(packed):
    dma = pltpu.SemaphoreType.DMA
    return pl.pallas_call(
        allsum_body,
        in_specs=[pl.BlockSpec(memory_space=pltpu.VMEM)],
        out_specs=pl.BlockSpec(memory_space=pltpu.VMEM),
        out_shape=jax.ShapeDtypeStruct((2, HALF, 128), F32),
        scratch_shapes=[
            pltpu.VMEM((HALF, 128), F32),
            pltpu.VMEM((3, 3, QUART, 128), F32),
            pltpu.VMEM((3, 3, SIXT, 128), F32),
            pltpu.VMEM((3, 4, SIXT, 128), F32),
            dma((10, 3)),
        ] + [dma((3, 3)) for _ in range(10)],
        compiler_params=pltpu.CompilerParams(collective_id=1, has_side_effects=True, vmem_limit_bytes=24 * MIB),
        cost_estimate=cost(1e9, 1e7),
        name="allsum",
    )(packed)


def solution(mesh):
    data_n, rep_n = mesh.shape["data"], mesh.shape["rep"]
    swap = [(src, (src + 1) % data_n) for src in range(data_n)]
    row_spec = P(("rep", "data"), None)

    def device_body(img_loc, txt_loc, w_img, w_txt, log_temp, logit_bias):
        rows, feat_i = img_loc.shape
        feat_t = txt_loc.shape[1]
        dim = w_img.shape[1]
        total_rows = float(rows * rep_n * data_n)
        scal = jnp.stack([jnp.exp(log_temp), logit_bias])
        raw_t, emb_t = head(txt_loc, w_txt, False, "text_head")
        emb_t = emb_t.reshape(rows // BN, BN, dim)
        away_t = lax.ppermute(emb_t, "data", swap)
        raw_i, emb_i, emb_it = head(img_loc, w_img, True, "image_head")
        away_di, away_dt, sums = away_tile(scal, emb_i, emb_it, away_t, total_rows)
        got_dt = lax.ppermute(away_dt, "data", swap)
        own_dt, dwi, sums = home_tile(scal, emb_i, emb_it, emb_t, raw_i, img_loc, away_di, sums, total_rows)
        packed = text_back(scal, own_dt, got_dt, raw_t, txt_loc, dwi, sums, total_rows)
        total = allsum(packed)
        size = 2 * (feat_i + feat_t)
        split = 4 * feat_i - size
        flat_i = jnp.concatenate([total[0, :size], total[1, :split]])
        flat_t = total[1, split:size]
        dw_img = flat_i.reshape(4, feat_i, 128).transpose(1, 0, 2).reshape(feat_i, dim)
        dw_txt = flat_t.reshape(4, feat_t, 128).transpose(1, 0, 2).reshape(feat_t, dim)
        return total[0, size, 0], total[0, size + 1, 0], total[0, size + 2, 0], dw_img, dw_txt

    return jax.shard_map(device_body, mesh=mesh, in_specs=(row_spec, row_spec, P(), P(), P(), P()), out_specs=(P(), P(), P(), P(), P()), check_vma=False)
```

```python
import functools

import jax
import jax.numpy as jnp
from jax import lax
from jax.experimental import pallas as pl
from jax.experimental.pallas import tpu as pltpu
from jax.sharding import PartitionSpec as P

LOG2E = 1.4426950408889634
LN2 = 0.6931471805599453
NT = (((1,), (1,)), ((), ()))
TN = (((0,), (0,)), ((), ()))
MESH = pl.DeviceIdType.MESH
F32 = jnp.float32
BF16 = jnp.bfloat16
MIB = 1024 * 1024

BM = 512
BN = 512
CR, CC = 16, 256
HALF = 2688
PART = HALF // 3
QUART = PART // 4
SIXT = QUART // 4


def inv_norm(raw):
    return lax.rsqrt(jnp.sum(raw * raw, axis=1, keepdims=True))


def params(vmem, **kw):
    return pltpu.CompilerParams(dimension_semantics=("arbitrary",), vmem_limit_bytes=vmem * MIB, **kw)


def cost(flops, nbytes):
    return pl.CostEstimate(flops=int(flops), bytes_accessed=int(nbytes), transcendentals=0)


def head_body(x_ref, w_ref, raw_ref, emb_ref, *maybe_t):
    raw = jnp.dot(x_ref[...], w_ref[...], preferred_element_type=F32)
    raw_ref[...] = raw
    emb = (raw * inv_norm(raw)).astype(BF16)
    emb_ref[...] = emb
    if maybe_t:
        maybe_t[0][...] = emb.T


def head(x, w, transposed, name):
    rows, feat = x.shape
    dim = w.shape[1]
    out_shape = [jax.ShapeDtypeStruct((rows, dim), F32), jax.ShapeDtypeStruct((rows, dim), BF16)]
    out_specs = [pl.BlockSpec((BM, dim), lambda i: (i, 0)), pl.BlockSpec((BM, dim), lambda i: (i, 0))]
    if transposed:
        out_shape.append(jax.ShapeDtypeStruct((dim, rows), BF16))
        out_specs.append(pl.BlockSpec((dim, BM), lambda i: (0, i)))
    return pl.pallas_call(
        head_body,
        grid=(rows // BM,),
        in_specs=[pl.BlockSpec((BM, feat), lambda i: (i, 0)), pl.BlockSpec((feat, dim), lambda i: (0, 0))],
        out_specs=out_specs,
        out_shape=out_shape,
        compiler_params=params(62),
        cost_estimate=cost(2 * rows * feat * dim, rows * (2 * feat + 8 * dim)),
        name=name,
    )(x, w)


def pair_terms(sc_ref, img_ref, imgt_ref, txt_ref, di_ref, dt_ref, acc, s_scr, h_scr, total_rows, home, di_init):
    step = pl.program_id(0)
    blocks = txt_ref.shape[0]
    s = sc_ref[0]
    a, b, hs = s * LOG2E, sc_ref[1] * LOG2E, s / total_rows
    img, imgt = img_ref[...], imgt_ref[...]

    def block_of(k):
        return lax.rem(step + k, blocks) if home else k

    def logits(k):
        s_scr[k % 2] = lax.dot_general(img, txt_ref[block_of(k)], NT, preferred_element_type=F32)

    def terms(k):
        zero = jnp.zeros((CR, CC), F32)
        top, prod, g_sum, gs_sum = zero, zero, zero, zero
        for r in range(0, BM, CR):
            for c in range(0, BN, CC):
                dots = s_scr[k % 2, r:r + CR, c:c + CC]
                z = dots * a + b
                pos = jnp.maximum(z, 0.0)
                t = jnp.exp2(-jnp.abs(z))
                rcp = 1.0 / (1.0 + t)
                sig = jnp.where(z >= 0, rcp, t * rcp)
                if home and k == 0 and r < c + CC and c < r + CR:
                    eye = (lax.broadcasted_iota(jnp.int32, (CR, CC), 0) + r) == (lax.broadcasted_iota(jnp.int32, (CR, CC), 1) + c)
                    sig = jnp.where(eye, -jnp.where(z >= 0, t * rcp, rcp), sig)
                    pos = jnp.where(eye, jnp.maximum(-z, 0.0), pos)
                top = top + pos
                prod = (prod + t) + prod * t
                g_sum = g_sum + sig
                gs_sum = gs_sum + sig * dots
                h_scr[k % 2, r:r + CR, c:c + CC] = (sig * hs).astype(BF16)
        acc[0] += LN2 * top + jnp.log1p(prod)
        acc[1] += gs_sum
        acc[2] += g_sum

    def grads(k):
        h = h_scr[k % 2]
        part = jnp.dot(h, txt_ref[block_of(k)], preferred_element_type=F32)
        if k == 0:
            di_ref[...] = part if di_init is None else di_init[...] + part
        else:
            di_ref[...] += part
        dt_ref[block_of(k)] += jnp.dot(imgt, h, preferred_element_type=F32)

    logits(0)
    for k in range(blocks):
        if k + 1 < blocks:
            logits(k + 1)
        terms(k)
        grads(k)


def away_body(sc_ref, img_ref, imgt_ref, txt_ref, di_ref, dt_ref, sums_ref, s_scr, h_scr, *, total_rows):
    @pl.when(pl.program_id(0) == 0)
    def _():
        sums_ref[...] = jnp.zeros_like(sums_ref)
        dt_ref[...] = jnp.zeros_like(dt_ref)

    pair_terms(sc_ref, img_ref, imgt_ref, txt_ref, di_ref, dt_ref, sums_ref, s_scr, h_scr, total_rows, False, None)


def home_body(sc_ref, img_ref, imgt_ref, txt_ref, raw_ref, x_ref, away_ref, sums_in, dt_ref, dw_ref, sums_ref, s_scr, h_scr, di_ref, *, total_rows):
    @pl.when(pl.program_id(0) == 0)
    def _():
        sums_ref[...] = sums_in[...]
        dt_ref[...] = jnp.zeros_like(dt_ref)
        dw_ref[...] = jnp.zeros_like(dw_ref)

    pair_terms(sc_ref, img_ref, imgt_ref, txt_ref, di_ref, dt_ref, sums_ref, s_scr, h_scr, total_rows, True, away_ref)
    dw_ref[...] += lax.dot_general(x_ref[...], raw_grad(raw_ref[...], di_ref[...]), TN, preferred_element_type=F32)


def raw_grad(raw, grad_unit):
    inv = inv_norm(raw)
    unit = raw * inv
    proj = jnp.sum(unit * grad_unit, axis=1, keepdims=True)
    return (inv * (grad_unit - unit * proj)).astype(BF16)


def tile_scratch():
    return [pltpu.VMEM((2, BM, BN), F32), pltpu.VMEM((2, BM, BN), BF16)]


def whole(shape, **kw):
    return pl.BlockSpec(shape, lambda i: (0,) * len(shape), **kw)


def away_tile(scal, img, imgt, txt, total_rows):
    rows, dim = img.shape
    blocks = txt.shape[0]
    once = dict(pipeline_mode=pl.Buffered(1))
    return pl.pallas_call(
        functools.partial(away_body, total_rows=total_rows),
        grid=(rows // BM,),
        in_specs=[
            pl.BlockSpec(memory_space=pltpu.SMEM),
            pl.BlockSpec((BM, dim), lambda i: (i, 0)),
            pl.BlockSpec((dim, BM), lambda i: (0, i)),
            whole((blocks, BN, dim), **once),
        ],
        out_specs=[pl.BlockSpec((BM, dim), lambda i: (i, 0)), whole((blocks, dim, BN), **once), whole((3, CR, CC))],
        out_shape=[
            jax.ShapeDtypeStruct((rows, dim), F32),
            jax.ShapeDtypeStruct((blocks, dim, BN), F32),
            jax.ShapeDtypeStruct((3, CR, CC), F32),
        ],
        scratch_shapes=tile_scratch(),
        compiler_params=params(62),
        cost_estimate=cost(6 * rows * rows * dim, 30 * rows * dim),
        name="away_tile",
    )(scal, img, imgt, txt)


def home_tile(scal, img, imgt, txt, raw, x, away, sums, total_rows):
    rows, dim = img.shape
    feat = x.shape[1]
    blocks = txt.shape[0]
    once = dict(pipeline_mode=pl.Buffered(1))
    return pl.pallas_call(
        functools.partial(home_body, total_rows=total_rows),
        grid=(rows // BM,),
        in_specs=[
            pl.BlockSpec(memory_space=pltpu.SMEM),
            pl.BlockSpec((BM, dim), lambda i: (i, 0)),
            pl.BlockSpec((dim, BM), lambda i: (0, i)),
            whole((blocks, BN, dim), **once),
            pl.BlockSpec((BM, dim), lambda i: (i, 0)),
            pl.BlockSpec((BM, feat), lambda i: (i, 0)),
            pl.BlockSpec((BM, dim), lambda i: (i, 0)),
            whole((3, CR, CC)),
        ],
        out_specs=[whole((blocks, dim, BN), **once), whole((feat, dim), **once), whole((3, CR, CC))],
        out_shape=[
            jax.ShapeDtypeStruct((blocks, dim, BN), F32),
            jax.ShapeDtypeStruct((feat, dim), F32),
            jax.ShapeDtypeStruct((3, CR, CC), F32),
        ],
        scratch_shapes=tile_scratch() + [pltpu.VMEM((BM, dim), F32)],
        compiler_params=params(62),
        cost_estimate=cost(6 * rows * rows * dim, 40 * rows * dim),
        name="home_tile",
    )(scal, img, imgt, txt, raw, x, away, sums)


def text_body(sc_ref, own_ref, got_ref, raw_ref, x_ref, dwi_ref, sums_ref, out_ref, dw_ref, *, total_rows):
    step = pl.program_id(0)

    @pl.when(step == 0)
    def _():
        dw_ref[...] = jnp.zeros_like(dw_ref)

    grad = (own_ref[0] + got_ref[0]).T
    dw_ref[...] += lax.dot_general(x_ref[...], raw_grad(raw_ref[...], grad), TN, preferred_element_type=F32)

    @pl.when(step == pl.num_programs(0) - 1)
    def _():
        feat_i, feat_t = dwi_ref.shape[0], dw_ref.shape[0]
        flat = []
        for l in range(4):
            flat.append((dwi_ref, l, feat_i))
        for l in range(4):
            flat.append((dw_ref, l, feat_t))
        pos = 0
        size = 2 * feat_i + 2 * feat_t
        for ref, l, n in flat:
            done = 0
            while done < n:
                half, at = divmod(pos, size)
                take = min(n - done, size - at)
                out_ref[half, at:at + take, :] = ref[done:done + take, 128 * l:128 * (l + 1)]
                done += take
                pos += take
        out_ref[:, size:, :] = jnp.zeros((2, HALF - size, 128), F32)
        s = sc_ref[0]
        row = lax.broadcasted_iota(jnp.int32, (8, 128), 0)
        loss = jnp.sum(sums_ref[0]) / total_rows
        temp = jnp.sum(sums_ref[1]) * (s / total_rows)
        bias = jnp.sum(sums_ref[2]) / total_rows
        out_ref[0, size:size + 8, :] = jnp.where(row == 0, loss, jnp.where(row == 1, temp, bias))


def text_back(scal, own, got, raw, x, dwi, sums, total_rows):
    rows, dim = raw.shape
    feat = x.shape[1]
    return pl.pallas_call(
        functools.partial(text_body, total_rows=total_rows),
        grid=(rows // BN,),
        in_specs=[
            pl.BlockSpec(memory_space=pltpu.SMEM),
            pl.BlockSpec((1, dim, BN), lambda i: (i, 0, 0)),
            pl.BlockSpec((1, dim, BN), lambda i: (i, 0, 0)),
            pl.BlockSpec((BN, dim), lambda i: (i, 0)),
            pl.BlockSpec((BN, feat), lambda i: (i, 0)),
            whole(dwi.shape),
            whole((3, CR, CC)),
        ],
        out_specs=whole((2, HALF, 128)),
        out_shape=jax.ShapeDtypeStruct((2, HALF, 128), F32),
        scratch_shapes=[pltpu.VMEM((feat, dim), F32)],
        compiler_params=params(57),
        cost_estimate=cost(2 * rows * feat * dim, rows * (2 * feat + 12 * dim)),
        name="text_back",
    )(scal, own, got, raw, x, dwi, sums)


def allsum_body(a_ref, o_ref, d2d, r1, r2, r3, dsem, s1, v1, s2, v2, s3, v3, s4, v4, s5, v5):
    rep, core = lax.axis_index("rep"), lax.axis_index("data")
    coord = [lax.rem(rep, 4), lax.rem(lax.div(rep, 4), 4), lax.div(rep, 16)]
    stride = [1, 4, 16]

    def peer(dim, off):
        return (rep + (lax.rem(coord[dim] + off, 4) - coord[dim]) * stride[dim], core)

    sib = (rep, 1 - core)
    bar = pltpu.get_barrier_semaphore()
    pl.semaphore_signal(bar, inc=1, device_id=sib, device_id_type=MESH)
    for dim in range(3):
        for off in (1, 2, 3):
            pl.semaphore_signal(bar, inc=1, device_id=peer(dim, off), device_id_type=MESH)
    pl.semaphore_wait(bar, 10)

    started = []

    def send(src, dst, ssem, rsem, dev):
        copy = pltpu.make_async_remote_copy(src_ref=src, dst_ref=dst, send_sem=ssem, recv_sem=rsem, device_id=dev, device_id_type=MESH)
        copy.start()
        started.append(copy)
        return copy

    out = o_ref.at[core]
    dims = [(p, (p + 1) % 3, (p + 2) % 3) for p in range(3)]
    offs = (2, 1, 3)

    c0 = []
    for p in range(3):
        rows = pl.ds(PART * p, PART)
        c0.append(send(a_ref.at[1 - core, rows], d2d.at[rows], dsem.at[0, p], dsem.at[1, p], sib))
    c1 = []
    for p in range(3):
        c0[p].wait_recv()
        rows = pl.ds(PART * p, PART)
        d2d[rows, :] = d2d[rows, :] + a_ref[core, rows, :]
        d = dims[p][0]
        c1.append([
            send(d2d.at[pl.ds(PART * p + lax.rem(coord[d] + o, 4) * QUART, QUART)], r1.at[p, o - 1], s1.at[p, o - 1], v1.at[p, o - 1], peer(d, o))
            for o in offs
        ])
    c2, base1 = [], []
    for p in range(3):
        for copy in c1[p]:
            copy.wait_recv()
        base = PART * p + coord[dims[p][0]] * QUART
        base1.append(base)
        mine = pl.ds(base, QUART)
        d2d[mine, :] = ((d2d[mine, :] + r1[p, 0]) + r1[p, 1]) + r1[p, 2]
        d = dims[p][1]
        c2.append([
            send(d2d.at[pl.ds(base + lax.rem(coord[d] + o, 4) * SIXT, SIXT)], r2.at[p, o - 1], s2.at[p, o - 1], v2.at[p, o - 1], peer(d, o))
            for o in offs
        ])
    c3, base2 = [], []
    for p in range(3):
        for copy in c2[p]:
            copy.wait_recv()
        base = base1[p] + coord[dims[p][1]] * SIXT
        base2.append(base)
        d = dims[p][2]
        k = coord[d]
        r3[p, k] = ((d2d[pl.ds(base, SIXT), :] + r2[p, 0]) + r2[p, 1]) + r2[p, 2]
        c3.append([send(r3.at[p, k], r3.at[p, k], s3.at[p, o - 1], v3.at[p, o - 1], peer(d, o)) for o in offs])
    c4 = []
    for p in range(3):
        for copy in c3[p]:
            copy.wait_recv()
        mine = pl.ds(base2[p], SIXT)
        o_ref[core, mine, :] = ((r3[p, 0] + r3[p, 1]) + r3[p, 2]) + r3[p, 3]
        c4.append([send(out.at[mine], out.at[mine], s4.at[p, o - 1], v4.at[p, o - 1], peer(dims[p][1], o)) for o in offs])
    c5, c6 = [], []
    for p in range(3):
        for copy in c4[p]:
            copy.wait_recv()
        mine = pl.ds(base1[p], QUART)
        c5.append([send(out.at[mine], out.at[mine], s5.at[p, o - 1], v5.at[p, o - 1], peer(dims[p][0], o)) for o in offs])
        c6.append(send(out.at[mine], out.at[mine], dsem.at[2, p], dsem.at[3, p], sib))
    for p in range(3):
        for i, o in enumerate(offs):
            c5[p][i].wait_recv()
            src = pl.ds(PART * p + lax.rem(coord[dims[p][0]] + 4 - o, 4) * QUART, QUART)
            c6.append(send(out.at[src], out.at[src], dsem.at[4 + 2 * i, p], dsem.at[5 + 2 * i, p], sib))
    for copy in c6:
        copy.wait_recv()
    for copy in started:
        copy.wait_send()


def allsum(packed):
    dma = pltpu.SemaphoreType.DMA
    return pl.pallas_call(
        allsum_body,
        in_specs=[pl.BlockSpec(memory_space=pltpu.VMEM)],
        out_specs=pl.BlockSpec(memory_space=pltpu.VMEM),
        out_shape=jax.ShapeDtypeStruct((2, HALF, 128), F32),
        scratch_shapes=[
            pltpu.VMEM((HALF, 128), F32),
            pltpu.VMEM((3, 3, QUART, 128), F32),
            pltpu.VMEM((3, 3, SIXT, 128), F32),
            pltpu.VMEM((3, 4, SIXT, 128), F32),
            dma((10, 3)),
        ] + [dma((3, 3)) for _ in range(10)],
        compiler_params=pltpu.CompilerParams(collective_id=1, has_side_effects=True, vmem_limit_bytes=24 * MIB),
        cost_estimate=cost(1e9, 1e7),
        name="allsum",
    )(packed)


def solution(mesh):
    data_n, rep_n = mesh.shape["data"], mesh.shape["rep"]
    swap = [(src, (src + 1) % data_n) for src in range(data_n)]
    row_spec = P(("rep", "data"), None)

    def device_body(img_loc, txt_loc, w_img, w_txt, log_temp, logit_bias):
        rows, feat_i = img_loc.shape
        feat_t = txt_loc.shape[1]
        dim = w_img.shape[1]
        total_rows = float(rows * rep_n * data_n)
        scal = jnp.stack([jnp.exp(log_temp), logit_bias])
        raw_t, emb_t = head(txt_loc, w_txt, False, "text_head")
        emb_t = emb_t.reshape(rows // BN, BN, dim)
        away_t = lax.ppermute(emb_t, "data", swap)
        raw_i, emb_i, emb_it = head(img_loc, w_img, True, "image_head")
        away_di, away_dt, sums = away_tile(scal, emb_i, emb_it, away_t, total_rows)
        got_dt = lax.ppermute(away_dt, "data", swap)
        own_dt, dwi, sums = home_tile(scal, emb_i, emb_it, emb_t, raw_i, img_loc, away_di, sums, total_rows)
        packed = text_back(scal, own_dt, got_dt, raw_t, txt_loc, dwi, sums, total_rows)
        total = allsum(packed)
        size = 2 * (feat_i + feat_t)
        split = 4 * feat_i - size
        flat_i = jnp.concatenate([total[0, :size], total[1, :split]])
        flat_t = total[1, split:size]
        dw_img = flat_i.reshape(4, feat_i, 128).transpose(1, 0, 2).reshape(feat_i, dim)
        dw_txt = flat_t.reshape(4, feat_t, 128).transpose(1, 0, 2).reshape(feat_t, dim)
        return total[0, size, 0], total[0, size + 1, 0], total[0, size + 2, 0], dw_img, dw_txt

    return jax.shard_map(device_body, mesh=mesh, in_specs=(row_spec, row_spec, P(), P(), P(), P()), out_specs=(P(), P(), P(), P(), P()), check_vma=False)
```

```python
import functools

import jax
import jax.numpy as jnp
from jax import lax
from jax.experimental import pallas as pl
from jax.experimental.pallas import tpu as pltpu
from jax.sharding import PartitionSpec as P

LOG2E = 1.4426950408889634
LN2 = 0.6931471805599453
NT = (((1,), (1,)), ((), ()))
TN = (((0,), (0,)), ((), ()))
MESH = pl.DeviceIdType.MESH
F32 = jnp.float32
BF16 = jnp.bfloat16
MIB = 1024 * 1024

BM = 512
BN = 512
CR, CC = 16, 256
HALF = 2688
PART = HALF // 3
QUART = PART // 4
SIXT = QUART // 4


def inv_norm(raw):
    return lax.rsqrt(jnp.sum(raw * raw, axis=1, keepdims=True))


def params(vmem, **kw):
    return pltpu.CompilerParams(dimension_semantics=("arbitrary",), vmem_limit_bytes=vmem * MIB, **kw)


def scale_of(temp_ref):
    return jnp.exp(jnp.full((8, 128), temp_ref[0], F32))[0, 0]


def cost(flops, nbytes):
    return pl.CostEstimate(flops=int(flops), bytes_accessed=int(nbytes), transcendentals=0)


def head_body(x_ref, w_ref, emb_ref, *maybe_raw):
    raw = jnp.dot(x_ref[...], w_ref[...], preferred_element_type=F32)
    if maybe_raw:
        maybe_raw[0][...] = raw
    emb_ref[...] = (raw * inv_norm(raw)).astype(BF16)


def head(x, w, keep_raw, name):
    rows, feat = x.shape
    dim = w.shape[1]
    out_shape = [jax.ShapeDtypeStruct((rows, dim), BF16)]
    out_specs = [pl.BlockSpec((BM, dim), lambda i: (i, 0))]
    if keep_raw:
        out_shape.append(jax.ShapeDtypeStruct((rows, dim), F32))
        out_specs.append(pl.BlockSpec((BM, dim), lambda i: (i, 0)))
    return pl.pallas_call(
        head_body,
        grid=(rows // BM,),
        in_specs=[pl.BlockSpec((BM, feat), lambda i: (i, 0)), pl.BlockSpec((feat, dim), lambda i: (0, 0))],
        out_specs=out_specs,
        out_shape=out_shape,
        compiler_params=params(62),
        cost_estimate=cost(2 * rows * feat * dim, rows * (2 * feat + 6 * dim)),
        name=name,
    )(x, w)


def pair_terms(temp_ref, bias_ref, img_ref, txt_ref, di_ref, dt_ref, acc, s_scr, h_scr, imgt_scr, total_rows, home, di_init):
    step = pl.program_id(0)
    blocks = txt_ref.shape[0]
    s = scale_of(temp_ref)
    a, b, hs = s * LOG2E, bias_ref[0] * LOG2E, s * (1.0 / total_rows)
    img = img_ref[...]
    imgt_scr[...] = img.T

    def block_of(k):
        return lax.rem(step + k, blocks) if home else k

    def logits(k):
        s_scr[k % 2] = lax.dot_general(img, txt_ref[block_of(k)], NT, preferred_element_type=F32)

    def terms(k):
        zero = jnp.zeros((CR, CC), F32)
        top, prod, g_sum, gs_sum = zero, zero, zero, zero
        for r in range(0, BM, CR):
            for c in range(0, BN, CC):
                dots = s_scr[k % 2, r:r + CR, c:c + CC]
                z = dots * a + b
                pos = jnp.maximum(z, 0.0)
                t = jnp.exp2(-jnp.abs(z))
                rcp = 1.0 / (1.0 + t)
                sig = jnp.where(z >= 0, rcp, t * rcp)
                if home and k == 0 and r < c + CC and c < r + CR:
                    eye = (lax.broadcasted_iota(jnp.int32, (CR, CC), 0) + r) == (lax.broadcasted_iota(jnp.int32, (CR, CC), 1) + c)
                    sig = jnp.where(eye, -jnp.where(z >= 0, t * rcp, rcp), sig)
                    pos = jnp.where(eye, jnp.maximum(-z, 0.0), pos)
                top = top + pos
                prod = (prod + t) + prod * t
                g_sum = g_sum + sig
                gs_sum = gs_sum + sig * dots
                h_scr[k % 2, r:r + CR, c:c + CC] = (sig * hs).astype(BF16)
        acc[0] += LN2 * top + jnp.log1p(prod)
        acc[1] += gs_sum
        acc[2] += g_sum

    def grads(k):
        h = h_scr[k % 2]
        part = jnp.dot(h, txt_ref[block_of(k)], preferred_element_type=F32)
        if k == 0:
            di_ref[...] = part if di_init is None else di_init[...] + part
        else:
            di_ref[...] += part
        dt_ref[block_of(k)] += jnp.dot(imgt_scr[...], h, preferred_element_type=F32)

    logits(0)
    for k in range(blocks):
        if k + 1 < blocks:
            logits(k + 1)
        terms(k)
        grads(k)


def away_body(temp_ref, bias_ref, img_ref, txt_ref, di_ref, dt_ref, sums_ref, s_scr, h_scr, imgt_scr, *, total_rows):
    @pl.when(pl.program_id(0) == 0)
    def _():
        sums_ref[...] = jnp.zeros_like(sums_ref)
        dt_ref[...] = jnp.zeros_like(dt_ref)

    pair_terms(temp_ref, bias_ref, img_ref, txt_ref, di_ref, dt_ref, sums_ref, s_scr, h_scr, imgt_scr, total_rows, False, None)


def home_body(temp_ref, bias_ref, img_ref, txt_ref, raw_ref, x_ref, away_ref, sums_in, dt_ref, dw_ref, sums_ref, s_scr, h_scr, imgt_scr, di_ref, *, total_rows):
    @pl.when(pl.program_id(0) == 0)
    def _():
        sums_ref[...] = sums_in[...]
        dt_ref[...] = jnp.zeros_like(dt_ref)
        dw_ref[...] = jnp.zeros_like(dw_ref)

    pair_terms(temp_ref, bias_ref, img_ref, txt_ref, di_ref, dt_ref, sums_ref, s_scr, h_scr, imgt_scr, total_rows, True, away_ref)
    dw_ref[...] += lax.dot_general(x_ref[...], raw_grad(raw_ref[...], di_ref[...]), TN, preferred_element_type=F32)


def raw_grad(raw, grad_unit):
    inv = inv_norm(raw)
    unit = raw * inv
    proj = jnp.sum(unit * grad_unit, axis=1, keepdims=True)
    return (inv * (grad_unit - unit * proj)).astype(BF16)


def tile_scratch(dim):
    return [pltpu.VMEM((2, BM, BN), F32), pltpu.VMEM((2, BM, BN), BF16), pltpu.VMEM((dim, BM), BF16)]


def whole(shape, **kw):
    return pl.BlockSpec(shape, lambda i: (0,) * len(shape), **kw)


def away_tile(temp, bias, img, txt, total_rows):
    rows, dim = img.shape
    blocks = txt.shape[0]
    once = dict(pipeline_mode=pl.Buffered(1))
    return pl.pallas_call(
        functools.partial(away_body, total_rows=total_rows),
        grid=(rows // BM,),
        in_specs=[
            pl.BlockSpec(memory_space=pltpu.SMEM),
            pl.BlockSpec(memory_space=pltpu.SMEM),
            pl.BlockSpec((BM, dim), lambda i: (i, 0)),
            whole((blocks, BN, dim), **once),
        ],
        out_specs=[pl.BlockSpec((BM, dim), lambda i: (i, 0)), whole((blocks, dim, BN), **once), whole((3, CR, CC))],
        out_shape=[
            jax.ShapeDtypeStruct((rows, dim), F32),
            jax.ShapeDtypeStruct((blocks, dim, BN), F32),
            jax.ShapeDtypeStruct((3, CR, CC), F32),
        ],
        scratch_shapes=tile_scratch(dim),
        compiler_params=params(62),
        cost_estimate=cost(6 * rows * rows * dim, 30 * rows * dim),
        name="away_tile",
    )(temp, bias, img, txt)


def home_tile(temp, bias, img, txt, raw, x, away, sums, total_rows):
    rows, dim = img.shape
    feat = x.shape[1]
    blocks = txt.shape[0]
    once = dict(pipeline_mode=pl.Buffered(1))
    return pl.pallas_call(
        functools.partial(home_body, total_rows=total_rows),
        grid=(rows // BM,),
        in_specs=[
            pl.BlockSpec(memory_space=pltpu.SMEM),
            pl.BlockSpec(memory_space=pltpu.SMEM),
            pl.BlockSpec((BM, dim), lambda i: (i, 0)),
            whole((blocks, BN, dim), **once),
            pl.BlockSpec((BM, dim), lambda i: (i, 0)),
            pl.BlockSpec((BM, feat), lambda i: (i, 0)),
            pl.BlockSpec((BM, dim), lambda i: (i, 0)),
            whole((3, CR, CC)),
        ],
        out_specs=[whole((blocks, dim, BN), **once), whole((feat, dim), **once), whole((3, CR, CC))],
        out_shape=[
            jax.ShapeDtypeStruct((blocks, dim, BN), F32),
            jax.ShapeDtypeStruct((feat, dim), F32),
            jax.ShapeDtypeStruct((3, CR, CC), F32),
        ],
        scratch_shapes=tile_scratch(dim) + [pltpu.VMEM((BM, dim), F32)],
        compiler_params=params(62),
        cost_estimate=cost(6 * rows * rows * dim, 40 * rows * dim),
        name="home_tile",
    )(temp, bias, img, txt, raw, x, away, sums)


def text_body(temp_ref, own_ref, got_ref, x_ref, w_ref, dwi_ref, sums_ref, out_ref, dwt_ref, wt_ref, *, total_rows):
    step = pl.program_id(0)

    @pl.when(step == 0)
    def _():
        dwt_ref[...] = jnp.zeros_like(dwt_ref)
        wt_ref[...] = w_ref[...].T

    x = x_ref[...]
    raw = lax.dot_general(wt_ref[...], x, NT, preferred_element_type=F32)
    inv = lax.rsqrt(jnp.sum(raw * raw, axis=0, keepdims=True))
    unit = raw * inv
    grad = own_ref[0] + got_ref[0]
    proj = jnp.sum(unit * grad, axis=0, keepdims=True)
    raw_grad_t = (inv * (grad - unit * proj)).astype(BF16)
    dwt_ref[...] += jnp.dot(raw_grad_t, x, preferred_element_type=F32)

    @pl.when(step == pl.num_programs(0) - 1)
    def _():
        feat_i, feat_t = dwi_ref.shape[0], dwt_ref.shape[1]
        flat = [(dwi_ref, l, feat_i) for l in range(4)] + [(dwt_ref, l, feat_t) for l in range(4)]
        pos = 0
        size = 2 * feat_i + 2 * feat_t
        for ref, l, n in flat:
            done = 0
            while done < n:
                half, at = divmod(pos, size)
                take = min(n - done, size - at)
                if ref is dwt_ref:
                    out_ref[half, at:at + take, :] = ref[128 * l:128 * (l + 1), done:done + take].T
                else:
                    out_ref[half, at:at + take, :] = ref[done:done + take, 128 * l:128 * (l + 1)]
                done += take
                pos += take
        out_ref[:, size:, :] = jnp.zeros((2, HALF - size, 128), F32)
        s = scale_of(temp_ref)
        row = lax.broadcasted_iota(jnp.int32, (8, 128), 0)
        loss = jnp.sum(sums_ref[0]) / total_rows
        temp = jnp.sum(sums_ref[1]) * (s * (1.0 / total_rows))
        bias = jnp.sum(sums_ref[2]) / total_rows
        out_ref[0, size:size + 8, :] = jnp.where(row == 0, loss, jnp.where(row == 1, temp, bias))


def text_back(temp, own, got, x, w, dwi, sums, total_rows):
    rows, feat = x.shape
    dim = w.shape[1]
    return pl.pallas_call(
        functools.partial(text_body, total_rows=total_rows),
        grid=(rows // BN,),
        in_specs=[
            pl.BlockSpec(memory_space=pltpu.SMEM),
            pl.BlockSpec((1, dim, BN), lambda i: (i, 0, 0)),
            pl.BlockSpec((1, dim, BN), lambda i: (i, 0, 0)),
            pl.BlockSpec((BN, feat), lambda i: (i, 0)),
            whole((feat, dim)),
            whole(dwi.shape),
            whole((3, CR, CC)),
        ],
        out_specs=whole((2, HALF, 128)),
        out_shape=jax.ShapeDtypeStruct((2, HALF, 128), F32),
        scratch_shapes=[pltpu.VMEM((dim, feat), F32), pltpu.VMEM((dim, feat), BF16)],
        compiler_params=params(48),
        cost_estimate=cost(4 * rows * feat * dim, rows * (2 * feat + 8 * dim)),
        name="text_back",
    )(temp, own, got, x, w, dwi, sums)


def allsum_body(a_ref, o_ref, d2d, r1, r2, r3, dsem, s1, v1, s2, v2, s3, v3, s4, v4, s5, v5):
    rep, core = lax.axis_index("rep"), lax.axis_index("data")
    coord = [lax.rem(rep, 4), lax.rem(lax.div(rep, 4), 4), lax.div(rep, 16)]
    stride = [1, 4, 16]

    def peer(dim, off):
        return (rep + (lax.rem(coord[dim] + off, 4) - coord[dim]) * stride[dim], core)

    sib = (rep, 1 - core)
    bar = pltpu.get_barrier_semaphore()
    pl.semaphore_signal(bar, inc=1, device_id=sib, device_id_type=MESH)
    for dim in range(3):
        for off in (1, 2, 3):
            pl.semaphore_signal(bar, inc=1, device_id=peer(dim, off), device_id_type=MESH)
    pl.semaphore_wait(bar, 10)

    started = []

    def send(src, dst, ssem, rsem, dev):
        copy = pltpu.make_async_remote_copy(src_ref=src, dst_ref=dst, send_sem=ssem, recv_sem=rsem, device_id=dev, device_id_type=MESH)
        copy.start()
        started.append(copy)
        return copy

    out = o_ref.at[core]
    dims = [(p, (p + 1) % 3, (p + 2) % 3) for p in range(3)]
    offs = (2, 1, 3)

    c0 = []
    for p in range(3):
        rows = pl.ds(PART * p, PART)
        c0.append(send(a_ref.at[1 - core, rows], d2d.at[rows], dsem.at[0, p], dsem.at[1, p], sib))
    c1 = []
    for p in range(3):
        c0[p].wait_recv()
        rows = pl.ds(PART * p, PART)
        d2d[rows, :] = d2d[rows, :] + a_ref[core, rows, :]
        d = dims[p][0]
        c1.append([
            send(d2d.at[pl.ds(PART * p + lax.rem(coord[d] + o, 4) * QUART, QUART)], r1.at[p, o - 1], s1.at[p, o - 1], v1.at[p, o - 1], peer(d, o))
            for o in offs
        ])
    c2, base1 = [], []
    for p in range(3):
        for copy in c1[p]:
            copy.wait_recv()
        base = PART * p + coord[dims[p][0]] * QUART
        base1.append(base)
        mine = pl.ds(base, QUART)
        d2d[mine, :] = ((d2d[mine, :] + r1[p, 0]) + r1[p, 1]) + r1[p, 2]
        d = dims[p][1]
        c2.append([
            send(d2d.at[pl.ds(base + lax.rem(coord[d] + o, 4) * SIXT, SIXT)], r2.at[p, o - 1], s2.at[p, o - 1], v2.at[p, o - 1], peer(d, o))
            for o in offs
        ])
    c3, base2 = [], []
    for p in range(3):
        for copy in c2[p]:
            copy.wait_recv()
        base = base1[p] + coord[dims[p][1]] * SIXT
        base2.append(base)
        d = dims[p][2]
        k = coord[d]
        r3[p, k] = ((d2d[pl.ds(base, SIXT), :] + r2[p, 0]) + r2[p, 1]) + r2[p, 2]
        c3.append([send(r3.at[p, k], r3.at[p, k], s3.at[p, o - 1], v3.at[p, o - 1], peer(d, o)) for o in offs])
    c4 = []
    for p in range(3):
        for copy in c3[p]:
            copy.wait_recv()
        mine = pl.ds(base2[p], SIXT)
        o_ref[core, mine, :] = ((r3[p, 0] + r3[p, 1]) + r3[p, 2]) + r3[p, 3]
        c4.append([send(out.at[mine], out.at[mine], s4.at[p, o - 1], v4.at[p, o - 1], peer(dims[p][1], o)) for o in offs])
    c5, c6 = [], []
    for p in range(3):
        for copy in c4[p]:
            copy.wait_recv()
        mine = pl.ds(base1[p], QUART)
        c5.append([send(out.at[mine], out.at[mine], s5.at[p, o - 1], v5.at[p, o - 1], peer(dims[p][0], o)) for o in offs])
        c6.append(send(out.at[mine], out.at[mine], dsem.at[2, p], dsem.at[3, p], sib))
    for p in range(3):
        for i, o in enumerate(offs):
            c5[p][i].wait_recv()
            src = pl.ds(PART * p + lax.rem(coord[dims[p][0]] + 4 - o, 4) * QUART, QUART)
            c6.append(send(out.at[src], out.at[src], dsem.at[4 + 2 * i, p], dsem.at[5 + 2 * i, p], sib))
    for copy in c6:
        copy.wait_recv()
    for copy in started:
        copy.wait_send()


def allsum(packed):
    dma = pltpu.SemaphoreType.DMA
    return pl.pallas_call(
        allsum_body,
        in_specs=[pl.BlockSpec(memory_space=pltpu.VMEM)],
        out_specs=pl.BlockSpec(memory_space=pltpu.VMEM),
        out_shape=jax.ShapeDtypeStruct((2, HALF, 128), F32),
        scratch_shapes=[
            pltpu.VMEM((HALF, 128), F32),
            pltpu.VMEM((3, 3, QUART, 128), F32),
            pltpu.VMEM((3, 3, SIXT, 128), F32),
            pltpu.VMEM((3, 4, SIXT, 128), F32),
            dma((10, 3)),
        ] + [dma((3, 3)) for _ in range(10)],
        compiler_params=pltpu.CompilerParams(collective_id=1, has_side_effects=True, vmem_limit_bytes=24 * MIB),
        cost_estimate=cost(1e9, 1e7),
        name="allsum",
    )(packed)


def solution(mesh):
    data_n, rep_n = mesh.shape["data"], mesh.shape["rep"]
    swap = [(src, (src + 1) % data_n) for src in range(data_n)]
    row_spec = P(("rep", "data"), None)

    def device_body(img_loc, txt_loc, w_img, w_txt, log_temp, logit_bias):
        rows, feat_i = img_loc.shape
        feat_t = txt_loc.shape[1]
        dim = w_img.shape[1]
        total_rows = float(rows * rep_n * data_n)
        temp, bias = log_temp.reshape(1), logit_bias.reshape(1)
        (emb_t,) = head(txt_loc, w_txt, False, "text_head")
        emb_t = emb_t.reshape(rows // BN, BN, dim)
        away_t = lax.ppermute(emb_t, "data", swap)
        emb_i, raw_i = head(img_loc, w_img, True, "image_head")
        away_di, away_dt, sums = away_tile(temp, bias, emb_i, away_t, total_rows)
        got_dt = lax.ppermute(away_dt, "data", swap)
        own_dt, dwi, sums = home_tile(temp, bias, emb_i, emb_t, raw_i, img_loc, away_di, sums, total_rows)
        packed = text_back(temp, own_dt, got_dt, txt_loc, w_txt, dwi, sums, total_rows)
        total = allsum(packed)
        size = 2 * (feat_i + feat_t)
        split = 4 * feat_i - size
        flat_i = jnp.concatenate([total[0, :size], total[1, :split]])
        flat_t = total[1, split:size]
        dw_img = flat_i.reshape(4, feat_i, 128).transpose(1, 0, 2).reshape(feat_i, dim)
        dw_txt = flat_t.reshape(4, feat_t, 128).transpose(1, 0, 2).reshape(feat_t, dim)
        return total[0, size, 0], total[0, size + 1, 0], total[0, size + 2, 0], dw_img, dw_txt

    return jax.shard_map(device_body, mesh=mesh, in_specs=(row_spec, row_spec, P(), P(), P(), P()), out_specs=(P(), P(), P(), P(), P()), check_vma=False)
```

```python
import functools

import jax
import jax.numpy as jnp
from jax import lax
from jax.experimental import pallas as pl
from jax.experimental.pallas import tpu as pltpu
from jax.sharding import PartitionSpec as P

LOG2E = 1.4426950408889634
LN2 = 0.6931471805599453
NT = (((1,), (1,)), ((), ()))
TN = (((0,), (0,)), ((), ()))
MESH = pl.DeviceIdType.MESH
F32 = jnp.float32
BF16 = jnp.bfloat16
MIB = 1024 * 1024

BM = 512
BN = 512
CR, CC = 16, 256


def inv_norm(raw):
    return lax.rsqrt(jnp.sum(raw * raw, axis=1, keepdims=True))


def params(vmem, **kw):
    return pltpu.CompilerParams(dimension_semantics=("arbitrary",), vmem_limit_bytes=vmem * MIB, **kw)


def scale_of(sc_ref):
    return jnp.exp(jnp.full((8, 128), sc_ref[0], F32))[0, 0]


def cost(flops, nbytes):
    return pl.CostEstimate(flops=int(flops), bytes_accessed=int(nbytes), transcendentals=0)


def fetch(pairs, sems):
    copies = [pltpu.make_async_copy(src, dst, sems.at[i]) for i, (src, dst) in enumerate(pairs)]
    for copy in copies:
        copy.start()
    return copies


def head_body(x_hbm, w_hbm, *refs, keep_raw):
    outs, (x_ref, w_ref, emb_ref, raw_ref, in_sem, out_sem) = refs[:-6], refs[-6:]
    blocks = x_ref.shape[0]
    arrive = fetch([(w_hbm, w_ref)] + [(x_hbm.at[pl.ds(BM * i, BM)], x_ref.at[i]) for i in range(blocks)], in_sem)
    arrive[0].wait()
    leave = []
    for i in range(blocks):
        arrive[i + 1].wait()
        raw = jnp.dot(x_ref[i], w_ref[...], preferred_element_type=F32)
        emb_ref[i] = (raw * inv_norm(raw)).astype(BF16)
        pairs = [(emb_ref.at[i], outs[0].at[pl.ds(BM * i, BM)])]
        if keep_raw:
            raw_ref[i] = raw
            pairs.append((raw_ref.at[i], outs[1].at[pl.ds(BM * i, BM)]))
        leave += fetch(pairs, out_sem.at[i])
    for copy in leave:
        copy.wait()


def head(x, w, keep_raw, name):
    rows, feat = x.shape
    dim = w.shape[1]
    blocks = rows // BM
    hbm = pl.BlockSpec(memory_space=pl.ANY)
    out_shape = [jax.ShapeDtypeStruct((rows, dim), BF16)]
    if keep_raw:
        out_shape.append(jax.ShapeDtypeStruct((rows, dim), F32))
    return pl.pallas_call(
        functools.partial(head_body, keep_raw=keep_raw),
        in_specs=[hbm, hbm],
        out_specs=[hbm] * len(out_shape),
        out_shape=out_shape,
        scratch_shapes=[
            pltpu.VMEM((blocks, BM, feat), BF16),
            pltpu.VMEM((feat, dim), BF16),
            pltpu.VMEM((blocks, BM, dim), BF16),
            pltpu.VMEM((blocks if keep_raw else 1, BM, dim), F32),
            pltpu.SemaphoreType.DMA((blocks + 1,)),
            pltpu.SemaphoreType.DMA((blocks, 2)),
        ],
        compiler_params=pltpu.CompilerParams(vmem_limit_bytes=62 * MIB),
        cost_estimate=cost(2 * rows * feat * dim, rows * (2 * feat + 6 * dim)),
        name=name,
    )(x, w)


def pair_terms(sc_ref, img_ref, txt_ref, di_ref, dt_ref, acc, s_scr, h_scr, imgt_scr, total_rows, home, di_init):
    step = pl.program_id(0)
    blocks = txt_ref.shape[0]
    s = scale_of(sc_ref)
    a, b, hs = s * LOG2E, sc_ref[1] * LOG2E, s * (1.0 / total_rows)
    img = img_ref[...]
    imgt_scr[...] = img.T

    def block_of(k):
        return lax.rem(step + k, blocks) if home else k

    def logits(k):
        s_scr[k % 2] = lax.dot_general(img, txt_ref[block_of(k)], NT, preferred_element_type=F32)

    def terms(k):
        zero = jnp.zeros((CR, CC), F32)
        top, prod, g_sum, gs_sum = zero, zero, zero, zero
        for r in range(0, BM, CR):
            for c in range(0, BN, CC):
                dots = s_scr[k % 2, r:r + CR, c:c + CC]
                z = dots * a + b
                pos = jnp.maximum(z, 0.0)
                t = jnp.exp2(-jnp.abs(z))
                rcp = 1.0 / (1.0 + t)
                sig = jnp.where(z >= 0, rcp, t * rcp)
                if home and k == 0 and r < c + CC and c < r + CR:
                    eye = (lax.broadcasted_iota(jnp.int32, (CR, CC), 0) + r) == (lax.broadcasted_iota(jnp.int32, (CR, CC), 1) + c)
                    sig = jnp.where(eye, -jnp.where(z >= 0, t * rcp, rcp), sig)
                    pos = jnp.where(eye, jnp.maximum(-z, 0.0), pos)
                top = top + pos
                prod = (prod + t) + prod * t
                g_sum = g_sum + sig
                gs_sum = gs_sum + sig * dots
                h_scr[k % 2, r:r + CR, c:c + CC] = (sig * hs).astype(BF16)
        acc[0] += LN2 * top + jnp.log1p(prod)
        acc[1] += gs_sum
        acc[2] += g_sum

    def grads(k):
        h = h_scr[k % 2]
        part = jnp.dot(h, txt_ref[block_of(k)], preferred_element_type=F32)
        if k == 0:
            di_ref[...] = part if di_init is None else di_init[...] + part
        else:
            di_ref[...] += part
        dt_ref[block_of(k)] += jnp.dot(imgt_scr[...], h, preferred_element_type=F32)

    logits(0)
    for k in range(blocks):
        if k + 1 < blocks:
            logits(k + 1)
        terms(k)
        grads(k)


def away_body(sc_ref, img_ref, txt_ref, di_ref, dt_ref, sums_ref, s_scr, h_scr, imgt_scr, *, total_rows):
    @pl.when(pl.program_id(0) == 0)
    def _():
        sums_ref[...] = jnp.zeros_like(sums_ref)
        dt_ref[...] = jnp.zeros_like(dt_ref)

    pair_terms(sc_ref, img_ref, txt_ref, di_ref, dt_ref, sums_ref, s_scr, h_scr, imgt_scr, total_rows, False, None)


def home_body(sc_ref, img_ref, txt_ref, raw_ref, x_ref, away_ref, sums_in, dt_ref, dw_ref, sums_ref, s_scr, h_scr, imgt_scr, di_ref, *, total_rows):
    @pl.when(pl.program_id(0) == 0)
    def _():
        sums_ref[...] = sums_in[...]
        dt_ref[...] = jnp.zeros_like(dt_ref)
        dw_ref[...] = jnp.zeros_like(dw_ref)

    pair_terms(sc_ref, img_ref, txt_ref, di_ref, dt_ref, sums_ref, s_scr, h_scr, imgt_scr, total_rows, True, away_ref)
    dw_ref[...] += lax.dot_general(x_ref[...], raw_grad(raw_ref[...], di_ref[...]), TN, preferred_element_type=F32)


def raw_grad(raw, grad_unit):
    inv = inv_norm(raw)
    unit = raw * inv
    proj = jnp.sum(unit * grad_unit, axis=1, keepdims=True)
    return (inv * (grad_unit - unit * proj)).astype(BF16)


def tile_scratch(dim):
    return [pltpu.VMEM((2, BM, BN), F32), pltpu.VMEM((2, BM, BN), BF16), pltpu.VMEM((dim, BM), BF16)]


def whole(shape, **kw):
    return pl.BlockSpec(shape, lambda i: (0,) * len(shape), **kw)


def away_tile(scal, img, txt, total_rows):
    rows, dim = img.shape
    blocks = txt.shape[0]
    once = dict(pipeline_mode=pl.Buffered(1))
    return pl.pallas_call(
        functools.partial(away_body, total_rows=total_rows),
        grid=(rows // BM,),
        in_specs=[
            pl.BlockSpec(memory_space=pltpu.SMEM),
            pl.BlockSpec((BM, dim), lambda i: (i, 0)),
            whole((blocks, BN, dim), **once),
        ],
        out_specs=[pl.BlockSpec((BM, dim), lambda i: (i, 0)), whole((blocks, dim, BN), **once), whole((3, CR, CC))],
        out_shape=[
            jax.ShapeDtypeStruct((rows, dim), F32),
            jax.ShapeDtypeStruct((blocks, dim, BN), F32),
            jax.ShapeDtypeStruct((3, CR, CC), F32),
        ],
        scratch_shapes=tile_scratch(dim),
        compiler_params=params(62),
        cost_estimate=cost(6 * rows * rows * dim, 30 * rows * dim),
        name="away_tile",
    )(scal, img, txt)


def home_tile(scal, img, txt, raw, x, away, sums, total_rows):
    rows, dim = img.shape
    feat = x.shape[1]
    blocks = txt.shape[0]
    once = dict(pipeline_mode=pl.Buffered(1))
    return pl.pallas_call(
        functools.partial(home_body, total_rows=total_rows),
        grid=(rows // BM,),
        in_specs=[
            pl.BlockSpec(memory_space=pltpu.SMEM),
            pl.BlockSpec((BM, dim), lambda i: (i, 0)),
            whole((blocks, BN, dim), **once),
            pl.BlockSpec((BM, dim), lambda i: (i, 0)),
            pl.BlockSpec((BM, feat), lambda i: (i, 0)),
            pl.BlockSpec((BM, dim), lambda i: (i, 0)),
            whole((3, CR, CC)),
        ],
        out_specs=[whole((blocks, dim, BN), **once), whole((feat, dim), **once), whole((3, CR, CC))],
        out_shape=[
            jax.ShapeDtypeStruct((blocks, dim, BN), F32),
            jax.ShapeDtypeStruct((feat, dim), F32),
            jax.ShapeDtypeStruct((3, CR, CC), F32),
        ],
        scratch_shapes=tile_scratch(dim) + [pltpu.VMEM((BM, dim), F32)],
        compiler_params=params(62),
        cost_estimate=cost(6 * rows * rows * dim, 40 * rows * dim),
        name="home_tile",
    )(scal, img, txt, raw, x, away, sums)


def all_sum(src, out, bufs, peer, coord, core, send):
    pair, r1, r2, r3, psem, ssem, rsem = bufs
    part = src.shape[1] // 3
    quart, sixt = part // 4, part // 16
    sib = peer(3, 1)
    mine = out.at[core]
    dims = [(p, (p + 1) % 3, (p + 2) % 3) for p in range(3)]
    offs = (2, 1, 3)

    def spread(phase, p, d, src_of, dst_of):
        return [send(src_of(o), dst_of(o), ssem.at[phase, p, o - 1], rsem.at[phase, p, o - 1], peer(d, o)) for o in offs]

    c0 = []
    for p in range(3):
        rows = pl.ds(part * p, part)
        c0.append(send(src.at[1 - core, rows], pair.at[rows], psem.at[0, p], psem.at[1, p], sib))
    yield
    c1 = []
    for p in range(3):
        c0[p].wait_recv()
        rows = pl.ds(part * p, part)
        pair[rows, :] = pair[rows, :] + src[core, rows, :]
        d = dims[p][0]
        c1.append(spread(0, p, d, lambda o: pair.at[pl.ds(part * p + lax.rem(coord[d] + o, 4) * quart, quart)], lambda o: r1.at[p, o - 1]))
    yield
    c2, base1 = [], []
    for p in range(3):
        for copy in c1[p]:
            copy.wait_recv()
        base = part * p + coord[dims[p][0]] * quart
        base1.append(base)
        rows = pl.ds(base, quart)
        pair[rows, :] = ((pair[rows, :] + r1[p, 0]) + r1[p, 1]) + r1[p, 2]
        d = dims[p][1]
        c2.append(spread(1, p, d, lambda o: pair.at[pl.ds(base + lax.rem(coord[d] + o, 4) * sixt, sixt)], lambda o: r2.at[p, o - 1]))
    yield
    c3, base2 = [], []
    for p in range(3):
        for copy in c2[p]:
            copy.wait_recv()
        base = base1[p] + coord[dims[p][1]] * sixt
        base2.append(base)
        d = dims[p][2]
        k = coord[d]
        r3[p, k] = ((pair[pl.ds(base, sixt), :] + r2[p, 0]) + r2[p, 1]) + r2[p, 2]
        c3.append(spread(2, p, d, lambda o: r3.at[p, k], lambda o: r3.at[p, k]))
    yield
    c4 = []
    for p in range(3):
        for copy in c3[p]:
            copy.wait_recv()
        rows = pl.ds(base2[p], sixt)
        out[core, rows, :] = ((r3[p, 0] + r3[p, 1]) + r3[p, 2]) + r3[p, 3]
        c4.append(spread(3, p, dims[p][1], lambda o: mine.at[rows], lambda o: mine.at[rows]))
    yield
    c5, c6 = [], []
    for p in range(3):
        for copy in c4[p]:
            copy.wait_recv()
        rows = pl.ds(base1[p], quart)
        c5.append(spread(4, p, dims[p][0], lambda o: mine.at[rows], lambda o: mine.at[rows]))
        c6.append(send(mine.at[rows], mine.at[rows], psem.at[2, p], psem.at[3, p], sib))
    yield
    for p in range(3):
        for i, o in enumerate(offs):
            c5[p][i].wait_recv()
            rows = pl.ds(part * p + lax.rem(coord[dims[p][0]] + 4 - o, 4) * quart, quart)
            c6.append(send(mine.at[rows], mine.at[rows], psem.at[4 + 2 * i, p], psem.at[5 + 2 * i, p], sib))
    yield
    for copy in c6:
        copy.wait_recv()
    yield


def sum_scratch(rows):
    part = rows // 3
    dma = pltpu.SemaphoreType.DMA
    return [
        pltpu.VMEM((rows, 128), F32),
        pltpu.VMEM((3, 3, part // 4, 128), F32),
        pltpu.VMEM((3, 3, part // 16, 128), F32),
        pltpu.VMEM((3, 4, part // 16, 128), F32),
        dma((10, 3)),
        dma((5, 3, 3)),
        dma((5, 3, 3)),
    ]


def finish_body(sc_ref, own_hbm, got_hbm, x_hbm, w_hbm, dwi_hbm, sums_hbm, oi_ref, ot_ref, own_ref, got_ref, x_ref, w_ref, dwi_ref, sums_ref, dwt_ref, ai_ref, at_ref, sem, *bufs, total_rows):
    rep, core = lax.axis_index("rep"), lax.axis_index("data")
    coord = [lax.rem(rep, 4), lax.rem(lax.div(rep, 4), 4), lax.div(rep, 16)]
    stride = [1, 4, 16]

    def peer(dim, off):
        if dim == 3:
            return (rep, 1 - core)
        return (rep + (lax.rem(coord[dim] + off, 4) - coord[dim]) * stride[dim], core)

    bar = pltpu.get_barrier_semaphore()
    partners = [peer(3, 1)] + [peer(dim, off) for dim in range(3) for off in (1, 2, 3)]
    for dev in partners:
        pl.semaphore_signal(bar, inc=1, device_id=dev, device_id_type=MESH)

    blocks = own_ref.shape[0]
    pairs = [(dwi_hbm, dwi_ref), (w_hbm, w_ref)]
    for i in range(blocks):
        pairs += [(x_hbm.at[pl.ds(BN * i, BN)], x_ref.at[i]), (own_hbm.at[i], own_ref.at[i]), (got_hbm.at[i], got_ref.at[i])]
    arrive = fetch(pairs + [(sums_hbm, sums_ref)], sem)

    feat_i, feat_t = dwi_ref.shape[0], dwt_ref.shape[1]
    arrive[0].wait()
    for l in range(4):
        ai_ref[l // 2, pl.ds(feat_i * (l % 2), feat_i), :] = dwi_ref[:, 128 * l:128 * (l + 1)]
    pl.semaphore_wait(bar, len(partners))

    started = []

    def send(src, dst, ssem, rsem, dev):
        copy = pltpu.make_async_remote_copy(src_ref=src, dst_ref=dst, send_sem=ssem, recv_sem=rsem, device_id=dev, device_id_type=MESH)
        copy.start()
        started.append(copy)
        return copy

    img = all_sum(ai_ref, oi_ref, bufs[:7], peer, coord, core, send)
    txt = all_sum(at_ref, ot_ref, bufs[7:], peer, coord, core, send)
    next(img)
    arrive[1].wait()
    w_t = w_ref[...].T

    def block(i):
        for copy in arrive[2 + 3 * i:5 + 3 * i]:
            copy.wait()
        x = x_ref[i]
        raw = lax.dot_general(w_t, x, NT, preferred_element_type=F32)
        inv = lax.rsqrt(jnp.sum(raw * raw, axis=0, keepdims=True))
        unit = raw * inv
        grad = own_ref[i] + got_ref[i]
        proj = jnp.sum(unit * grad, axis=0, keepdims=True)
        raw_grad_t = (inv * (grad - unit * proj)).astype(BF16)
        part = jnp.dot(raw_grad_t, x, preferred_element_type=F32)
        dwt_ref[...] = part if i == 0 else dwt_ref[...] + part

    for i in range(blocks):
        block(i)
        if i == 1:
            next(img)
    for l in range(4):
        at_ref[l // 2, pl.ds(feat_t * (l % 2), feat_t), :] = dwt_ref[128 * l:128 * (l + 1), :].T
    arrive[-1].wait()
    s = scale_of(sc_ref)
    row = lax.broadcasted_iota(jnp.int32, (128, 128), 0)
    loss = jnp.sum(sums_ref[0]) / total_rows
    temp = jnp.sum(sums_ref[1]) * (s * (1.0 / total_rows))
    bias = jnp.sum(sums_ref[2]) / total_rows
    scalars = jnp.where(row == 0, loss, jnp.where(row == 1, temp, jnp.where(row == 2, bias, 0.0)))
    at_ref[0, 2 * feat_t:, :] = scalars
    at_ref[1, 2 * feat_t:, :] = jnp.zeros_like(scalars)
    next(txt)
    next(img)
    for _ in range(6):
        next(txt, None)
        next(img, None)
    next(txt, None)
    for copy in started:
        copy.wait_send()


def finish(scal, own, got, x, w, dwi, sums, total_rows):
    rows, feat = x.shape
    dim = w.shape[1]
    blocks = rows // BN
    img_rows, txt_rows = 2 * dwi.shape[0], 2 * feat + 128
    hbm = pl.BlockSpec(memory_space=pl.ANY)
    vmem = pl.BlockSpec(memory_space=pltpu.VMEM)
    return pl.pallas_call(
        functools.partial(finish_body, total_rows=total_rows),
        in_specs=[pl.BlockSpec(memory_space=pltpu.SMEM)] + [hbm] * 6,
        out_specs=[vmem, vmem],
        out_shape=[jax.ShapeDtypeStruct((2, img_rows, 128), F32), jax.ShapeDtypeStruct((2, txt_rows, 128), F32)],
        scratch_shapes=[
            pltpu.VMEM(own.shape, F32),
            pltpu.VMEM(own.shape, F32),
            pltpu.VMEM((blocks, BN, feat), BF16),
            pltpu.VMEM(w.shape, BF16),
            pltpu.VMEM(dwi.shape, F32),
            pltpu.VMEM(sums.shape, F32),
            pltpu.VMEM((dim, feat), F32),
            pltpu.VMEM((2, img_rows, 128), F32),
            pltpu.VMEM((2, txt_rows, 128), F32),
            pltpu.SemaphoreType.DMA((3 * blocks + 3,)),
        ] + sum_scratch(img_rows) + sum_scratch(txt_rows),
        compiler_params=pltpu.CompilerParams(collective_id=1, has_side_effects=True, vmem_limit_bytes=62 * MIB),
        cost_estimate=cost(1e9, 1e7),
        name="finish",
    )(scal, own, got, x, w, dwi, sums)


def solution(mesh):
    data_n, rep_n = mesh.shape["data"], mesh.shape["rep"]
    swap = [(src, (src + 1) % data_n) for src in range(data_n)]
    row_spec = P(("rep", "data"), None)

    def device_body(img_loc, txt_loc, w_img, w_txt, log_temp, logit_bias):
        rows, feat_i = img_loc.shape
        feat_t = txt_loc.shape[1]
        dim = w_img.shape[1]
        total_rows = float(rows * rep_n * data_n)
        scal = jnp.where(jnp.arange(2) == 0, log_temp, logit_bias)
        (emb_t,) = head(txt_loc, w_txt, False, "text_head")
        emb_t = emb_t.reshape(rows // BN, BN, dim)
        away_t = lax.ppermute(emb_t, "data", swap)
        emb_i, raw_i = head(img_loc, w_img, True, "image_head")
        away_di, away_dt, sums = away_tile(scal, emb_i, away_t, total_rows)
        got_dt = lax.ppermute(away_dt, "data", swap)
        own_dt, dwi, sums = home_tile(scal, emb_i, emb_t, raw_i, img_loc, away_di, sums, total_rows)
        img_sum, txt_sum = finish(scal, own_dt, got_dt, txt_loc, w_txt, dwi, sums, total_rows)
        dw_img = img_sum.reshape(4, feat_i, 128).transpose(1, 0, 2).reshape(feat_i, dim)
        dw_txt = txt_sum[:, :2 * feat_t].reshape(4, feat_t, 128).transpose(1, 0, 2).reshape(feat_t, dim)
        scalars = txt_sum[0, 2 * feat_t:2 * feat_t + 3, 0]
        return scalars[0], scalars[1], scalars[2], dw_img, dw_txt

    return jax.shard_map(device_body, mesh=mesh, in_specs=(row_spec, row_spec, P(), P(), P(), P()), out_specs=(P(), P(), P(), P(), P()), check_vma=False)
```

```python
import functools

import jax
import jax.numpy as jnp
from jax import lax
from jax.experimental import pallas as pl
from jax.experimental.pallas import tpu as pltpu
from jax.sharding import PartitionSpec as P

LOG2E = 1.4426950408889634
LN2 = 0.6931471805599453
NT = (((1,), (1,)), ((), ()))
TN = (((0,), (0,)), ((), ()))
MESH = pl.DeviceIdType.MESH
F32 = jnp.float32
BF16 = jnp.bfloat16
MIB = 1024 * 1024

BM = 512
BN = 256
CR, CC = 16, 256


def inv_norm(raw):
    return lax.rsqrt(jnp.sum(raw * raw, axis=1, keepdims=True))


def params(vmem):
    return pltpu.CompilerParams(
        dimension_semantics=("arbitrary",),
        vmem_limit_bytes=vmem * MIB,
    )


def scale_of(sc_ref):
    return jnp.exp(jnp.full((8, 128), sc_ref[0], F32))[0, 0]


def cost(flops, nbytes):
    return pl.CostEstimate(flops=int(flops), bytes_accessed=int(nbytes), transcendentals=0)


def fetch(pairs, sems):
    copies = [pltpu.make_async_copy(src, dst, sems.at[i]) for i, (src, dst) in enumerate(pairs)]
    for copy in copies:
        copy.start()
    return copies


def head_body(x_hbm, w_hbm, *refs, keep_raw):
    outs, (x_ref, w_ref, emb_ref, raw_ref, in_sem, out_sem) = refs[:-6], refs[-6:]
    blocks = x_ref.shape[0]
    arrive = fetch([(w_hbm, w_ref)] + [(x_hbm.at[pl.ds(BM * i, BM)], x_ref.at[i]) for i in range(blocks)], in_sem)
    arrive[0].wait()
    leave = []
    for i in range(blocks):
        arrive[i + 1].wait()
        raw = jnp.dot(x_ref[i], w_ref[...], preferred_element_type=F32)
        emb_ref[i] = (raw * inv_norm(raw)).astype(BF16)
        pairs = [(emb_ref.at[i], outs[0].at[pl.ds(BM * i, BM)])]
        if keep_raw:
            raw_ref[i] = raw
            pairs.append((raw_ref.at[i], outs[1].at[pl.ds(BM * i, BM)]))
        leave += fetch(pairs, out_sem.at[i])
    for copy in leave:
        copy.wait()


def head(x, w, keep_raw, name):
    rows, feat = x.shape
    dim = w.shape[1]
    blocks = rows // BM
    hbm = pl.BlockSpec(memory_space=pl.ANY)
    out_shape = [jax.ShapeDtypeStruct((rows, dim), BF16)]
    if keep_raw:
        out_shape.append(jax.ShapeDtypeStruct((rows, dim), F32))
    return pl.pallas_call(
        functools.partial(head_body, keep_raw=keep_raw),
        in_specs=[hbm, hbm],
        out_specs=[hbm] * len(out_shape),
        out_shape=out_shape,
        scratch_shapes=[
            pltpu.VMEM((blocks, BM, feat), BF16),
            pltpu.VMEM((feat, dim), BF16),
            pltpu.VMEM((blocks, BM, dim), BF16),
            pltpu.VMEM((blocks if keep_raw else 1, BM, dim), F32),
            pltpu.SemaphoreType.DMA((blocks + 1,)),
            pltpu.SemaphoreType.DMA((blocks, 2)),
        ],
        compiler_params=pltpu.CompilerParams(vmem_limit_bytes=62 * MIB),
        cost_estimate=cost(2 * rows * feat * dim, rows * (2 * feat + 6 * dim)),
        name=name,
    )(x, w)


def pair_terms(sc_ref, img_ref, txt_ref, di_ref, dt_ref, acc, s_scr, h_scr, imgt_scr, total_rows, home, di_init):
    step = pl.program_id(0)
    blocks = txt_ref.shape[0]
    s = scale_of(sc_ref)
    a, b, hs = s * LOG2E, sc_ref[1] * LOG2E, s * (1.0 / total_rows)
    img = img_ref[...]
    imgt_scr[...] = img.T

    def block_of(k):
        return lax.rem(step * (BM // BN) + k, blocks) if home else k

    def logits(k):
        s_scr[k % 2] = lax.dot_general(img, txt_ref[block_of(k)], NT, preferred_element_type=F32)

    def terms(k):
        zero = jnp.zeros((CR, CC), F32)
        top, prod, g_sum, gs_sum = zero, zero, zero, zero
        for r in range(0, BM, CR):
            for c in range(0, BN, CC):
                dots = s_scr[k % 2, r:r + CR, c:c + CC]
                z = dots * a + b
                pos = jnp.maximum(z, 0.0)
                t = jnp.exp2(-jnp.abs(z))
                rcp = 1.0 / (1.0 + t)
                sig = jnp.where(z >= 0, rcp, t * rcp)
                col = c + BN * k
                if home and r < col + CC and col < r + CR:
                    eye = (lax.broadcasted_iota(jnp.int32, (CR, CC), 0) + r) == (lax.broadcasted_iota(jnp.int32, (CR, CC), 1) + col)
                    sig = jnp.where(eye, -jnp.where(z >= 0, t * rcp, rcp), sig)
                    pos = jnp.where(eye, jnp.maximum(-z, 0.0), pos)
                top = top + pos
                prod = (prod + t) + prod * t
                g_sum = g_sum + sig
                gs_sum = gs_sum + sig * dots
                h_scr[k % 2, r:r + CR, c:c + CC] = (sig * hs).astype(BF16)
        acc[0] += LN2 * top + jnp.log1p(prod)
        acc[1] += gs_sum
        acc[2] += g_sum

    def grads(k):
        h = h_scr[k % 2]
        part = jnp.dot(h, txt_ref[block_of(k)], preferred_element_type=F32)
        if k == 0:
            di_ref[...] = part if di_init is None else di_init[...] + part
        else:
            di_ref[...] += part
        dt_ref[block_of(k)] += jnp.dot(imgt_scr[...], h, preferred_element_type=F32)

    logits(0)
    for k in range(blocks):
        if k + 1 < blocks:
            logits(k + 1)
        terms(k)
        grads(k)


def away_body(sc_ref, img_ref, txt_ref, di_ref, dt_ref, sums_ref, s_scr, h_scr, imgt_scr, *, total_rows):
    @pl.when(pl.program_id(0) == 0)
    def _():
        sums_ref[...] = jnp.zeros_like(sums_ref)
        dt_ref[...] = jnp.zeros_like(dt_ref)

    pair_terms(sc_ref, img_ref, txt_ref, di_ref, dt_ref, sums_ref, s_scr, h_scr, imgt_scr, total_rows, False, None)


def home_body(sc_ref, img_ref, txt_ref, raw_ref, x_ref, away_ref, sums_in, dt_ref, dw_ref, sums_ref, s_scr, h_scr, imgt_scr, di_ref, *, total_rows):
    @pl.when(pl.program_id(0) == 0)
    def _():
        sums_ref[...] = sums_in[...]
        dt_ref[...] = jnp.zeros_like(dt_ref)
        dw_ref[...] = jnp.zeros_like(dw_ref)

    pair_terms(sc_ref, img_ref, txt_ref, di_ref, dt_ref, sums_ref, s_scr, h_scr, imgt_scr, total_rows, True, away_ref)
    dw_ref[...] += lax.dot_general(x_ref[...], raw_grad(raw_ref[...], di_ref[...]), TN, preferred_element_type=F32)


def raw_grad(raw, grad_unit):
    inv = inv_norm(raw)
    unit = raw * inv
    proj = jnp.sum(unit * grad_unit, axis=1, keepdims=True)
    return (inv * (grad_unit - unit * proj)).astype(BF16)


def tile_scratch(dim):
    return [pltpu.VMEM((2, BM, BN), F32), pltpu.VMEM((2, BM, BN), BF16), pltpu.VMEM((dim, BM), BF16)]


def whole(shape, **kw):
    return pl.BlockSpec(shape, lambda i: (0,) * len(shape), **kw)


def away_tile(scal, img, txt, total_rows):
    rows, dim = img.shape
    blocks = txt.shape[0]
    once = dict(pipeline_mode=pl.Buffered(1))
    return pl.pallas_call(
        functools.partial(away_body, total_rows=total_rows),
        grid=(rows // BM,),
        in_specs=[
            pl.BlockSpec(memory_space=pltpu.SMEM),
            pl.BlockSpec((BM, dim), lambda i: (i, 0)),
            whole((blocks, BN, dim), **once),
        ],
        out_specs=[pl.BlockSpec((BM, dim), lambda i: (i, 0)), whole((blocks, dim, BN), **once), whole((3, CR, CC))],
        out_shape=[
            jax.ShapeDtypeStruct((rows, dim), F32),
            jax.ShapeDtypeStruct((blocks, dim, BN), F32),
            jax.ShapeDtypeStruct((3, CR, CC), F32),
        ],
        scratch_shapes=tile_scratch(dim),
        compiler_params=params(62),
        cost_estimate=cost(6 * rows * rows * dim, 30 * rows * dim),
        name="away_tile",
    )(scal, img, txt)


def home_tile(scal, img, txt, raw, x, away, sums, total_rows):
    rows, dim = img.shape
    feat = x.shape[1]
    blocks = txt.shape[0]
    once = dict(pipeline_mode=pl.Buffered(1))
    return pl.pallas_call(
        functools.partial(home_body, total_rows=total_rows),
        grid=(rows // BM,),
        in_specs=[
            pl.BlockSpec(memory_space=pltpu.SMEM),
            pl.BlockSpec((BM, dim), lambda i: (i, 0)),
            whole((blocks, BN, dim), **once),
            pl.BlockSpec((BM, dim), lambda i: (i, 0)),
            pl.BlockSpec((BM, feat), lambda i: (i, 0)),
            pl.BlockSpec((BM, dim), lambda i: (i, 0)),
            whole((3, CR, CC)),
        ],
        out_specs=[whole((blocks, dim, BN), **once), whole((feat, dim), **once), whole((3, CR, CC))],
        out_shape=[
            jax.ShapeDtypeStruct((blocks, dim, BN), F32),
            jax.ShapeDtypeStruct((feat, dim), F32),
            jax.ShapeDtypeStruct((3, CR, CC), F32),
        ],
        scratch_shapes=tile_scratch(dim) + [pltpu.VMEM((BM, dim), F32)],
        compiler_params=params(62),
        cost_estimate=cost(6 * rows * rows * dim, 40 * rows * dim),
        name="home_tile",
    )(scal, img, txt, raw, x, away, sums)


def all_sum(src, out, bufs, peer, coord, core, send):
    pair, r1, r2, r3, psem, ssem, rsem = bufs
    part = src.shape[1] // 3
    quart, sixt = part // 4, part // 16
    sib = peer(3, 1)
    mine = out.at[core]
    dims = [(p, (p + 1) % 3, (p + 2) % 3) for p in range(3)]
    offs = (2, 1, 3)

    def spread(phase, p, d, src_of, dst_of):
        return [send(src_of(o), dst_of(o), ssem.at[phase, p, o - 1], rsem.at[phase, p, o - 1], peer(d, o)) for o in offs]

    c0 = []
    for p in range(3):
        rows = pl.ds(part * p, part)
        c0.append(send(src.at[1 - core, rows], pair.at[rows], psem.at[0, p], psem.at[1, p], sib))
    yield
    c1 = []
    for p in range(3):
        c0[p].wait_recv()
        rows = pl.ds(part * p, part)
        pair[rows, :] = pair[rows, :] + src[core, rows, :]
        d = dims[p][0]
        c1.append(spread(0, p, d, lambda o: pair.at[pl.ds(part * p + lax.rem(coord[d] + o, 4) * quart, quart)], lambda o: r1.at[p, o - 1]))
    yield
    c2, base1 = [], []
    for p in range(3):
        for copy in c1[p]:
            copy.wait_recv()
        base = part * p + coord[dims[p][0]] * quart
        base1.append(base)
        rows = pl.ds(base, quart)
        pair[rows, :] = ((pair[rows, :] + r1[p, 0]) + r1[p, 1]) + r1[p, 2]
        d = dims[p][1]
        c2.append(spread(1, p, d, lambda o: pair.at[pl.ds(base + lax.rem(coord[d] + o, 4) * sixt, sixt)], lambda o: r2.at[p, o - 1]))
    yield
    c3, base2 = [], []
    for p in range(3):
        for copy in c2[p]:
            copy.wait_recv()
        base = base1[p] + coord[dims[p][1]] * sixt
        base2.append(base)
        d = dims[p][2]
        k = coord[d]
        r3[p, k] = ((pair[pl.ds(base, sixt), :] + r2[p, 0]) + r2[p, 1]) + r2[p, 2]
        c3.append(spread(2, p, d, lambda o: r3.at[p, k], lambda o: r3.at[p, k]))
    yield
    c4 = []
    for p in range(3):
        for copy in c3[p]:
            copy.wait_recv()
        rows = pl.ds(base2[p], sixt)
        out[core, rows, :] = ((r3[p, 0] + r3[p, 1]) + r3[p, 2]) + r3[p, 3]
        c4.append(spread(3, p, dims[p][1], lambda o: mine.at[rows], lambda o: mine.at[rows]))
    yield
    c5, c6 = [], []
    for p in range(3):
        for copy in c4[p]:
            copy.wait_recv()
        rows = pl.ds(base1[p], quart)
        c5.append(spread(4, p, dims[p][0], lambda o: mine.at[rows], lambda o: mine.at[rows]))
        c6.append(send(mine.at[rows], mine.at[rows], psem.at[2, p], psem.at[3, p], sib))
    yield
    for p in range(3):
        for i, o in enumerate(offs):
            c5[p][i].wait_recv()
            rows = pl.ds(part * p + lax.rem(coord[dims[p][0]] + 4 - o, 4) * quart, quart)
            c6.append(send(mine.at[rows], mine.at[rows], psem.at[4 + 2 * i, p], psem.at[5 + 2 * i, p], sib))
    yield
    for copy in c6:
        copy.wait_recv()
    yield


def sum_scratch(rows):
    part = rows // 3
    dma = pltpu.SemaphoreType.DMA
    return [
        pltpu.VMEM((rows, 128), F32),
        pltpu.VMEM((3, 3, part // 4, 128), F32),
        pltpu.VMEM((3, 3, part // 16, 128), F32),
        pltpu.VMEM((3, 4, part // 16, 128), F32),
        dma((10, 3)),
        dma((5, 3, 3)),
        dma((5, 3, 3)),
    ]


def finish_body(sc_ref, own_hbm, got_hbm, x_hbm, w_hbm, dwi_hbm, sums_hbm, dw_img_ref, dw_txt_ref, scal_ref, own_ref, got_ref, x_ref, w_ref, dwi_ref, sums_ref, dwt_ref, ai_ref, at_ref, oi_ref, ot_ref, sem, *bufs, total_rows):
    rep, core = lax.axis_index("rep"), lax.axis_index("data")
    coord = [lax.rem(rep, 4), lax.rem(lax.div(rep, 4), 4), lax.div(rep, 16)]
    stride = [1, 4, 16]

    def peer(dim, off):
        if dim == 3:
            return (rep, 1 - core)
        return (rep + (lax.rem(coord[dim] + off, 4) - coord[dim]) * stride[dim], core)

    bar = pltpu.get_barrier_semaphore()
    partners = [peer(3, 1)] + [peer(dim, off) for dim in range(3) for off in (1, 2, 3)]
    for dev in partners:
        pl.semaphore_signal(bar, inc=1, device_id=dev, device_id_type=MESH)

    blocks = own_ref.shape[0]
    pairs = [(dwi_hbm, dwi_ref), (w_hbm, w_ref)]
    for i in range(blocks):
        pairs += [(x_hbm.at[pl.ds(BN * i, BN)], x_ref.at[i]), (own_hbm.at[i], own_ref.at[i]), (got_hbm.at[i], got_ref.at[i])]
    arrive = fetch(pairs + [(sums_hbm, sums_ref)], sem)

    feat_i, feat_t = dwi_ref.shape[0], dwt_ref.shape[1]
    arrive[0].wait()
    for l in range(4):
        ai_ref[l // 2, pl.ds(feat_i * (l % 2), feat_i), :] = dwi_ref[:, 128 * l:128 * (l + 1)]
    pl.semaphore_wait(bar, len(partners))

    started = []

    def send(src, dst, ssem, rsem, dev):
        copy = pltpu.make_async_remote_copy(src_ref=src, dst_ref=dst, send_sem=ssem, recv_sem=rsem, device_id=dev, device_id_type=MESH)
        copy.start()
        started.append(copy)
        return copy

    img = all_sum(ai_ref, oi_ref, bufs[:7], peer, coord, core, send)
    txt = all_sum(at_ref, ot_ref, bufs[7:], peer, coord, core, send)
    next(img)
    arrive[1].wait()
    w_t = w_ref[...].T

    def block(i):
        for copy in arrive[2 + 3 * i:5 + 3 * i]:
            copy.wait()
        x = x_ref[i]
        raw = lax.dot_general(w_t, x, NT, preferred_element_type=F32)
        inv = lax.rsqrt(jnp.sum(raw * raw, axis=0, keepdims=True))
        unit = raw * inv
        grad = own_ref[i] + got_ref[i]
        proj = jnp.sum(unit * grad, axis=0, keepdims=True)
        raw_grad_t = (inv * (grad - unit * proj)).astype(BF16)
        part = jnp.dot(raw_grad_t, x, preferred_element_type=F32)
        dwt_ref[...] = part if i == 0 else dwt_ref[...] + part

    for i in range(blocks):
        block(i)
        if i == blocks // 3:
            next(img)
    for l in range(4):
        at_ref[l // 2, pl.ds(feat_t * (l % 2), feat_t), :] = dwt_ref[128 * l:128 * (l + 1), :].T
    arrive[-1].wait()
    s = scale_of(sc_ref)
    row = lax.broadcasted_iota(jnp.int32, (128, 128), 0)
    loss = jnp.sum(sums_ref[0]) / total_rows
    temp = jnp.sum(sums_ref[1]) * (s * (1.0 / total_rows))
    bias = jnp.sum(sums_ref[2]) / total_rows
    scalars = jnp.where(row == 0, loss, jnp.where(row == 1, temp, jnp.where(row == 2, bias, 0.0)))
    at_ref[0, 2 * feat_t:, :] = scalars
    at_ref[1, 2 * feat_t:, :] = jnp.zeros_like(scalars)
    next(txt)
    next(img)
    for _ in range(6):
        next(txt, None)
        next(img, None)
    next(txt, None)
    for l in range(4):
        lanes = slice(128 * l, 128 * (l + 1))
        dw_img_ref[:, lanes] = oi_ref[l // 2, pl.ds(feat_i * (l % 2), feat_i), :]
        dw_txt_ref[:, lanes] = ot_ref[l // 2, pl.ds(feat_t * (l % 2), feat_t), :]
    scal_ref[...] = ot_ref[0, 2 * feat_t:2 * feat_t + 8, :]
    for copy in started:
        copy.wait_send()


def finish(scal, own, got, x, w, dwi, sums, total_rows):
    rows, feat = x.shape
    dim = w.shape[1]
    blocks = rows // BN
    img_rows, txt_rows = 2 * dwi.shape[0], 2 * feat + 128
    hbm = pl.BlockSpec(memory_space=pl.ANY)
    vmem = pl.BlockSpec(memory_space=pltpu.VMEM)
    return pl.pallas_call(
        functools.partial(finish_body, total_rows=total_rows),
        in_specs=[pl.BlockSpec(memory_space=pltpu.SMEM)] + [hbm] * 6,
        out_specs=[vmem, vmem, vmem],
        out_shape=[jax.ShapeDtypeStruct(dwi.shape, F32), jax.ShapeDtypeStruct(w.shape, F32), jax.ShapeDtypeStruct((8, 128), F32)],
        scratch_shapes=[
            pltpu.VMEM(own.shape, F32),
            pltpu.VMEM(own.shape, F32),
            pltpu.VMEM((blocks, BN, feat), BF16),
            pltpu.VMEM(w.shape, BF16),
            pltpu.VMEM(dwi.shape, F32),
            pltpu.VMEM(sums.shape, F32),
            pltpu.VMEM((dim, feat), F32),
            pltpu.VMEM((2, img_rows, 128), F32),
            pltpu.VMEM((2, txt_rows, 128), F32),
            pltpu.VMEM((2, img_rows, 128), F32),
            pltpu.VMEM((2, txt_rows, 128), F32),
            pltpu.SemaphoreType.DMA((3 * blocks + 3,)),
        ] + sum_scratch(img_rows) + sum_scratch(txt_rows),
        compiler_params=pltpu.CompilerParams(collective_id=1, has_side_effects=True, vmem_limit_bytes=62 * MIB),
        cost_estimate=cost(1e9, 1e7),
        name="finish",
    )(scal, own, got, x, w, dwi, sums)


def solution(mesh):
    data_n, rep_n = mesh.shape["data"], mesh.shape["rep"]
    swap = [(src, (src + 1) % data_n) for src in range(data_n)]
    row_spec = P(("rep", "data"), None)

    def device_body(img_loc, txt_loc, w_img, w_txt, log_temp, logit_bias):
        rows = img_loc.shape[0]
        dim = w_img.shape[1]
        total_rows = float(rows * rep_n * data_n)
        scal = jnp.where(jnp.arange(2) == 0, log_temp, logit_bias)
        (emb_t,) = head(txt_loc, w_txt, False, "text_head")
        emb_t = emb_t.reshape(rows // BN, BN, dim)
        away_t = lax.ppermute(emb_t, "data", swap)
        emb_i, raw_i = head(img_loc, w_img, True, "image_head")
        away_di, away_dt, sums = away_tile(scal, emb_i, away_t, total_rows)
        got_dt = lax.ppermute(away_dt, "data", swap)
        own_dt, dwi, sums = home_tile(scal, emb_i, emb_t, raw_i, img_loc, away_di, sums, total_rows)
        dw_img, dw_txt, totals = finish(scal, own_dt, got_dt, txt_loc, w_txt, dwi, sums, total_rows)
        return totals[0, 0], totals[1, 0], totals[2, 0], dw_img, dw_txt

    return jax.shard_map(device_body, mesh=mesh, in_specs=(row_spec, row_spec, P(), P(), P(), P()), out_specs=(P(), P(), P(), P(), P()), check_vma=False)
```

```python
import functools

import jax
import jax.numpy as jnp
from jax import lax
from jax.experimental import pallas as pl
from jax.experimental.pallas import tpu as pltpu
from jax.sharding import PartitionSpec as P

LOG2E = 1.4426950408889634
LN2 = 0.6931471805599453
NT = (((1,), (1,)), ((), ()))
TN = (((0,), (0,)), ((), ()))
MESH = pl.DeviceIdType.MESH
F32 = jnp.float32
BF16 = jnp.bfloat16
MIB = 1024 * 1024

BM = 512
BN = 256
CR, CC = 16, 256


def inv_norm(raw):
    return lax.rsqrt(jnp.sum(raw * raw, axis=1, keepdims=True))


def params(vmem):
    return pltpu.CompilerParams(
        dimension_semantics=("arbitrary",),
        vmem_limit_bytes=vmem * MIB,
    )


def scale_of(sc_ref):
    return jnp.exp(jnp.full((8, 128), sc_ref[0], F32))[0, 0]


def cost(flops, nbytes):
    return pl.CostEstimate(flops=int(flops), bytes_accessed=int(nbytes), transcendentals=0)


def fetch(pairs, sems):
    copies = [pltpu.make_async_copy(src, dst, sems.at[i]) for i, (src, dst) in enumerate(pairs)]
    for copy in copies:
        copy.start()
    return copies


def head_body(x_hbm, w_hbm, *refs, keep_raw):
    outs, (x_ref, w_ref, emb_ref, raw_ref, in_sem, out_sem) = refs[:-6], refs[-6:]
    blocks = x_ref.shape[0]
    arrive = fetch([(w_hbm, w_ref)] + [(x_hbm.at[pl.ds(BM * i, BM)], x_ref.at[i]) for i in range(blocks)], in_sem)
    arrive[0].wait()
    leave = []

    def product(i):
        arrive[i + 1].wait()
        raw_ref[i] = jnp.dot(x_ref[i], w_ref[...], preferred_element_type=F32)

    product(0)
    for i in range(blocks):
        if i + 1 < blocks:
            product(i + 1)
        raw = raw_ref[i]
        emb_ref[i] = (raw * inv_norm(raw)).astype(BF16)
        pairs = [(emb_ref.at[i], outs[0].at[pl.ds(BM * i, BM)])]
        if keep_raw:
            pairs.append((raw_ref.at[i], outs[1].at[pl.ds(BM * i, BM)]))
        leave += fetch(pairs, out_sem.at[i])
    for copy in leave:
        copy.wait()


def head(x, w, keep_raw, name):
    rows, feat = x.shape
    dim = w.shape[1]
    blocks = rows // BM
    hbm = pl.BlockSpec(memory_space=pl.ANY)
    out_shape = [jax.ShapeDtypeStruct((rows, dim), BF16)]
    if keep_raw:
        out_shape.append(jax.ShapeDtypeStruct((rows, dim), F32))
    return pl.pallas_call(
        functools.partial(head_body, keep_raw=keep_raw),
        in_specs=[hbm, hbm],
        out_specs=[hbm] * len(out_shape),
        out_shape=out_shape,
        scratch_shapes=[
            pltpu.VMEM((blocks, BM, feat), BF16),
            pltpu.VMEM((feat, dim), BF16),
            pltpu.VMEM((blocks, BM, dim), BF16),
            pltpu.VMEM((blocks, BM, dim), F32),
            pltpu.SemaphoreType.DMA((blocks + 1,)),
            pltpu.SemaphoreType.DMA((blocks, 2)),
        ],
        compiler_params=pltpu.CompilerParams(vmem_limit_bytes=62 * MIB),
        cost_estimate=cost(2 * rows * feat * dim, rows * (2 * feat + 6 * dim)),
        name=name,
    )(x, w)


def pair_terms(sc_ref, img_ref, txt_ref, di_ref, dt_ref, acc, s_scr, h_scr, imgt_scr, total_rows, home, di_init):
    step = pl.program_id(0)
    blocks = txt_ref.shape[0]
    s = scale_of(sc_ref)
    a, b, hs = s * LOG2E, sc_ref[1] * LOG2E, s * (1.0 / total_rows)
    img = img_ref[...]
    imgt_scr[...] = img.T

    def block_of(k):
        return lax.rem(step * (BM // BN) + k, blocks) if home else k

    def logits(k):
        s_scr[k % 2] = lax.dot_general(img, txt_ref[block_of(k)], NT, preferred_element_type=F32)

    def terms(k):
        zero = jnp.zeros((CR, CC), F32)
        top, prod, g_sum, gs_sum = zero, zero, zero, zero
        for r in range(0, BM, CR):
            for c in range(0, BN, CC):
                dots = s_scr[k % 2, r:r + CR, c:c + CC]
                z = dots * a + b
                pos = jnp.maximum(z, 0.0)
                t = jnp.exp2(-jnp.abs(z))
                rcp = 1.0 / (1.0 + t)
                sig = jnp.where(z >= 0, rcp, t * rcp)
                col = c + BN * k
                if home and r < col + CC and col < r + CR:
                    eye = (lax.broadcasted_iota(jnp.int32, (CR, CC), 0) + r) == (lax.broadcasted_iota(jnp.int32, (CR, CC), 1) + col)
                    sig = jnp.where(eye, -jnp.where(z >= 0, t * rcp, rcp), sig)
                    pos = jnp.where(eye, jnp.maximum(-z, 0.0), pos)
                top = top + pos
                prod = (prod + t) + prod * t
                g_sum = g_sum + sig
                gs_sum = gs_sum + sig * dots
                h_scr[k % 2, r:r + CR, c:c + CC] = (sig * hs).astype(BF16)
        acc[0] += LN2 * top + jnp.log1p(prod)
        acc[1] += gs_sum
        acc[2] += g_sum

    def grads(k):
        h = h_scr[k % 2]
        part = jnp.dot(h, txt_ref[block_of(k)], preferred_element_type=F32)
        if k == 0:
            di_ref[...] = part if di_init is None else di_init[...] + part
        else:
            di_ref[...] += part
        dt_ref[block_of(k)] += jnp.dot(imgt_scr[...], h, preferred_element_type=F32)

    logits(0)
    for k in range(blocks):
        if k + 1 < blocks:
            logits(k + 1)
        terms(k)
        grads(k)


def away_body(sc_ref, img_ref, txt_ref, di_ref, dt_ref, sums_ref, s_scr, h_scr, imgt_scr, *, total_rows):
    @pl.when(pl.program_id(0) == 0)
    def _():
        sums_ref[...] = jnp.zeros_like(sums_ref)
        dt_ref[...] = jnp.zeros_like(dt_ref)

    pair_terms(sc_ref, img_ref, txt_ref, di_ref, dt_ref, sums_ref, s_scr, h_scr, imgt_scr, total_rows, False, None)


def home_body(sc_ref, img_ref, txt_ref, raw_ref, x_ref, away_ref, sums_in, dt_ref, dw_ref, sums_ref, s_scr, h_scr, imgt_scr, di_ref, *, total_rows):
    @pl.when(pl.program_id(0) == 0)
    def _():
        sums_ref[...] = sums_in[...]
        dt_ref[...] = jnp.zeros_like(dt_ref)
        dw_ref[...] = jnp.zeros_like(dw_ref)

    pair_terms(sc_ref, img_ref, txt_ref, di_ref, dt_ref, sums_ref, s_scr, h_scr, imgt_scr, total_rows, True, away_ref)
    dw_ref[...] += lax.dot_general(x_ref[...], raw_grad(raw_ref[...], di_ref[...]), TN, preferred_element_type=F32)


def raw_grad(raw, grad_unit):
    inv = inv_norm(raw)
    unit = raw * inv
    proj = jnp.sum(unit * grad_unit, axis=1, keepdims=True)
    return (inv * (grad_unit - unit * proj)).astype(BF16)


def tile_scratch(dim):
    return [pltpu.VMEM((2, BM, BN), F32), pltpu.VMEM((2, BM, BN), BF16), pltpu.VMEM((dim, BM), BF16)]


def whole(shape, **kw):
    return pl.BlockSpec(shape, lambda i: (0,) * len(shape), **kw)


def away_tile(scal, img, txt, total_rows):
    rows, dim = img.shape
    blocks = txt.shape[0]
    once = dict(pipeline_mode=pl.Buffered(1))
    return pl.pallas_call(
        functools.partial(away_body, total_rows=total_rows),
        grid=(rows // BM,),
        in_specs=[
            pl.BlockSpec(memory_space=pltpu.SMEM),
            pl.BlockSpec((BM, dim), lambda i: (i, 0)),
            whole((blocks, BN, dim), **once),
        ],
        out_specs=[pl.BlockSpec((BM, dim), lambda i: (i, 0)), whole((blocks, dim, BN), **once), whole((3, CR, CC))],
        out_shape=[
            jax.ShapeDtypeStruct((rows, dim), F32),
            jax.ShapeDtypeStruct((blocks, dim, BN), F32),
            jax.ShapeDtypeStruct((3, CR, CC), F32),
        ],
        scratch_shapes=tile_scratch(dim),
        compiler_params=params(62),
        cost_estimate=cost(6 * rows * rows * dim, 30 * rows * dim),
        name="away_tile",
    )(scal, img, txt)


def home_tile(scal, img, txt, raw, x, away, sums, total_rows):
    rows, dim = img.shape
    feat = x.shape[1]
    blocks = txt.shape[0]
    once = dict(pipeline_mode=pl.Buffered(1))
    return pl.pallas_call(
        functools.partial(home_body, total_rows=total_rows),
        grid=(rows // BM,),
        in_specs=[
            pl.BlockSpec(memory_space=pltpu.SMEM),
            pl.BlockSpec((BM, dim), lambda i: (i, 0)),
            whole((blocks, BN, dim), **once),
            pl.BlockSpec((BM, dim), lambda i: (i, 0)),
            pl.BlockSpec((BM, feat), lambda i: (i, 0)),
            pl.BlockSpec((BM, dim), lambda i: (i, 0)),
            whole((3, CR, CC)),
        ],
        out_specs=[whole((blocks, dim, BN), **once), whole((feat, dim), **once), whole((3, CR, CC))],
        out_shape=[
            jax.ShapeDtypeStruct((blocks, dim, BN), F32),
            jax.ShapeDtypeStruct((feat, dim), F32),
            jax.ShapeDtypeStruct((3, CR, CC), F32),
        ],
        scratch_shapes=tile_scratch(dim) + [pltpu.VMEM((BM, dim), F32)],
        compiler_params=params(62),
        cost_estimate=cost(6 * rows * rows * dim, 40 * rows * dim),
        name="home_tile",
    )(scal, img, txt, raw, x, away, sums)


def all_sum(src, out, bufs, peer, coord, core, send):
    pair, r1, r2, r3, psem, ssem, rsem = bufs
    part = src.shape[1] // 3
    quart, sixt = part // 4, part // 16
    sib = peer(3, 1)
    mine = out.at[core]
    dims = [(p, (p + 1) % 3, (p + 2) % 3) for p in range(3)]
    offs = (2, 1, 3)

    def spread(phase, p, d, src_of, dst_of):
        return [send(src_of(o), dst_of(o), ssem.at[phase, p, o - 1], rsem.at[phase, p, o - 1], peer(d, o)) for o in offs]

    c0 = []
    for p in range(3):
        rows = pl.ds(part * p, part)
        c0.append(send(src.at[1 - core, rows], pair.at[rows], psem.at[0, p], psem.at[1, p], sib))
    yield
    c1 = []
    for p in range(3):
        c0[p].wait_recv()
        rows = pl.ds(part * p, part)
        pair[rows, :] = pair[rows, :] + src[core, rows, :]
        d = dims[p][0]
        c1.append(spread(0, p, d, lambda o: pair.at[pl.ds(part * p + lax.rem(coord[d] + o, 4) * quart, quart)], lambda o: r1.at[p, o - 1]))
    yield
    c2, base1 = [], []
    for p in range(3):
        for copy in c1[p]:
            copy.wait_recv()
        base = part * p + coord[dims[p][0]] * quart
        base1.append(base)
        rows = pl.ds(base, quart)
        pair[rows, :] = ((pair[rows, :] + r1[p, 0]) + r1[p, 1]) + r1[p, 2]
        d = dims[p][1]
        c2.append(spread(1, p, d, lambda o: pair.at[pl.ds(base + lax.rem(coord[d] + o, 4) * sixt, sixt)], lambda o: r2.at[p, o - 1]))
    yield
    c3, base2 = [], []
    for p in range(3):
        for copy in c2[p]:
            copy.wait_recv()
        base = base1[p] + coord[dims[p][1]] * sixt
        base2.append(base)
        d = dims[p][2]
        k = coord[d]
        r3[p, k] = ((pair[pl.ds(base, sixt), :] + r2[p, 0]) + r2[p, 1]) + r2[p, 2]
        c3.append(spread(2, p, d, lambda o: r3.at[p, k], lambda o: r3.at[p, k]))
    yield
    c4 = []
    for p in range(3):
        for copy in c3[p]:
            copy.wait_recv()
        rows = pl.ds(base2[p], sixt)
        out[core, rows, :] = ((r3[p, 0] + r3[p, 1]) + r3[p, 2]) + r3[p, 3]
        c4.append(spread(3, p, dims[p][1], lambda o: mine.at[rows], lambda o: mine.at[rows]))
    yield
    c5, c6 = [], []
    for p in range(3):
        for copy in c4[p]:
            copy.wait_recv()
        rows = pl.ds(base1[p], quart)
        c5.append(spread(4, p, dims[p][0], lambda o: mine.at[rows], lambda o: mine.at[rows]))
        c6.append(send(mine.at[rows], mine.at[rows], psem.at[2, p], psem.at[3, p], sib))
    yield
    for p in range(3):
        for i, o in enumerate(offs):
            c5[p][i].wait_recv()
            rows = pl.ds(part * p + lax.rem(coord[dims[p][0]] + 4 - o, 4) * quart, quart)
            c6.append(send(mine.at[rows], mine.at[rows], psem.at[4 + 2 * i, p], psem.at[5 + 2 * i, p], sib))
    yield
    for copy in c6:
        copy.wait_recv()
    yield


def sum_scratch(rows):
    part = rows // 3
    dma = pltpu.SemaphoreType.DMA
    return [
        pltpu.VMEM((rows, 128), F32),
        pltpu.VMEM((3, 3, part // 4, 128), F32),
        pltpu.VMEM((3, 3, part // 16, 128), F32),
        pltpu.VMEM((3, 4, part // 16, 128), F32),
        dma((10, 3)),
        dma((5, 3, 3)),
        dma((5, 3, 3)),
    ]


def finish_body(sc_ref, own_hbm, got_hbm, x_hbm, w_hbm, dwi_hbm, sums_hbm, oi_ref, txt_ref, scal_ref, own_ref, got_ref, x_ref, w_ref, dwi_ref, sums_ref, raw_ref, dwt_ref, ai_ref, at_ref, ot_ref, sem, *bufs, total_rows):
    rep, core = lax.axis_index("rep"), lax.axis_index("data")
    coord = [lax.rem(rep, 4), lax.rem(lax.div(rep, 4), 4), lax.div(rep, 16)]
    stride = [1, 4, 16]

    def peer(dim, off):
        if dim == 3:
            return (rep, 1 - core)
        return (rep + (lax.rem(coord[dim] + off, 4) - coord[dim]) * stride[dim], core)

    bar = pltpu.get_barrier_semaphore()
    partners = [peer(3, 1)] + [peer(dim, off) for dim in range(3) for off in (1, 2, 3)]
    for dev in partners:
        pl.semaphore_signal(bar, inc=1, device_id=dev, device_id_type=MESH)

    blocks = x_ref.shape[0]
    cols = BM // BN
    pairs = [(dwi_hbm, dwi_ref), (w_hbm, w_ref)]
    for i in range(blocks):
        part = pl.ds(cols * i, cols)
        pairs += [(x_hbm.at[pl.ds(BM * i, BM)], x_ref.at[i]), (own_hbm.at[part], own_ref.at[part]), (got_hbm.at[part], got_ref.at[part])]
    arrive = fetch(pairs + [(sums_hbm, sums_ref)], sem)

    feat_i, feat_t = dwi_ref.shape[0], dwt_ref.shape[1]
    arrive[0].wait()
    for l in range(4):
        ai_ref[l // 2, pl.ds(feat_i * (l % 2), feat_i), :] = dwi_ref[:, 128 * l:128 * (l + 1)]
    pl.semaphore_wait(bar, len(partners))

    started = []

    def send(src, dst, ssem, rsem, dev):
        copy = pltpu.make_async_remote_copy(src_ref=src, dst_ref=dst, send_sem=ssem, recv_sem=rsem, device_id=dev, device_id_type=MESH)
        copy.start()
        started.append(copy)
        return copy

    img = all_sum(ai_ref, oi_ref, bufs[:7], peer, coord, core, send)
    txt = all_sum(at_ref, ot_ref, bufs[7:], peer, coord, core, send)
    next(img)
    arrive[1].wait()
    w_t = w_ref[...].T

    def product(i):
        arrive[2 + 3 * i].wait()
        raw_ref[i % 2] = lax.dot_general(w_t, x_ref[i], NT, preferred_element_type=F32)

    def block(i):
        for copy in arrive[3 + 3 * i:5 + 3 * i]:
            copy.wait()
        raw = raw_ref[i % 2]
        inv = lax.rsqrt(jnp.sum(raw * raw, axis=0, keepdims=True))
        unit = raw * inv
        grad = jnp.concatenate([own_ref[cols * i + j] + got_ref[cols * i + j] for j in range(cols)], axis=1)
        proj = jnp.sum(unit * grad, axis=0, keepdims=True)
        raw_grad_t = (inv * (grad - unit * proj)).astype(BF16)
        part = jnp.dot(raw_grad_t, x_ref[i], preferred_element_type=F32)
        dwt_ref[...] = part if i == 0 else dwt_ref[...] + part

    product(0)
    for i in range(blocks):
        if i + 1 < blocks:
            product(i + 1)
        block(i)
        if i == 1:
            next(img)
    for l in range(4):
        at_ref[l // 2, pl.ds(feat_t * (l % 2), feat_t), :] = dwt_ref[128 * l:128 * (l + 1), :].T
    arrive[-1].wait()
    s = scale_of(sc_ref)
    row = lax.broadcasted_iota(jnp.int32, (128, 128), 0)
    loss = jnp.sum(sums_ref[0]) / total_rows
    temp = jnp.sum(sums_ref[1]) * (s * (1.0 / total_rows))
    bias = jnp.sum(sums_ref[2]) / total_rows
    scalars = jnp.where(row == 0, loss, jnp.where(row == 1, temp, jnp.where(row == 2, bias, 0.0)))
    at_ref[0, 2 * feat_t:, :] = scalars
    at_ref[1, 2 * feat_t:, :] = jnp.zeros_like(scalars)
    next(txt)
    next(img)
    for _ in range(6):
        next(txt, None)
        next(img, None)
    next(txt, None)
    txt_ref[...] = ot_ref[:, :2 * feat_t, :]
    scal_ref[...] = ot_ref[0, 2 * feat_t:2 * feat_t + 8, :]
    for copy in started:
        copy.wait_send()


def finish(scal, own, got, x, w, dwi, sums, total_rows):
    rows, feat = x.shape
    dim = w.shape[1]
    blocks = rows // BM
    img_rows, txt_rows = 2 * dwi.shape[0], 2 * feat + 128
    hbm = pl.BlockSpec(memory_space=pl.ANY)
    vmem = pl.BlockSpec(memory_space=pltpu.VMEM)
    return pl.pallas_call(
        functools.partial(finish_body, total_rows=total_rows),
        in_specs=[pl.BlockSpec(memory_space=pltpu.SMEM)] + [hbm] * 6,
        out_specs=[vmem, vmem, vmem],
        out_shape=[
            jax.ShapeDtypeStruct((2, img_rows, 128), F32),
            jax.ShapeDtypeStruct((2, 2 * feat, 128), F32),
            jax.ShapeDtypeStruct((8, 128), F32),
        ],
        scratch_shapes=[
            pltpu.VMEM(own.shape, F32),
            pltpu.VMEM(own.shape, F32),
            pltpu.VMEM((blocks, BM, feat), BF16),
            pltpu.VMEM(w.shape, BF16),
            pltpu.VMEM(dwi.shape, F32),
            pltpu.VMEM(sums.shape, F32),
            pltpu.VMEM((2, dim, BM), F32),
            pltpu.VMEM((dim, feat), F32),
            pltpu.VMEM((2, img_rows, 128), F32),
            pltpu.VMEM((2, txt_rows, 128), F32),
            pltpu.VMEM((2, txt_rows, 128), F32),
            pltpu.SemaphoreType.DMA((3 * blocks + 3,)),
        ] + sum_scratch(img_rows) + sum_scratch(txt_rows),
        compiler_params=pltpu.CompilerParams(collective_id=1, has_side_effects=True, vmem_limit_bytes=62 * MIB),
        cost_estimate=cost(1e9, 1e7),
        name="finish",
    )(scal, own, got, x, w, dwi, sums)


def solution(mesh):
    data_n, rep_n = mesh.shape["data"], mesh.shape["rep"]
    swap = [(src, (src + 1) % data_n) for src in range(data_n)]
    row_spec = P(("rep", "data"), None)

    def device_body(img_loc, txt_loc, w_img, w_txt, log_temp, logit_bias):
        rows = img_loc.shape[0]
        dim = w_img.shape[1]
        total_rows = float(rows * rep_n * data_n)
        scal = jnp.where(jnp.arange(2) == 0, log_temp, logit_bias)
        (emb_t,) = head(txt_loc, w_txt, False, "text_head")
        emb_t = emb_t.reshape(rows // BN, BN, dim)
        away_t = lax.ppermute(emb_t, "data", swap)
        emb_i, raw_i = head(img_loc, w_img, True, "image_head")
        away_di, away_dt, sums = away_tile(scal, emb_i, away_t, total_rows)
        got_dt = lax.ppermute(away_dt, "data", swap)
        own_dt, dwi, sums = home_tile(scal, emb_i, emb_t, raw_i, img_loc, away_di, sums, total_rows)
        img_sum, txt_sum, totals = finish(scal, own_dt, got_dt, txt_loc, w_txt, dwi, sums, total_rows)
        dw_img = img_sum.reshape(4, -1, 128).transpose(1, 0, 2).reshape(-1, dim)
        dw_txt = txt_sum.reshape(4, -1, 128).transpose(1, 0, 2).reshape(-1, dim)
        return totals[0, 0], totals[1, 0], totals[2, 0], dw_img, dw_txt

    return jax.shard_map(device_body, mesh=mesh, in_specs=(row_spec, row_spec, P(), P(), P(), P()), out_specs=(P(), P(), P(), P(), P()), check_vma=False)
```

```python
import functools

import jax
import jax.numpy as jnp
from jax import lax
from jax.experimental import pallas as pl
from jax.experimental.pallas import tpu as pltpu
from jax.sharding import PartitionSpec as P

LOG2E = 1.4426950408889634
LN2 = 0.6931471805599453
NT = (((1,), (1,)), ((), ()))
TN = (((0,), (0,)), ((), ()))
MESH = pl.DeviceIdType.MESH
F32 = jnp.float32
BF16 = jnp.bfloat16
MIB = 1024 * 1024

BM = 512
BN = 256
CR, CC = 16, 256


def inv_norm(raw):
    return lax.rsqrt(jnp.sum(raw * raw, axis=1, keepdims=True))


def params(vmem, **more):
    return pltpu.CompilerParams(
        dimension_semantics=("arbitrary",),
        vmem_limit_bytes=vmem * MIB,
        **more,
    )


def scale_of(sc_ref):
    return jnp.exp(jnp.full((8, 128), sc_ref[0], F32))[0, 0]


def cost(flops, nbytes):
    return pl.CostEstimate(flops=int(flops), bytes_accessed=int(nbytes), transcendentals=0)


def fetch(pairs, sems):
    copies = [pltpu.make_async_copy(src, dst, sems.at[i]) for i, (src, dst) in enumerate(pairs)]
    for copy in copies:
        copy.start()
    return copies


def head_body(x_hbm, w_hbm, *refs, keep_raw):
    outs, (x_ref, w_ref, emb_ref, raw_ref, in_sem, out_sem) = refs[:-6], refs[-6:]
    blocks = x_ref.shape[0]
    arrive = fetch([(w_hbm, w_ref)] + [(x_hbm.at[pl.ds(BM * i, BM)], x_ref.at[i]) for i in range(blocks)], in_sem)
    arrive[0].wait()
    leave = []

    def product(i):
        arrive[i + 1].wait()
        raw_ref[i] = jnp.dot(x_ref[i], w_ref[...], preferred_element_type=F32)

    product(0)
    for i in range(blocks):
        if i + 1 < blocks:
            product(i + 1)
        raw = raw_ref[i]
        emb_ref[i] = (raw * inv_norm(raw)).astype(BF16)
        pairs = [(emb_ref.at[i], outs[0].at[pl.ds(BM * i, BM)])]
        if keep_raw:
            pairs.append((raw_ref.at[i], outs[1].at[pl.ds(BM * i, BM)]))
        leave += fetch(pairs, out_sem.at[i])
    for copy in leave:
        copy.wait()


def head(x, w, keep_raw, name):
    rows, feat = x.shape
    dim = w.shape[1]
    blocks = rows // BM
    hbm = pl.BlockSpec(memory_space=pl.ANY)
    out_shape = [jax.ShapeDtypeStruct((rows, dim), BF16)]
    if keep_raw:
        out_shape.append(jax.ShapeDtypeStruct((rows, dim), F32))
    return pl.pallas_call(
        functools.partial(head_body, keep_raw=keep_raw),
        in_specs=[hbm, hbm],
        out_specs=[hbm] * len(out_shape),
        out_shape=out_shape,
        scratch_shapes=[
            pltpu.VMEM((blocks, BM, feat), BF16),
            pltpu.VMEM((feat, dim), BF16),
            pltpu.VMEM((blocks, BM, dim), BF16),
            pltpu.VMEM((blocks, BM, dim), F32),
            pltpu.SemaphoreType.DMA((blocks + 1,)),
            pltpu.SemaphoreType.DMA((blocks, 2)),
        ],
        compiler_params=pltpu.CompilerParams(vmem_limit_bytes=62 * MIB),
        cost_estimate=cost(2 * rows * feat * dim, rows * (2 * feat + 6 * dim)),
        name=name,
    )(x, w)


def pair_terms(sc_ref, img_ref, txt_ref, di_ref, dt_ref, acc, s_scr, h_scr, imgt_scr, total_rows, home, di_init):
    step = pl.program_id(0)
    blocks = txt_ref.shape[0]
    s = scale_of(sc_ref)
    a, b, hs = s * LOG2E, sc_ref[1] * LOG2E, s * (1.0 / total_rows)
    img = img_ref[...]
    imgt_scr[...] = img.T

    def block_of(k):
        return lax.rem(step * (BM // BN) + k, blocks) if home else k

    def logits(k):
        s_scr[k % 2] = lax.dot_general(img, txt_ref[block_of(k)], NT, preferred_element_type=F32)

    def terms(k):
        zero = jnp.zeros((CR, CC), F32)
        top, prod, g_sum, gs_sum = zero, zero, zero, zero
        for r in range(0, BM, CR):
            for c in range(0, BN, CC):
                dots = s_scr[k % 2, r:r + CR, c:c + CC]
                z = dots * a + b
                pos = jnp.maximum(z, 0.0)
                t = jnp.exp2(-jnp.abs(z))
                rcp = 1.0 / (1.0 + t)
                sig = jnp.where(z >= 0, rcp, t * rcp)
                col = c + BN * k
                if home and r < col + CC and col < r + CR:
                    eye = (lax.broadcasted_iota(jnp.int32, (CR, CC), 0) + r) == (lax.broadcasted_iota(jnp.int32, (CR, CC), 1) + col)
                    sig = jnp.where(eye, -jnp.where(z >= 0, t * rcp, rcp), sig)
                    pos = jnp.where(eye, jnp.maximum(-z, 0.0), pos)
                top = top + pos
                prod = (prod + t) + prod * t
                g_sum = g_sum + sig
                gs_sum = gs_sum + sig * dots
                h_scr[k % 2, r:r + CR, c:c + CC] = (sig * hs).astype(BF16)
        acc[0] += LN2 * top + jnp.log1p(prod)
        acc[1] += gs_sum
        acc[2] += g_sum

    def grads(k):
        h = h_scr[k % 2]
        part = jnp.dot(h, txt_ref[block_of(k)], preferred_element_type=F32)
        if k == 0:
            di_ref[...] = part if di_init is None else di_init[...] + part
        else:
            di_ref[...] += part
        dt_ref[block_of(k)] += jnp.dot(imgt_scr[...], h, preferred_element_type=F32)

    logits(0)
    for k in range(blocks):
        if k + 1 < blocks:
            logits(k + 1)
        terms(k)
        grads(k)


def away_body(sc_ref, img_ref, txt_ref, di_ref, dt_ref, sums_ref, s_scr, h_scr, imgt_scr, *, total_rows):
    @pl.when(pl.program_id(0) == 0)
    def _():
        sums_ref[...] = jnp.zeros_like(sums_ref)
        dt_ref[...] = jnp.zeros_like(dt_ref)

    pair_terms(sc_ref, img_ref, txt_ref, di_ref, dt_ref, sums_ref, s_scr, h_scr, imgt_scr, total_rows, False, None)


def raw_grad(raw, grad_unit):
    inv = inv_norm(raw)
    unit = raw * inv
    proj = jnp.sum(unit * grad_unit, axis=1, keepdims=True)
    return (inv * (grad_unit - unit * proj)).astype(BF16)


def tile_scratch(dim):
    return [pltpu.VMEM((2, BM, BN), F32), pltpu.VMEM((2, BM, BN), BF16), pltpu.VMEM((dim, BM), BF16)]


def whole(shape, **kw):
    return pl.BlockSpec(shape, lambda i: (0,) * len(shape), **kw)


def away_tile(scal, img, txt, total_rows):
    rows, dim = img.shape
    blocks = txt.shape[0]
    once = dict(pipeline_mode=pl.Buffered(1))
    return pl.pallas_call(
        functools.partial(away_body, total_rows=total_rows),
        grid=(rows // BM,),
        in_specs=[
            pl.BlockSpec(memory_space=pltpu.SMEM),
            pl.BlockSpec((BM, dim), lambda i: (i, 0)),
            whole((blocks, BN, dim), **once),
        ],
        out_specs=[pl.BlockSpec((BM, dim), lambda i: (i, 0)), whole((blocks, dim, BN), **once), whole((3, CR, CC))],
        out_shape=[
            jax.ShapeDtypeStruct((rows, dim), F32),
            jax.ShapeDtypeStruct((blocks, dim, BN), F32),
            jax.ShapeDtypeStruct((3, CR, CC), F32),
        ],
        scratch_shapes=tile_scratch(dim),
        compiler_params=params(62),
        cost_estimate=cost(6 * rows * rows * dim, 30 * rows * dim),
        name="away_tile",
    )(scal, img, txt)


def all_sum(src, out, bufs, peer, coord, core, send):
    pair, r1, r2, r3, psem, ssem, rsem = bufs
    part = src.shape[1] // 3
    quart, sixt = part // 4, part // 16
    sib = peer(3, 1)
    mine = out.at[core]
    dims = [(p, (p + 1) % 3, (p + 2) % 3) for p in range(3)]
    offs = (2, 1, 3)

    def spread(phase, p, d, src_of, dst_of):
        return [send(src_of(o), dst_of(o), ssem.at[phase, p, o - 1], rsem.at[phase, p, o - 1], peer(d, o)) for o in offs]

    c0 = []
    for p in range(3):
        rows = pl.ds(part * p, part)
        c0.append(send(src.at[1 - core, rows], pair.at[rows], psem.at[0, p], psem.at[1, p], sib))
    yield
    c1 = []
    for p in range(3):
        c0[p].wait_recv()
        rows = pl.ds(part * p, part)
        pair[rows, :] = pair[rows, :] + src[core, rows, :]
        d = dims[p][0]
        c1.append(spread(0, p, d, lambda o: pair.at[pl.ds(part * p + lax.rem(coord[d] + o, 4) * quart, quart)], lambda o: r1.at[p, o - 1]))
    yield
    c2, base1 = [], []
    for p in range(3):
        for copy in c1[p]:
            copy.wait_recv()
        base = part * p + coord[dims[p][0]] * quart
        base1.append(base)
        rows = pl.ds(base, quart)
        pair[rows, :] = ((pair[rows, :] + r1[p, 0]) + r1[p, 1]) + r1[p, 2]
        d = dims[p][1]
        c2.append(spread(1, p, d, lambda o: pair.at[pl.ds(base + lax.rem(coord[d] + o, 4) * sixt, sixt)], lambda o: r2.at[p, o - 1]))
    yield
    c3, base2 = [], []
    for p in range(3):
        for copy in c2[p]:
            copy.wait_recv()
        base = base1[p] + coord[dims[p][1]] * sixt
        base2.append(base)
        d = dims[p][2]
        k = coord[d]
        r3[p, k] = ((pair[pl.ds(base, sixt), :] + r2[p, 0]) + r2[p, 1]) + r2[p, 2]
        c3.append(spread(2, p, d, lambda o: r3.at[p, k], lambda o: r3.at[p, k]))
    yield
    c4 = []
    for p in range(3):
        for copy in c3[p]:
            copy.wait_recv()
        rows = pl.ds(base2[p], sixt)
        out[core, rows, :] = ((r3[p, 0] + r3[p, 1]) + r3[p, 2]) + r3[p, 3]
        c4.append(spread(3, p, dims[p][1], lambda o: mine.at[rows], lambda o: mine.at[rows]))
    yield
    c5, c6 = [], []
    for p in range(3):
        for copy in c4[p]:
            copy.wait_recv()
        rows = pl.ds(base1[p], quart)
        c5.append(spread(4, p, dims[p][0], lambda o: mine.at[rows], lambda o: mine.at[rows]))
        c6.append(send(mine.at[rows], mine.at[rows], psem.at[2, p], psem.at[3, p], sib))
    yield
    for p in range(3):
        for i, o in enumerate(offs):
            c5[p][i].wait_recv()
            rows = pl.ds(part * p + lax.rem(coord[dims[p][0]] + 4 - o, 4) * quart, quart)
            c6.append(send(mine.at[rows], mine.at[rows], psem.at[4 + 2 * i, p], psem.at[5 + 2 * i, p], sib))
    yield
    for copy in c6:
        copy.wait_recv()
    yield


def sum_scratch(rows):
    part = rows // 3
    dma = pltpu.SemaphoreType.DMA
    return [
        pltpu.VMEM((rows, 128), F32),
        pltpu.VMEM((3, 3, part // 4, 128), F32),
        pltpu.VMEM((3, 3, part // 16, 128), F32),
        pltpu.VMEM((3, 4, part // 16, 128), F32),
        dma((10, 3)),
        dma((5, 3, 3)),
        dma((5, 3, 3)),
    ]


def home_body(
    sc_ref, img_ref, txt_ref, raw_ref, x_ref, away_ref, sums_in, away_dt, xt_hbm, wt_hbm,
    img_out, txt_out, scal_out,
    s_scr, h_scr, imgt_scr, di_ref, dt_ref, dw_ref, sums_ref, got_ref, xt_ref, wt_ref, rawt_ref, dwt_ref, ai_ref, at_ref, oi_ref, ot_ref, sem, gsem, *bufs,
    total_rows,
):
    step = pl.program_id(0)
    rep, core = lax.axis_index("rep"), lax.axis_index("data")
    coord = [lax.rem(rep, 4), lax.rem(lax.div(rep, 4), 4), lax.div(rep, 16)]
    stride = [1, 4, 16]

    def peer(dim, off):
        if dim == 3:
            return (rep, 1 - core)
        return (rep + (lax.rem(coord[dim] + off, 4) - coord[dim]) * stride[dim], core)

    def remote(src, dst, ssem, rsem, dev):
        return pltpu.make_async_remote_copy(src_ref=src, dst_ref=dst, send_sem=ssem, recv_sem=rsem, device_id=dev, device_id_type=MESH)

    partners = [peer(3, 1)] + [peer(dim, off) for dim in range(3) for off in (1, 2, 3)]
    blocks = xt_ref.shape[0]
    cols = BM // BN
    local = [pltpu.make_async_copy(wt_hbm, wt_ref, sem.at[0])]
    local += [pltpu.make_async_copy(xt_hbm.at[pl.ds(BM * i, BM)], xt_ref.at[i], sem.at[i + 1]) for i in range(blocks)]
    swap = remote(away_dt, got_ref, gsem.at[0], gsem.at[1], peer(3, 1))

    @pl.when(step == 0)
    def _():
        for dev in partners:
            pl.semaphore_signal(pltpu.get_barrier_semaphore(), inc=1, device_id=dev, device_id_type=MESH)
        for copy in local:
            copy.start()
        sums_ref[...] = sums_in[...]
        dt_ref[...] = jnp.zeros_like(dt_ref)
        dw_ref[...] = jnp.zeros_like(dw_ref)

    @pl.when(step == 1)
    def _():
        pl.semaphore_wait(pltpu.get_barrier_semaphore(), len(partners))
        swap.start()

    pair_terms(sc_ref, img_ref, txt_ref, di_ref, dt_ref, sums_ref, s_scr, h_scr, imgt_scr, total_rows, True, away_ref)
    dw_ref[...] += lax.dot_general(x_ref[...], raw_grad(raw_ref[...], di_ref[...]), TN, preferred_element_type=F32)

    @pl.when(step == pl.num_programs(0) - 1)
    def _():
        started = []

        def send(*args):
            copy = remote(*args)
            copy.start()
            started.append(copy)
            return copy

        feat_i, feat_t = dw_ref.shape[0], dwt_ref.shape[1]
        for l in range(4):
            ai_ref[l // 2, pl.ds(feat_i * (l % 2), feat_i), :] = dw_ref[:, 128 * l:128 * (l + 1)]
        img = all_sum(ai_ref, oi_ref, bufs[:7], peer, coord, core, send)
        txt = all_sum(at_ref, ot_ref, bufs[7:], peer, coord, core, send)
        next(img)
        for copy in local:
            copy.wait()
        swap.wait()
        w_t = wt_ref[...].T

        def product(i):
            rawt_ref[i % 2] = lax.dot_general(w_t, xt_ref[i], NT, preferred_element_type=F32)

        def block(i):
            raw = rawt_ref[i % 2]
            inv = lax.rsqrt(jnp.sum(raw * raw, axis=0, keepdims=True))
            unit = raw * inv
            grad = jnp.concatenate([dt_ref[cols * i + j] + got_ref[cols * i + j] for j in range(cols)], axis=1)
            proj = jnp.sum(unit * grad, axis=0, keepdims=True)
            raw_grad_t = (inv * (grad - unit * proj)).astype(BF16)
            part = jnp.dot(raw_grad_t, xt_ref[i], preferred_element_type=F32)
            dwt_ref[...] = part if i == 0 else dwt_ref[...] + part

        product(0)
        for i in range(blocks):
            if i + 1 < blocks:
                product(i + 1)
            block(i)
            if i == 2:
                next(img)
        for l in range(4):
            at_ref[l // 2, pl.ds(feat_t * (l % 2), feat_t), :] = dwt_ref[128 * l:128 * (l + 1), :].T
        s = scale_of(sc_ref)
        row = lax.broadcasted_iota(jnp.int32, (128, 128), 0)
        loss = jnp.sum(sums_ref[0]) / total_rows
        temp = jnp.sum(sums_ref[1]) * (s * (1.0 / total_rows))
        bias = jnp.sum(sums_ref[2]) / total_rows
        scalars = jnp.where(row == 0, loss, jnp.where(row == 1, temp, jnp.where(row == 2, bias, 0.0)))
        at_ref[0, 2 * feat_t:, :] = scalars
        at_ref[1, 2 * feat_t:, :] = jnp.zeros_like(scalars)
        next(txt)
        next(txt)
        next(img)
        for _ in range(6):
            next(txt, None)
            next(img, None)
        img_out[...] = oi_ref[...]
        txt_out[...] = ot_ref[:, :2 * feat_t, :]
        scal_out[...] = ot_ref[0, 2 * feat_t:2 * feat_t + 8, :]
        for copy in started:
            copy.wait_send()


def home_tile(scal, img, txt, raw, x, away, sums, away_dt, xt, wt, total_rows):
    rows, dim = img.shape
    feat = x.shape[1]
    feat_t = xt.shape[1]
    blocks = txt.shape[0]
    once = dict(pipeline_mode=pl.Buffered(1))
    hbm = pl.BlockSpec(memory_space=pl.ANY)
    img_rows, txt_rows = 2 * feat, 2 * feat_t + 128
    outs = [(2, img_rows, 128), (2, 2 * feat_t, 128), (8, 128)]
    return pl.pallas_call(
        functools.partial(home_body, total_rows=total_rows),
        grid=(rows // BM,),
        in_specs=[
            pl.BlockSpec(memory_space=pltpu.SMEM),
            pl.BlockSpec((BM, dim), lambda i: (i, 0)),
            whole((blocks, BN, dim), **once),
            pl.BlockSpec((BM, dim), lambda i: (i, 0)),
            pl.BlockSpec((BM, feat), lambda i: (i, 0)),
            pl.BlockSpec((BM, dim), lambda i: (i, 0)),
            whole((3, CR, CC)),
            hbm, hbm, hbm,
        ],
        out_specs=[whole(shape, **once) for shape in outs],
        out_shape=[jax.ShapeDtypeStruct(shape, F32) for shape in outs],
        scratch_shapes=tile_scratch(dim) + [
            pltpu.VMEM((BM, dim), F32),
            pltpu.VMEM((blocks, dim, BN), F32),
            pltpu.VMEM((feat, dim), F32),
            pltpu.VMEM((3, CR, CC), F32),
            pltpu.VMEM((blocks, dim, BN), F32),
            pltpu.VMEM((rows // BM, BM, feat_t), BF16),
            pltpu.VMEM((feat_t, dim), BF16),
            pltpu.VMEM((2, dim, BM), F32),
            pltpu.VMEM((dim, feat_t), F32),
            pltpu.VMEM((2, img_rows, 128), F32),
            pltpu.VMEM((2, txt_rows, 128), F32),
            pltpu.VMEM((2, img_rows, 128), F32),
            pltpu.VMEM((2, txt_rows, 128), F32),
            pltpu.SemaphoreType.DMA((rows // BM + 1,)),
            pltpu.SemaphoreType.DMA((2,)),
        ] + sum_scratch(img_rows) + sum_scratch(txt_rows),
        compiler_params=params(62, collective_id=1, has_side_effects=True),
        cost_estimate=cost(6 * rows * rows * dim, 40 * rows * dim),
        name="home_tile",
    )(scal, img, txt, raw, x, away, sums, away_dt, xt, wt)


def solution(mesh):
    data_n, rep_n = mesh.shape["data"], mesh.shape["rep"]
    swap = [(src, (src + 1) % data_n) for src in range(data_n)]
    row_spec = P(("rep", "data"), None)

    def device_body(img_loc, txt_loc, w_img, w_txt, log_temp, logit_bias):
        rows = img_loc.shape[0]
        dim = w_img.shape[1]
        total_rows = float(rows * rep_n * data_n)
        scal = jnp.where(jnp.arange(2) == 0, log_temp, logit_bias)
        (emb_t,) = head(txt_loc, w_txt, False, "text_head")
        emb_t = emb_t.reshape(rows // BN, BN, dim)
        away_t = lax.ppermute(emb_t, "data", swap)
        emb_i, raw_i = head(img_loc, w_img, True, "image_head")
        away_di, away_dt, sums = away_tile(scal, emb_i, away_t, total_rows)
        img_sum, txt_sum, totals = home_tile(scal, emb_i, emb_t, raw_i, img_loc, away_di, sums, away_dt, txt_loc, w_txt, total_rows)
        dw_img = img_sum.reshape(4, -1, 128).transpose(1, 0, 2).reshape(-1, dim)
        dw_txt = txt_sum.reshape(4, -1, 128).transpose(1, 0, 2).reshape(-1, dim)
        return totals[0, 0], totals[1, 0], totals[2, 0], dw_img, dw_txt

    return jax.shard_map(device_body, mesh=mesh, in_specs=(row_spec, row_spec, P(), P(), P(), P()), out_specs=(P(), P(), P(), P(), P()), check_vma=False)
```

```python
import functools

import jax
import jax.numpy as jnp
from jax import lax
from jax.experimental import pallas as pl
from jax.experimental.pallas import tpu as pltpu
from jax.sharding import PartitionSpec as P

LOG2E = 1.4426950408889634
LN2 = 0.6931471805599453
NT = (((1,), (1,)), ((), ()))
TN = (((0,), (0,)), ((), ()))
MESH = pl.DeviceIdType.MESH
F32 = jnp.float32
BF16 = jnp.bfloat16
MIB = 1024 * 1024

BM = 512
BN = 256
CR, CC = 16, 256


def inv_norm(raw):
    return lax.rsqrt(jnp.sum(raw * raw, axis=1, keepdims=True))


def params(vmem, **more):
    return pltpu.CompilerParams(
        dimension_semantics=("arbitrary",),
        vmem_limit_bytes=vmem * MIB,
        **more,
    )


def scale_of(sc_ref):
    return jnp.exp(jnp.full((8, 128), sc_ref[0][0], F32))[0, 0]


def cost(flops, nbytes):
    return pl.CostEstimate(flops=int(flops), bytes_accessed=int(nbytes), transcendentals=0)


def fetch(pairs, sems):
    copies = [pltpu.make_async_copy(src, dst, sems.at[i]) for i, (src, dst) in enumerate(pairs)]
    for copy in copies:
        copy.start()
    return copies


def head_body(x_hbm, w_hbm, *refs, keep_raw):
    outs, (x_ref, w_ref, emb_ref, raw_ref, in_sem, out_sem) = refs[:-6], refs[-6:]
    blocks = x_ref.shape[0]
    arrive = fetch([(w_hbm, w_ref)] + [(x_hbm.at[pl.ds(BM * i, BM)], x_ref.at[i]) for i in range(blocks)], in_sem)
    arrive[0].wait()
    leave = []

    def product(i):
        arrive[i + 1].wait()
        raw_ref[i] = jnp.dot(x_ref[i], w_ref[...], preferred_element_type=F32)

    product(0)
    for i in range(blocks):
        if i + 1 < blocks:
            product(i + 1)
        raw = raw_ref[i]
        emb_ref[i] = (raw * inv_norm(raw)).astype(BF16)
        pairs = [(emb_ref.at[i], outs[0].at[pl.ds(BM * i, BM)])]
        if keep_raw:
            pairs.append((raw_ref.at[i], outs[1].at[pl.ds(BM * i, BM)]))
        leave += fetch(pairs, out_sem.at[i])
    for copy in leave:
        copy.wait()


def head(x, w, keep_raw, name):
    rows, feat = x.shape
    dim = w.shape[1]
    blocks = rows // BM
    hbm = pl.BlockSpec(memory_space=pl.ANY)
    out_shape = [jax.ShapeDtypeStruct((rows, dim), BF16)]
    if keep_raw:
        out_shape.append(jax.ShapeDtypeStruct((rows, dim), F32))
    return pl.pallas_call(
        functools.partial(head_body, keep_raw=keep_raw),
        in_specs=[hbm, hbm],
        out_specs=[hbm] * len(out_shape),
        out_shape=out_shape,
        scratch_shapes=[
            pltpu.VMEM((blocks, BM, feat), BF16),
            pltpu.VMEM((feat, dim), BF16),
            pltpu.VMEM((blocks, BM, dim), BF16),
            pltpu.VMEM((blocks, BM, dim), F32),
            pltpu.SemaphoreType.DMA((blocks + 1,)),
            pltpu.SemaphoreType.DMA((blocks, 2)),
        ],
        compiler_params=pltpu.CompilerParams(vmem_limit_bytes=62 * MIB),
        cost_estimate=cost(2 * rows * feat * dim, rows * (2 * feat + 6 * dim)),
        name=name,
    )(x, w)


def pair_terms(sc_ref, img_ref, txt_ref, di_ref, dt_ref, acc, s_scr, h_scr, imgt_scr, total_rows, home, di_init):
    step = pl.program_id(0)
    blocks = txt_ref.shape[0]
    s = scale_of(sc_ref)
    a, b, hs = s * LOG2E, sc_ref[1][0] * LOG2E, s * (1.0 / total_rows)
    img = img_ref[...]
    imgt_scr[...] = img.T

    def block_of(k):
        return lax.rem(step * (BM // BN) + k, blocks) if home else k

    def logits(k):
        s_scr[k % 2] = lax.dot_general(img, txt_ref[block_of(k)], NT, preferred_element_type=F32)

    def terms(k):
        zero = jnp.zeros((CR, CC), F32)
        top, prod, g_sum, gs_sum = zero, zero, zero, zero
        for r in range(0, BM, CR):
            for c in range(0, BN, CC):
                dots = s_scr[k % 2, r:r + CR, c:c + CC]
                z = dots * a + b
                pos = jnp.maximum(z, 0.0)
                t = jnp.exp2(-jnp.abs(z))
                rcp = 1.0 / (1.0 + t)
                sig = jnp.where(z >= 0, rcp, t * rcp)
                col = c + BN * k
                if home and r < col + CC and col < r + CR:
                    eye = (lax.broadcasted_iota(jnp.int32, (CR, CC), 0) + r) == (lax.broadcasted_iota(jnp.int32, (CR, CC), 1) + col)
                    sig = jnp.where(eye, -jnp.where(z >= 0, t * rcp, rcp), sig)
                    pos = jnp.where(eye, jnp.maximum(-z, 0.0), pos)
                top = top + pos
                prod = (prod + t) + prod * t
                g_sum = g_sum + sig
                gs_sum = gs_sum + sig * dots
                h_scr[k % 2, r:r + CR, c:c + CC] = (sig * hs).astype(BF16)
        acc[0] += LN2 * top + jnp.log1p(prod)
        acc[1] += gs_sum
        acc[2] += g_sum

    def grads(k):
        h = h_scr[k % 2]
        part = jnp.dot(h, txt_ref[block_of(k)], preferred_element_type=F32)
        if k == 0:
            di_ref[...] = part if di_init is None else di_init[...] + part
        else:
            di_ref[...] += part
        dt_ref[block_of(k)] += jnp.dot(imgt_scr[...], h, preferred_element_type=F32)

    logits(0)
    for k in range(blocks):
        if k + 1 < blocks:
            logits(k + 1)
        terms(k)
        grads(k)


def away_body(temp_ref, bias_ref, img_ref, txt_ref, di_ref, dt_ref, s_scr, h_scr, imgt_scr, sums_ref, *, total_rows):
    step = pl.program_id(0)

    @pl.when(step == 0)
    def _():
        sums_ref[...] = jnp.zeros_like(sums_ref)
        dt_ref[...] = jnp.zeros_like(dt_ref)

    pair_terms((temp_ref, bias_ref), img_ref, txt_ref, di_ref, dt_ref, sums_ref, s_scr, h_scr, imgt_scr, total_rows, False, None)

    @pl.when(step == pl.num_programs(0) - 1)
    def _():
        for j in range(3):
            dt_ref[txt_ref.shape[0], pl.ds(CR * j, CR), :] = sums_ref[j]


def raw_grad(raw, grad_unit):
    inv = inv_norm(raw)
    unit = raw * inv
    proj = jnp.sum(unit * grad_unit, axis=1, keepdims=True)
    return (inv * (grad_unit - unit * proj)).astype(BF16)


def tile_scratch(dim):
    return [pltpu.VMEM((2, BM, BN), F32), pltpu.VMEM((2, BM, BN), BF16), pltpu.VMEM((dim, BM), BF16)]


def whole(shape, **kw):
    return pl.BlockSpec(shape, lambda i: (0,) * len(shape), **kw)


def away_tile(temp, bias, img, txt, total_rows):
    rows, dim = img.shape
    blocks = txt.shape[0]
    once = dict(pipeline_mode=pl.Buffered(1))
    smem = pl.BlockSpec(memory_space=pltpu.SMEM)
    return pl.pallas_call(
        functools.partial(away_body, total_rows=total_rows),
        grid=(rows // BM,),
        in_specs=[smem, smem, pl.BlockSpec((BM, dim), lambda i: (i, 0)), whole((blocks, BN, dim), **once)],
        out_specs=[pl.BlockSpec((BM, dim), lambda i: (i, 0)), whole((blocks + 1, dim, BN), **once)],
        out_shape=[jax.ShapeDtypeStruct((rows, dim), F32), jax.ShapeDtypeStruct((blocks + 1, dim, BN), F32)],
        scratch_shapes=tile_scratch(dim) + [pltpu.VMEM((3, CR, CC), F32)],
        compiler_params=params(62),
        cost_estimate=cost(6 * rows * rows * dim, 30 * rows * dim),
        name="away_tile",
    )(temp, bias, img, txt)


def all_sum(src, out, bufs, peer, coord, core, send):
    pair, r1, r2, r3, psem, ssem, rsem = bufs
    part = src.shape[1] // 3
    quart, sixt = part // 4, part // 16
    sib = peer(3, 1)
    mine = out.at[core]
    dims = [(p, (p + 1) % 3, (p + 2) % 3) for p in range(3)]
    offs = (2, 1, 3)

    def spread(phase, p, d, src_of, dst_of):
        return [send(src_of(o), dst_of(o), ssem.at[phase, p, o - 1], rsem.at[phase, p, o - 1], peer(d, o)) for o in offs]

    c0 = []
    for p in range(3):
        rows = pl.ds(part * p, part)
        c0.append(send(src.at[1 - core, rows], pair.at[rows], psem.at[0, p], psem.at[1, p], sib))
    yield
    c1 = []
    for p in range(3):
        c0[p].wait_recv()
        rows = pl.ds(part * p, part)
        pair[rows, :] = pair[rows, :] + src[core, rows, :]
        d = dims[p][0]
        c1.append(spread(0, p, d, lambda o: pair.at[pl.ds(part * p + lax.rem(coord[d] + o, 4) * quart, quart)], lambda o: r1.at[p, o - 1]))
    yield
    c2, base1 = [], []
    for p in range(3):
        for copy in c1[p]:
            copy.wait_recv()
        base = part * p + coord[dims[p][0]] * quart
        base1.append(base)
        rows = pl.ds(base, quart)
        pair[rows, :] = ((pair[rows, :] + r1[p, 0]) + r1[p, 1]) + r1[p, 2]
        d = dims[p][1]
        c2.append(spread(1, p, d, lambda o: pair.at[pl.ds(base + lax.rem(coord[d] + o, 4) * sixt, sixt)], lambda o: r2.at[p, o - 1]))
    yield
    c3, base2 = [], []
    for p in range(3):
        for copy in c2[p]:
            copy.wait_recv()
        base = base1[p] + coord[dims[p][1]] * sixt
        base2.append(base)
        d = dims[p][2]
        k = coord[d]
        r3[p, k] = ((pair[pl.ds(base, sixt), :] + r2[p, 0]) + r2[p, 1]) + r2[p, 2]
        c3.append(spread(2, p, d, lambda o: r3.at[p, k], lambda o: r3.at[p, k]))
    yield
    c4 = []
    for p in range(3):
        for copy in c3[p]:
            copy.wait_recv()
        rows = pl.ds(base2[p], sixt)
        out[core, rows, :] = ((r3[p, 0] + r3[p, 1]) + r3[p, 2]) + r3[p, 3]
        c4.append(spread(3, p, dims[p][1], lambda o: mine.at[rows], lambda o: mine.at[rows]))
    yield
    c5, c6 = [], []
    for p in range(3):
        for copy in c4[p]:
            copy.wait_recv()
        rows = pl.ds(base1[p], quart)
        c5.append(spread(4, p, dims[p][0], lambda o: mine.at[rows], lambda o: mine.at[rows]))
        c6.append(send(mine.at[rows], mine.at[rows], psem.at[2, p], psem.at[3, p], sib))
    yield
    for p in range(3):
        for i, o in enumerate(offs):
            c5[p][i].wait_recv()
            rows = pl.ds(part * p + lax.rem(coord[dims[p][0]] + 4 - o, 4) * quart, quart)
            c6.append(send(mine.at[rows], mine.at[rows], psem.at[4 + 2 * i, p], psem.at[5 + 2 * i, p], sib))
    yield
    for copy in c6:
        copy.wait_recv()
    yield


def sum_scratch(rows):
    part = rows // 3
    dma = pltpu.SemaphoreType.DMA
    return [
        pltpu.VMEM((rows, 128), F32),
        pltpu.VMEM((3, 3, part // 4, 128), F32),
        pltpu.VMEM((3, 3, part // 16, 128), F32),
        pltpu.VMEM((3, 4, part // 16, 128), F32),
        dma((10, 3)),
        dma((5, 3, 3)),
        dma((5, 3, 3)),
    ]


def home_body(
    temp_ref, bias_ref, img_ref, txt_ref, raw_ref, x_ref, away_ref, away_dt, xt_hbm, wt_hbm,
    img_out, txt_out, scal_out,
    s_scr, h_scr, imgt_scr, di_ref, dt_ref, dw_ref, sums_ref, away_sums, got_ref, xt_ref, wt_ref, rawt_ref, dwt_ref, ai_ref, at_ref, oi_ref, ot_ref, sem, gsem, *bufs,
    total_rows,
):
    step = pl.program_id(0)
    sc_ref = (temp_ref, bias_ref)
    rep, core = lax.axis_index("rep"), lax.axis_index("data")
    coord = [lax.rem(rep, 4), lax.rem(lax.div(rep, 4), 4), lax.div(rep, 16)]
    stride = [1, 4, 16]

    def peer(dim, off):
        if dim == 3:
            return (rep, 1 - core)
        return (rep + (lax.rem(coord[dim] + off, 4) - coord[dim]) * stride[dim], core)

    def remote(src, dst, ssem, rsem, dev):
        return pltpu.make_async_remote_copy(src_ref=src, dst_ref=dst, send_sem=ssem, recv_sem=rsem, device_id=dev, device_id_type=MESH)

    partners = [peer(3, 1)] + [peer(dim, off) for dim in range(3) for off in (1, 2, 3)]
    blocks = xt_ref.shape[0]
    cols = BM // BN
    local = [pltpu.make_async_copy(wt_hbm, wt_ref, sem.at[0])]
    local += [pltpu.make_async_copy(xt_hbm.at[pl.ds(BM * i, BM)], xt_ref.at[i], sem.at[i + 1]) for i in range(blocks)]
    own = got_ref.shape[0]
    local.append(pltpu.make_async_copy(away_dt.at[own, pl.ds(0, 3 * CR)], away_sums, sem.at[blocks + 1]))
    swap = remote(away_dt.at[pl.ds(0, own)], got_ref, gsem.at[0], gsem.at[1], peer(3, 1))

    @pl.when(step == 0)
    def _():
        for dev in partners:
            pl.semaphore_signal(pltpu.get_barrier_semaphore(), inc=1, device_id=dev, device_id_type=MESH)
        for copy in local:
            copy.start()
        sums_ref[...] = jnp.zeros_like(sums_ref)
        dt_ref[...] = jnp.zeros_like(dt_ref)
        dw_ref[...] = jnp.zeros_like(dw_ref)

    @pl.when(step == 1)
    def _():
        pl.semaphore_wait(pltpu.get_barrier_semaphore(), len(partners))
        swap.start()

    pair_terms(sc_ref, img_ref, txt_ref, di_ref, dt_ref, sums_ref, s_scr, h_scr, imgt_scr, total_rows, True, away_ref)
    dw_ref[...] += lax.dot_general(x_ref[...], raw_grad(raw_ref[...], di_ref[...]), TN, preferred_element_type=F32)

    @pl.when(step == pl.num_programs(0) - 1)
    def _():
        started = []

        def send(*args):
            copy = remote(*args)
            copy.start()
            started.append(copy)
            return copy

        feat_i, feat_t = dw_ref.shape[0], dwt_ref.shape[1]
        for l in range(4):
            ai_ref[l // 2, pl.ds(feat_i * (l % 2), feat_i), :] = dw_ref[:, 128 * l:128 * (l + 1)]
        img = all_sum(ai_ref, oi_ref, bufs[:7], peer, coord, core, send)
        txt = all_sum(at_ref, ot_ref, bufs[7:], peer, coord, core, send)
        next(img)
        for copy in local:
            copy.wait()
        swap.wait()
        w_t = wt_ref[...].T

        def product(i):
            rawt_ref[i % 2] = lax.dot_general(w_t, xt_ref[i], NT, preferred_element_type=F32)

        def block(i):
            raw = rawt_ref[i % 2]
            inv = lax.rsqrt(jnp.sum(raw * raw, axis=0, keepdims=True))
            unit = raw * inv
            grad = jnp.concatenate([dt_ref[cols * i + j] + got_ref[cols * i + j] for j in range(cols)], axis=1)
            proj = jnp.sum(unit * grad, axis=0, keepdims=True)
            raw_grad_t = (inv * (grad - unit * proj)).astype(BF16)
            part = jnp.dot(raw_grad_t, xt_ref[i], preferred_element_type=F32)
            dwt_ref[...] = part if i == 0 else dwt_ref[...] + part

        product(0)
        for i in range(blocks):
            if i + 1 < blocks:
                product(i + 1)
            block(i)
            if i == 2:
                next(img)
        for l in range(4):
            at_ref[l // 2, pl.ds(feat_t * (l % 2), feat_t), :] = dwt_ref[128 * l:128 * (l + 1), :].T
        s = scale_of(sc_ref)
        row = lax.broadcasted_iota(jnp.int32, (128, 128), 0)
        both = [jnp.sum(sums_ref[j] + away_sums[CR * j:CR * (j + 1), :]) for j in range(3)]
        loss = both[0] / total_rows
        temp = both[1] * (s * (1.0 / total_rows))
        bias = both[2] / total_rows
        scalars = jnp.where(row == 0, loss, jnp.where(row == 1, temp, jnp.where(row == 2, bias, 0.0)))
        at_ref[0, 2 * feat_t:, :] = scalars
        at_ref[1, 2 * feat_t:, :] = jnp.zeros_like(scalars)
        next(txt)
        next(txt)
        next(img)
        for _ in range(6):
            next(txt, None)
            next(img, None)
        img_out[...] = oi_ref[...]
        txt_out[...] = ot_ref[:, :2 * feat_t, :]
        scal_out[...] = ot_ref[0, 2 * feat_t:2 * feat_t + 8, :]
        for copy in started:
            copy.wait_send()


def home_tile(temp, bias, img, txt, raw, x, away, away_dt, xt, wt, total_rows):
    rows, dim = img.shape
    feat = x.shape[1]
    feat_t = xt.shape[1]
    blocks = txt.shape[0]
    once = dict(pipeline_mode=pl.Buffered(1))
    hbm = pl.BlockSpec(memory_space=pl.ANY)
    img_rows, txt_rows = 2 * feat, 2 * feat_t + 128
    outs = [(2, img_rows, 128), (2, 2 * feat_t, 128), (8, 128)]
    return pl.pallas_call(
        functools.partial(home_body, total_rows=total_rows),
        grid=(rows // BM,),
        in_specs=[
            pl.BlockSpec(memory_space=pltpu.SMEM),
            pl.BlockSpec(memory_space=pltpu.SMEM),
            pl.BlockSpec((BM, dim), lambda i: (i, 0)),
            whole((blocks, BN, dim), **once),
            pl.BlockSpec((BM, dim), lambda i: (i, 0)),
            pl.BlockSpec((BM, feat), lambda i: (i, 0)),
            pl.BlockSpec((BM, dim), lambda i: (i, 0)),
            hbm, hbm, hbm,
        ],
        out_specs=[whole(shape, **once) for shape in outs],
        out_shape=[jax.ShapeDtypeStruct(shape, F32) for shape in outs],
        scratch_shapes=tile_scratch(dim) + [
            pltpu.VMEM((BM, dim), F32),
            pltpu.VMEM((blocks, dim, BN), F32),
            pltpu.VMEM((feat, dim), F32),
            pltpu.VMEM((3, CR, CC), F32),
            pltpu.VMEM((3 * CR, CC), F32),
            pltpu.VMEM((blocks, dim, BN), F32),
            pltpu.VMEM((rows // BM, BM, feat_t), BF16),
            pltpu.VMEM((feat_t, dim), BF16),
            pltpu.VMEM((2, dim, BM), F32),
            pltpu.VMEM((dim, feat_t), F32),
            pltpu.VMEM((2, img_rows, 128), F32),
            pltpu.VMEM((2, txt_rows, 128), F32),
            pltpu.VMEM((2, img_rows, 128), F32),
            pltpu.VMEM((2, txt_rows, 128), F32),
            pltpu.SemaphoreType.DMA((rows // BM + 2,)),
            pltpu.SemaphoreType.DMA((2,)),
        ] + sum_scratch(img_rows) + sum_scratch(txt_rows),
        compiler_params=params(48, collective_id=1, has_side_effects=True),
        cost_estimate=cost(6 * rows * rows * dim, 40 * rows * dim),
        name="home_tile",
    )(temp, bias, img, txt, raw, x, away, away_dt, xt, wt)


def solution(mesh):
    data_n, rep_n = mesh.shape["data"], mesh.shape["rep"]
    swap = [(src, (src + 1) % data_n) for src in range(data_n)]
    row_spec = P(("rep", "data"), None)

    def device_body(img_loc, txt_loc, w_img, w_txt, log_temp, logit_bias):
        rows = img_loc.shape[0]
        dim = w_img.shape[1]
        total_rows = float(rows * rep_n * data_n)
        temp, bias = log_temp.reshape(1), logit_bias.reshape(1)
        (emb_t,) = head(txt_loc, w_txt, False, "text_head")
        emb_t = emb_t.reshape(rows // BN, BN, dim)
        away_t = lax.ppermute(emb_t, "data", swap)
        emb_i, raw_i = head(img_loc, w_img, True, "image_head")
        away_di, away_dt = away_tile(temp, bias, emb_i, away_t, total_rows)
        img_sum, txt_sum, totals = home_tile(temp, bias, emb_i, emb_t, raw_i, img_loc, away_di, away_dt, txt_loc, w_txt, total_rows)
        dw_img = img_sum.reshape(4, -1, 128).transpose(1, 0, 2).reshape(-1, dim)
        dw_txt = txt_sum.reshape(4, -1, 128).transpose(1, 0, 2).reshape(-1, dim)
        return totals[0, 0], totals[1, 0], totals[2, 0], dw_img, dw_txt

    return jax.shard_map(device_body, mesh=mesh, in_specs=(row_spec, row_spec, P(), P(), P(), P()), out_specs=(P(), P(), P(), P(), P()), check_vma=False)
```

```python
import functools

import jax
import jax.numpy as jnp
from jax import lax
from jax.experimental import pallas as pl
from jax.experimental.pallas import tpu as pltpu
from jax.sharding import PartitionSpec as P

LOG2E = 1.4426950408889634
LN2 = 0.6931471805599453
NT = (((1,), (1,)), ((), ()))
TN = (((0,), (0,)), ((), ()))
MESH = pl.DeviceIdType.MESH
F32 = jnp.float32
BF16 = jnp.bfloat16
MIB = 1024 * 1024

BM = 512
BN = 256
CR, CC = 16, 256
DIAG = 4


def inv_norm(raw):
    return lax.rsqrt(jnp.sum(raw * raw, axis=1, keepdims=True))


def params(vmem, **more):
    return pltpu.CompilerParams(
        dimension_semantics=("arbitrary",),
        vmem_limit_bytes=vmem * MIB,
        **more,
    )


def scale_of(sc_ref):
    return jnp.exp(jnp.full((8, 128), sc_ref[0][0], F32))[0, 0]


def cost(flops, nbytes):
    return pl.CostEstimate(flops=int(flops), bytes_accessed=int(nbytes), transcendentals=0)


def fetch(pairs, sems):
    copies = [pltpu.make_async_copy(src, dst, sems.at[i]) for i, (src, dst) in enumerate(pairs)]
    for copy in copies:
        copy.start()
    return copies


def head_body(x_hbm, w_hbm, *refs, keep_raw):
    outs, (x_ref, w_ref, emb_ref, raw_ref, in_sem, out_sem) = refs[:-6], refs[-6:]
    blocks = x_ref.shape[0]
    arrive = fetch([(w_hbm, w_ref)] + [(x_hbm.at[pl.ds(BM * i, BM)], x_ref.at[i]) for i in range(blocks)], in_sem)
    arrive[0].wait()
    leave = []

    def product(i):
        arrive[i + 1].wait()
        raw_ref[i] = jnp.dot(x_ref[i], w_ref[...], preferred_element_type=F32)

    product(0)
    for i in range(blocks):
        if i + 1 < blocks:
            product(i + 1)
        raw = raw_ref[i]
        emb_ref[i] = (raw * inv_norm(raw)).astype(BF16)
        pairs = [(emb_ref.at[i], outs[0].at[pl.ds(BM * i, BM)])]
        if keep_raw:
            pairs.append((raw_ref.at[i], outs[1].at[pl.ds(BM * i, BM)]))
        leave += fetch(pairs, out_sem.at[i])
    for copy in leave:
        copy.wait()


def head(x, w, keep_raw, name):
    rows, feat = x.shape
    dim = w.shape[1]
    blocks = rows // BM
    hbm = pl.BlockSpec(memory_space=pl.ANY)
    out_shape = [jax.ShapeDtypeStruct((rows, dim), BF16)]
    if keep_raw:
        out_shape.append(jax.ShapeDtypeStruct((rows, dim), F32))
    return pl.pallas_call(
        functools.partial(head_body, keep_raw=keep_raw),
        in_specs=[hbm, hbm],
        out_specs=[hbm] * len(out_shape),
        out_shape=out_shape,
        scratch_shapes=[
            pltpu.VMEM((blocks, BM, feat), BF16),
            pltpu.VMEM((feat, dim), BF16),
            pltpu.VMEM((blocks, BM, dim), BF16),
            pltpu.VMEM((blocks, BM, dim), F32),
            pltpu.SemaphoreType.DMA((blocks + 1,)),
            pltpu.SemaphoreType.DMA((blocks, 2)),
        ],
        compiler_params=pltpu.CompilerParams(vmem_limit_bytes=62 * MIB),
        cost_estimate=cost(2 * rows * feat * dim, rows * (2 * feat + 6 * dim)),
        name=name,
    )(x, w)


def pair_terms(sc_ref, img_ref, txt_ref, di_ref, dt_ref, acc, s_scr, h_scr, imgt_scr, total_rows, home, di_init):
    step = pl.program_id(0)
    blocks = txt_ref.shape[0]
    s = scale_of(sc_ref)
    a, b, hs = s * LOG2E, sc_ref[1][0] * LOG2E, s * (1.0 / total_rows)
    img = img_ref[...]
    imgt_scr[...] = img.T

    def block_of(k):
        return lax.rem(step * (BM // BN) + k + blocks - DIAG, blocks) if home else k

    def logits(k):
        s_scr[k % 2] = lax.dot_general(img, txt_ref[block_of(k)], NT, preferred_element_type=F32)

    def terms(k):
        zero = jnp.zeros((CR, CC), F32)
        top, prod, g_sum, gs_sum = zero, zero, zero, zero
        for r in range(0, BM, CR):
            for c in range(0, BN, CC):
                dots = s_scr[k % 2, r:r + CR, c:c + CC]
                z = dots * a + b
                pos = jnp.maximum(z, 0.0)
                t = jnp.exp2(-jnp.abs(z))
                rcp = 1.0 / (1.0 + t)
                sig = jnp.where(z >= 0, rcp, t * rcp)
                col = c + BN * (k - DIAG)
                if home and r < col + CC and col < r + CR:
                    eye = (lax.broadcasted_iota(jnp.int32, (CR, CC), 0) + r) == (lax.broadcasted_iota(jnp.int32, (CR, CC), 1) + col)
                    sig = jnp.where(eye, -jnp.where(z >= 0, t * rcp, rcp), sig)
                    pos = jnp.where(eye, jnp.maximum(-z, 0.0), pos)
                top = top + pos
                prod = (prod + t) + prod * t
                g_sum = g_sum + sig
                gs_sum = gs_sum + sig * dots
                h_scr[k % 2, r:r + CR, c:c + CC] = (sig * hs).astype(BF16)
        acc[0] += LN2 * top + jnp.log1p(prod)
        acc[1] += gs_sum
        acc[2] += g_sum

    def grads(k):
        h = h_scr[k % 2]
        part = jnp.dot(h, txt_ref[block_of(k)], preferred_element_type=F32)
        if k == 0:
            di_ref[...] = part if di_init is None else di_init[...] + part
        else:
            di_ref[...] += part
        dt_ref[block_of(k)] += jnp.dot(imgt_scr[...], h, preferred_element_type=F32)

    logits(0)
    for k in range(blocks):
        if k + 1 < blocks:
            logits(k + 1)
        terms(k)
        grads(k)


def away_body(temp_ref, bias_ref, img_ref, txt_ref, di_ref, dt_ref, s_scr, h_scr, imgt_scr, sums_ref, *, total_rows):
    step = pl.program_id(0)

    @pl.when(step == 0)
    def _():
        sums_ref[...] = jnp.zeros_like(sums_ref)
        dt_ref[...] = jnp.zeros_like(dt_ref)

    pair_terms((temp_ref, bias_ref), img_ref, txt_ref, di_ref, dt_ref, sums_ref, s_scr, h_scr, imgt_scr, total_rows, False, None)

    @pl.when(step == pl.num_programs(0) - 1)
    def _():
        for j in range(3):
            dt_ref[txt_ref.shape[0], pl.ds(CR * j, CR), :] = sums_ref[j]


def raw_grad(raw, grad_unit):
    inv = inv_norm(raw)
    unit = raw * inv
    proj = jnp.sum(unit * grad_unit, axis=1, keepdims=True)
    return (inv * (grad_unit - unit * proj)).astype(BF16)


def tile_scratch(dim):
    return [pltpu.VMEM((2, BM, BN), F32), pltpu.VMEM((2, BM, BN), BF16), pltpu.VMEM((dim, BM), BF16)]


def whole(shape, **kw):
    return pl.BlockSpec(shape, lambda i: (0,) * len(shape), **kw)


def away_tile(temp, bias, img, txt, total_rows):
    rows, dim = img.shape
    blocks = txt.shape[0]
    once = dict(pipeline_mode=pl.Buffered(1))
    smem = pl.BlockSpec(memory_space=pltpu.SMEM)
    return pl.pallas_call(
        functools.partial(away_body, total_rows=total_rows),
        grid=(rows // BM,),
        in_specs=[smem, smem, pl.BlockSpec((BM, dim), lambda i: (i, 0)), whole((blocks, BN, dim), **once)],
        out_specs=[pl.BlockSpec((BM, dim), lambda i: (i, 0)), whole((blocks + 1, dim, BN), **once)],
        out_shape=[jax.ShapeDtypeStruct((rows, dim), F32), jax.ShapeDtypeStruct((blocks + 1, dim, BN), F32)],
        scratch_shapes=tile_scratch(dim) + [pltpu.VMEM((3, CR, CC), F32)],
        compiler_params=params(62),
        cost_estimate=cost(6 * rows * rows * dim, 30 * rows * dim),
        name="away_tile",
    )(temp, bias, img, txt)


def all_sum(src, out, bufs, peer, coord, core, send):
    pair, r1, r2, r3, psem, ssem, rsem = bufs
    part = src.shape[1] // 3
    quart, sixt = part // 4, part // 16
    sib = peer(3, 1)
    mine = out.at[core]
    dims = [(p, (p + 1) % 3, (p + 2) % 3) for p in range(3)]
    offs = (2, 1, 3)

    def spread(phase, p, d, src_of, dst_of):
        return [send(src_of(o), dst_of(o), ssem.at[phase, p, o - 1], rsem.at[phase, p, o - 1], peer(d, o)) for o in offs]

    c0 = []
    for p in range(3):
        rows = pl.ds(part * p, part)
        c0.append(send(src.at[1 - core, rows], pair.at[rows], psem.at[0, p], psem.at[1, p], sib))
    yield
    c1 = []
    for p in range(3):
        c0[p].wait_recv()
        rows = pl.ds(part * p, part)
        pair[rows, :] = pair[rows, :] + src[core, rows, :]
        d = dims[p][0]
        c1.append(spread(0, p, d, lambda o: pair.at[pl.ds(part * p + lax.rem(coord[d] + o, 4) * quart, quart)], lambda o: r1.at[p, o - 1]))
    yield
    c2, base1 = [], []
    for p in range(3):
        for copy in c1[p]:
            copy.wait_recv()
        base = part * p + coord[dims[p][0]] * quart
        base1.append(base)
        rows = pl.ds(base, quart)
        pair[rows, :] = ((pair[rows, :] + r1[p, 0]) + r1[p, 1]) + r1[p, 2]
        d = dims[p][1]
        c2.append(spread(1, p, d, lambda o: pair.at[pl.ds(base + lax.rem(coord[d] + o, 4) * sixt, sixt)], lambda o: r2.at[p, o - 1]))
    yield
    c3, base2 = [], []
    for p in range(3):
        for copy in c2[p]:
            copy.wait_recv()
        base = base1[p] + coord[dims[p][1]] * sixt
        base2.append(base)
        d = dims[p][2]
        k = coord[d]
        r3[p, k] = ((pair[pl.ds(base, sixt), :] + r2[p, 0]) + r2[p, 1]) + r2[p, 2]
        c3.append(spread(2, p, d, lambda o: r3.at[p, k], lambda o: r3.at[p, k]))
    yield
    c4 = []
    for p in range(3):
        for copy in c3[p]:
            copy.wait_recv()
        rows = pl.ds(base2[p], sixt)
        out[core, rows, :] = ((r3[p, 0] + r3[p, 1]) + r3[p, 2]) + r3[p, 3]
        c4.append(spread(3, p, dims[p][1], lambda o: mine.at[rows], lambda o: mine.at[rows]))
    yield
    c5, c6 = [], []
    for p in range(3):
        for copy in c4[p]:
            copy.wait_recv()
        rows = pl.ds(base1[p], quart)
        c5.append(spread(4, p, dims[p][0], lambda o: mine.at[rows], lambda o: mine.at[rows]))
        c6.append(send(mine.at[rows], mine.at[rows], psem.at[2, p], psem.at[3, p], sib))
    yield
    for p in range(3):
        for i, o in enumerate(offs):
            c5[p][i].wait_recv()
            rows = pl.ds(part * p + lax.rem(coord[dims[p][0]] + 4 - o, 4) * quart, quart)
            c6.append(send(mine.at[rows], mine.at[rows], psem.at[4 + 2 * i, p], psem.at[5 + 2 * i, p], sib))
    yield
    for copy in c6:
        copy.wait_recv()
    yield


def sum_scratch(rows):
    part = rows // 3
    dma = pltpu.SemaphoreType.DMA
    return [
        pltpu.VMEM((rows, 128), F32),
        pltpu.VMEM((3, 3, part // 4, 128), F32),
        pltpu.VMEM((3, 3, part // 16, 128), F32),
        pltpu.VMEM((3, 4, part // 16, 128), F32),
        dma((10, 3)),
        dma((5, 3, 3)),
        dma((5, 3, 3)),
    ]


def home_body(
    temp_ref, bias_ref, img_ref, txt_ref, raw_ref, x_ref, away_ref, away_dt, xt_hbm, xb_ref, wt_ref,
    img_out, txt_out, scal_out,
    s_scr, h_scr, imgt_scr, di_ref, dt_ref, dw_ref, sums_ref, away_sums, got_ref, xt_ref, rawt_ref, dwt_ref, ai_ref, at_ref, oi_ref, ot_ref, sem, gsem, *bufs,
    total_rows,
):
    step = pl.program_id(0)
    sc_ref = (temp_ref, bias_ref)
    rep, core = lax.axis_index("rep"), lax.axis_index("data")
    coord = [lax.rem(rep, 4), lax.rem(lax.div(rep, 4), 4), lax.div(rep, 16)]
    stride = [1, 4, 16]

    def peer(dim, off):
        if dim == 3:
            return (rep, 1 - core)
        return (rep + (lax.rem(coord[dim] + off, 4) - coord[dim]) * stride[dim], core)

    def remote(src, dst, ssem, rsem, dev):
        return pltpu.make_async_remote_copy(src_ref=src, dst_ref=dst, send_sem=ssem, recv_sem=rsem, device_id=dev, device_id_type=MESH)

    partners = [peer(3, 1)] + [peer(dim, off) for dim in range(3) for off in (1, 2, 3)]
    blocks = xt_ref.shape[0]
    cols = BM // BN
    local = [pltpu.make_async_copy(xt_hbm.at[pl.ds(BM * i, BM)], xt_ref.at[i], sem.at[i]) for i in range(blocks)]
    own = got_ref.shape[0]
    local.append(pltpu.make_async_copy(away_dt.at[own, pl.ds(0, 3 * CR)], away_sums, sem.at[blocks]))
    swap = remote(away_dt.at[pl.ds(0, own)], got_ref, gsem.at[0], gsem.at[1], peer(3, 1))

    @pl.when(step == 0)
    def _():
        for dev in partners:
            pl.semaphore_signal(pltpu.get_barrier_semaphore(), inc=1, device_id=dev, device_id_type=MESH)
        for copy in local:
            copy.start()
        sums_ref[...] = jnp.zeros_like(sums_ref)
        dt_ref[...] = jnp.zeros_like(dt_ref)
        dw_ref[...] = jnp.zeros_like(dw_ref)

    @pl.when(step == 1)
    def _():
        pl.semaphore_wait(pltpu.get_barrier_semaphore(), len(partners))
        swap.start()

    rawt_ref[step] = lax.dot_general(wt_ref[...], xb_ref[...], (((0,), (1,)), ((), ())), preferred_element_type=F32)
    pair_terms(sc_ref, img_ref, txt_ref, di_ref, dt_ref, sums_ref, s_scr, h_scr, imgt_scr, total_rows, True, away_ref)
    dw_ref[...] += lax.dot_general(x_ref[...], raw_grad(raw_ref[...], di_ref[...]), TN, preferred_element_type=F32)

    @pl.when(step == pl.num_programs(0) - 1)
    def _():
        started = []

        def send(*args):
            copy = remote(*args)
            copy.start()
            started.append(copy)
            return copy

        feat_i, feat_t = dw_ref.shape[0], dwt_ref.shape[1]
        for l in range(4):
            ai_ref[l // 2, pl.ds(feat_i * (l % 2), feat_i), :] = dw_ref[:, 128 * l:128 * (l + 1)]
        img = all_sum(ai_ref, oi_ref, bufs[:7], peer, coord, core, send)
        txt = all_sum(at_ref, ot_ref, bufs[7:], peer, coord, core, send)
        next(img)
        for copy in local:
            copy.wait()
        swap.wait()

        def block(i):
            raw = rawt_ref[i]
            inv = lax.rsqrt(jnp.sum(raw * raw, axis=0, keepdims=True))
            unit = raw * inv
            grad = jnp.concatenate([dt_ref[cols * i + j] + got_ref[cols * i + j] for j in range(cols)], axis=1)
            proj = jnp.sum(unit * grad, axis=0, keepdims=True)
            raw_grad_t = (inv * (grad - unit * proj)).astype(BF16)
            part = jnp.dot(raw_grad_t, xt_ref[i], preferred_element_type=F32)
            dwt_ref[...] = part if i == 0 else dwt_ref[...] + part

        for i in range(blocks):
            block(i)
            if i == 2:
                next(img)
        for l in range(4):
            at_ref[l // 2, pl.ds(feat_t * (l % 2), feat_t), :] = dwt_ref[128 * l:128 * (l + 1), :].T
        s = scale_of(sc_ref)
        row = lax.broadcasted_iota(jnp.int32, (128, 128), 0)
        both = [jnp.sum(sums_ref[j] + away_sums[CR * j:CR * (j + 1), :]) for j in range(3)]
        loss = both[0] / total_rows
        temp = both[1] * (s * (1.0 / total_rows))
        bias = both[2] / total_rows
        scalars = jnp.where(row == 0, loss, jnp.where(row == 1, temp, jnp.where(row == 2, bias, 0.0)))
        at_ref[0, 2 * feat_t:, :] = scalars
        at_ref[1, 2 * feat_t:, :] = jnp.zeros_like(scalars)
        next(txt)
        next(txt)
        next(img)
        for _ in range(6):
            next(txt, None)
            next(img, None)
        img_out[...] = oi_ref[...]
        txt_out[...] = ot_ref[:, :2 * feat_t, :]
        scal_out[...] = ot_ref[0, 2 * feat_t:2 * feat_t + 8, :]
        for copy in started:
            copy.wait_send()


def home_tile(temp, bias, img, txt, raw, x, away, away_dt, xt, wt, total_rows):
    rows, dim = img.shape
    feat = x.shape[1]
    feat_t = xt.shape[1]
    blocks = txt.shape[0]
    once = dict(pipeline_mode=pl.Buffered(1))
    hbm = pl.BlockSpec(memory_space=pl.ANY)
    img_rows, txt_rows = 2 * feat, 2 * feat_t + 128
    outs = [(2, img_rows, 128), (2, 2 * feat_t, 128), (8, 128)]
    return pl.pallas_call(
        functools.partial(home_body, total_rows=total_rows),
        grid=(rows // BM,),
        in_specs=[
            pl.BlockSpec(memory_space=pltpu.SMEM),
            pl.BlockSpec(memory_space=pltpu.SMEM),
            pl.BlockSpec((BM, dim), lambda i: (i, 0)),
            whole((blocks, BN, dim), **once),
            pl.BlockSpec((BM, dim), lambda i: (i, 0)),
            pl.BlockSpec((BM, feat), lambda i: (i, 0)),
            pl.BlockSpec((BM, dim), lambda i: (i, 0)),
            hbm, hbm,
            pl.BlockSpec((BM, feat_t), lambda i: (i, 0)),
            whole((feat_t, dim), **once),
        ],
        out_specs=[whole(shape, **once) for shape in outs],
        out_shape=[jax.ShapeDtypeStruct(shape, F32) for shape in outs],
        scratch_shapes=tile_scratch(dim) + [
            pltpu.VMEM((BM, dim), F32),
            pltpu.VMEM((blocks, dim, BN), F32),
            pltpu.VMEM((feat, dim), F32),
            pltpu.VMEM((3, CR, CC), F32),
            pltpu.VMEM((3 * CR, CC), F32),
            pltpu.VMEM((blocks, dim, BN), F32),
            pltpu.VMEM((rows // BM, BM, feat_t), BF16),
            pltpu.VMEM((rows // BM, dim, BM), F32),
            pltpu.VMEM((dim, feat_t), F32),
            pltpu.VMEM((2, img_rows, 128), F32),
            pltpu.VMEM((2, txt_rows, 128), F32),
            pltpu.VMEM((2, img_rows, 128), F32),
            pltpu.VMEM((2, txt_rows, 128), F32),
            pltpu.SemaphoreType.DMA((rows // BM + 1,)),
            pltpu.SemaphoreType.DMA((2,)),
        ] + sum_scratch(img_rows) + sum_scratch(txt_rows),
        compiler_params=params(48, collective_id=1, has_side_effects=True),
        cost_estimate=cost(6 * rows * rows * dim, 40 * rows * dim),
        name="home_tile",
    )(temp, bias, img, txt, raw, x, away, away_dt, xt, xt, wt)


def solution(mesh):
    data_n, rep_n = mesh.shape["data"], mesh.shape["rep"]
    swap = [(src, (src + 1) % data_n) for src in range(data_n)]
    row_spec = P(("rep", "data"), None)

    def device_body(img_loc, txt_loc, w_img, w_txt, log_temp, logit_bias):
        rows = img_loc.shape[0]
        dim = w_img.shape[1]
        total_rows = float(rows * rep_n * data_n)
        temp, bias = log_temp.reshape(1), logit_bias.reshape(1)
        (emb_t,) = head(txt_loc, w_txt, False, "text_head")
        emb_t = emb_t.reshape(rows // BN, BN, dim)
        away_t = lax.ppermute(emb_t, "data", swap)
        emb_i, raw_i = head(img_loc, w_img, True, "image_head")
        away_di, away_dt = away_tile(temp, bias, emb_i, away_t, total_rows)
        img_sum, txt_sum, totals = home_tile(temp, bias, emb_i, emb_t, raw_i, img_loc, away_di, away_dt, txt_loc, w_txt, total_rows)
        dw_img = img_sum.reshape(4, -1, 128).transpose(1, 0, 2).reshape(-1, dim)
        dw_txt = txt_sum.reshape(4, -1, 128).transpose(1, 0, 2).reshape(-1, dim)
        return totals[0, 0], totals[1, 0], totals[2, 0], dw_img, dw_txt

    return jax.shard_map(device_body, mesh=mesh, in_specs=(row_spec, row_spec, P(), P(), P(), P()), out_specs=(P(), P(), P(), P(), P()), check_vma=False)
```

```python
import functools

import jax
import jax.numpy as jnp
from jax import lax
from jax.experimental import pallas as pl
from jax.experimental.pallas import tpu as pltpu
from jax.sharding import PartitionSpec as P

LOG2E = 1.4426950408889634
LN2 = 0.6931471805599453
NT = (((1,), (1,)), ((), ()))
TN = (((0,), (0,)), ((), ()))
MESH = pl.DeviceIdType.MESH
F32 = jnp.float32
BF16 = jnp.bfloat16
MIB = 1024 * 1024

BM = 512
BN = 256
CR, CC = 16, 256


def inv_norm(raw):
    return lax.rsqrt(jnp.sum(raw * raw, axis=1, keepdims=True))


def params(vmem, **more):
    return pltpu.CompilerParams(
        dimension_semantics=("arbitrary",),
        vmem_limit_bytes=vmem * MIB,
        **more,
    )


def scale_of(sc_ref):
    return jnp.exp(jnp.full((8, 128), sc_ref[0][0], F32))[0, 0]


def cost(flops, nbytes):
    return pl.CostEstimate(flops=int(flops), bytes_accessed=int(nbytes), transcendentals=0)


def fetch(pairs, sems):
    copies = [pltpu.make_async_copy(src, dst, sems.at[i]) for i, (src, dst) in enumerate(pairs)]
    for copy in copies:
        copy.start()
    return copies


def heads_body(xt_hbm, wt_hbm, xi_hbm, wi_hbm, embt_out, away_out, embi_out, raw_out, xt, wt, xi, wi, embt, embi, rawt, rawi, in_sem, out_sem, ssem, rsem):
    sib = (lax.axis_index("rep"), 1 - lax.axis_index("data"))
    bar = pltpu.get_barrier_semaphore()
    pl.semaphore_signal(bar, inc=1, device_id=sib, device_id_type=MESH)
    blocks = xt.shape[0]
    rows = [pl.ds(BM * i, BM) for i in range(blocks)]
    pairs = [(wt_hbm, wt)] + [(xt_hbm.at[rows[i]], xt.at[i]) for i in range(blocks)]
    arrive = fetch(pairs + [(wi_hbm, wi)] + [(xi_hbm.at[rows[i]], xi.at[i]) for i in range(blocks)], in_sem)
    leave = []

    def product_t(i):
        arrive[i + 1].wait()
        rawt[i % 2] = jnp.dot(xt[i], wt[...], preferred_element_type=F32)

    def product_i(i):
        arrive[blocks + i + 2].wait()
        rawi[i] = jnp.dot(xi[i], wi[...], preferred_element_type=F32)

    arrive[0].wait()
    product_t(0)
    pl.semaphore_wait(bar, 1)
    for i in range(blocks):
        if i + 1 < blocks:
            product_t(i + 1)
        else:
            arrive[blocks + 1].wait()
            product_i(0)
        raw = rawt[i % 2]
        embt[i] = (raw * inv_norm(raw)).astype(BF16)
        leave += fetch([(embt.at[i], embt_out.at[rows[i]])], out_sem.at[0, pl.ds(i, 1)])
        copy = pltpu.make_async_remote_copy(src_ref=embt.at[i], dst_ref=away_out.at[rows[i]], send_sem=ssem.at[i], recv_sem=rsem.at[i], device_id=sib, device_id_type=MESH)
        copy.start()
        leave.append(copy)
    for i in range(blocks):
        if i + 1 < blocks:
            product_i(i + 1)
        raw = rawi[i]
        embi[i] = (raw * inv_norm(raw)).astype(BF16)
        leave += fetch([(rawi.at[i], raw_out.at[rows[i]])], out_sem.at[1, pl.ds(i, 1)])
        leave += fetch([(embi.at[i], embi_out.at[rows[i]])], out_sem.at[2, pl.ds(i, 1)])
    for copy in leave:
        copy.wait()


def heads(xt, wt, xi, wi):
    rows, feat_t = xt.shape
    feat_i, dim = wi.shape
    blocks = rows // BM
    hbm = pl.BlockSpec(memory_space=pl.ANY)
    emb = jax.ShapeDtypeStruct((rows, dim), BF16)
    dma = pltpu.SemaphoreType.DMA
    return pl.pallas_call(
        heads_body,
        in_specs=[hbm] * 4,
        out_specs=[hbm] * 4,
        out_shape=[emb, emb, emb, jax.ShapeDtypeStruct((rows, dim), F32)],
        scratch_shapes=[
            pltpu.VMEM((blocks, BM, feat_t), BF16),
            pltpu.VMEM((feat_t, dim), BF16),
            pltpu.VMEM((blocks, BM, feat_i), BF16),
            pltpu.VMEM((feat_i, dim), BF16),
            pltpu.VMEM((blocks, BM, dim), BF16),
            pltpu.VMEM((blocks, BM, dim), BF16),
            pltpu.VMEM((2, BM, dim), F32),
            pltpu.VMEM((blocks, BM, dim), F32),
            dma((2 * blocks + 2,)),
            dma((3, blocks)),
            dma((blocks,)),
            dma((blocks,)),
        ],
        compiler_params=pltpu.CompilerParams(collective_id=2, has_side_effects=True, vmem_limit_bytes=62 * MIB),
        cost_estimate=cost(2 * rows * (feat_t + feat_i) * dim, rows * (2 * feat_t + 2 * feat_i + 10 * dim)),
        name="heads",
    )(xt, wt, xi, wi)


def pair_terms(sc_ref, img_ref, txt_ref, di_ref, dt_ref, acc, s_scr, h_scr, imgt_scr, total_rows, home, di_init):
    step = pl.program_id(0)
    blocks = txt_ref.shape[0]
    s = scale_of(sc_ref)
    a, b, hs = s * LOG2E, sc_ref[1][0] * LOG2E, s * (1.0 / total_rows)
    img = img_ref[...]
    imgt_scr[...] = img.T

    def block_of(k):
        return lax.rem(step * (BM // BN) + k, blocks) if home else k

    def logits(k):
        s_scr[k % 2] = lax.dot_general(img, txt_ref[block_of(k)], NT, preferred_element_type=F32)

    def terms(k):
        zero = jnp.zeros((CR, CC), F32)
        top, prod, g_sum, gs_sum = zero, zero, zero, zero
        for r in range(0, BM, CR):
            for c in range(0, BN, CC):
                dots = s_scr[k % 2, r:r + CR, c:c + CC]
                z = dots * a + b
                pos = jnp.maximum(z, 0.0)
                t = jnp.exp2(-jnp.abs(z))
                rcp = 1.0 / (1.0 + t)
                sig = jnp.where(z >= 0, rcp, t * rcp)
                col = c + BN * k
                if home and r < col + CC and col < r + CR:
                    eye = (lax.broadcasted_iota(jnp.int32, (CR, CC), 0) + r) == (lax.broadcasted_iota(jnp.int32, (CR, CC), 1) + col)
                    sig = jnp.where(eye, -jnp.where(z >= 0, t * rcp, rcp), sig)
                    pos = jnp.where(eye, jnp.maximum(-z, 0.0), pos)
                top = top + pos
                prod = (prod + t) + prod * t
                g_sum = g_sum + sig
                gs_sum = gs_sum + sig * dots
                h_scr[k % 2, r:r + CR, c:c + CC] = (sig * hs).astype(BF16)
        acc[0] += LN2 * top + jnp.log1p(prod)
        acc[1] += gs_sum
        acc[2] += g_sum

    def grads(k):
        h = h_scr[k % 2]
        part = jnp.dot(h, txt_ref[block_of(k)], preferred_element_type=F32)
        if k == 0:
            di_ref[...] = part if di_init is None else di_init[...] + part
        else:
            di_ref[...] += part
        dt_ref[block_of(k)] += jnp.dot(imgt_scr[...], h, preferred_element_type=F32)

    logits(0)
    for k in range(blocks):
        if k + 1 < blocks:
            logits(k + 1)
        terms(k)
        grads(k)


def away_body(temp_ref, bias_ref, img_ref, txt_ref, di_ref, dt_ref, s_scr, h_scr, imgt_scr, sums_ref, *, total_rows):
    step = pl.program_id(0)

    @pl.when(step == 0)
    def _():
        sums_ref[...] = jnp.zeros_like(sums_ref)
        dt_ref[...] = jnp.zeros_like(dt_ref)

    pair_terms((temp_ref, bias_ref), img_ref, txt_ref, di_ref, dt_ref, sums_ref, s_scr, h_scr, imgt_scr, total_rows, False, None)

    @pl.when(step == pl.num_programs(0) - 1)
    def _():
        for j in range(3):
            dt_ref[txt_ref.shape[0], pl.ds(CR * j, CR), :] = sums_ref[j]


def raw_grad(raw, grad_unit):
    inv = inv_norm(raw)
    unit = raw * inv
    proj = jnp.sum(unit * grad_unit, axis=1, keepdims=True)
    return (inv * (grad_unit - unit * proj)).astype(BF16)


def tile_scratch(dim):
    return [pltpu.VMEM((2, BM, BN), F32), pltpu.VMEM((2, BM, BN), BF16), pltpu.VMEM((dim, BM), BF16)]


def whole(shape, **kw):
    return pl.BlockSpec(shape, lambda i: (0,) * len(shape), **kw)


def away_tile(temp, bias, img, txt, total_rows):
    rows, dim = img.shape
    blocks = txt.shape[0]
    once = dict(pipeline_mode=pl.Buffered(1))
    smem = pl.BlockSpec(memory_space=pltpu.SMEM)
    return pl.pallas_call(
        functools.partial(away_body, total_rows=total_rows),
        grid=(rows // BM,),
        in_specs=[smem, smem, pl.BlockSpec((BM, dim), lambda i: (i, 0)), whole((blocks, BN, dim), **once)],
        out_specs=[pl.BlockSpec((BM, dim), lambda i: (i, 0)), whole((blocks + 1, dim, BN), **once)],
        out_shape=[jax.ShapeDtypeStruct((rows, dim), F32), jax.ShapeDtypeStruct((blocks + 1, dim, BN), F32)],
        scratch_shapes=tile_scratch(dim) + [pltpu.VMEM((3, CR, CC), F32)],
        compiler_params=params(62),
        cost_estimate=cost(6 * rows * rows * dim, 30 * rows * dim),
        name="away_tile",
    )(temp, bias, img, txt)


def all_sum(src, out, bufs, peer, coord, core, send):
    pair, r1, r2, r3, psem, ssem, rsem = bufs
    part = src.shape[1] // 3
    quart, sixt = part // 4, part // 16
    sib = peer(3, 1)
    mine = out.at[core]
    dims = [(p, (p + 1) % 3, (p + 2) % 3) for p in range(3)]
    offs = (2, 1, 3)

    def spread(phase, p, d, src_of, dst_of):
        return [send(src_of(o), dst_of(o), ssem.at[phase, p, o - 1], rsem.at[phase, p, o - 1], peer(d, o)) for o in offs]

    c0 = []
    for p in range(3):
        rows = pl.ds(part * p, part)
        c0.append(send(src.at[1 - core, rows], pair.at[rows], psem.at[0, p], psem.at[1, p], sib))
    yield
    c1 = []
    for p in range(3):
        c0[p].wait_recv()
        rows = pl.ds(part * p, part)
        pair[rows, :] = pair[rows, :] + src[core, rows, :]
        d = dims[p][0]
        c1.append(spread(0, p, d, lambda o: pair.at[pl.ds(part * p + lax.rem(coord[d] + o, 4) * quart, quart)], lambda o: r1.at[p, o - 1]))
    yield
    c2, base1 = [], []
    for p in range(3):
        for copy in c1[p]:
            copy.wait_recv()
        base = part * p + coord[dims[p][0]] * quart
        base1.append(base)
        rows = pl.ds(base, quart)
        pair[rows, :] = ((pair[rows, :] + r1[p, 0]) + r1[p, 1]) + r1[p, 2]
        d = dims[p][1]
        c2.append(spread(1, p, d, lambda o: pair.at[pl.ds(base + lax.rem(coord[d] + o, 4) * sixt, sixt)], lambda o: r2.at[p, o - 1]))
    yield
    c3, base2 = [], []
    for p in range(3):
        for copy in c2[p]:
            copy.wait_recv()
        base = base1[p] + coord[dims[p][1]] * sixt
        base2.append(base)
        d = dims[p][2]
        k = coord[d]
        r3[p, k] = ((pair[pl.ds(base, sixt), :] + r2[p, 0]) + r2[p, 1]) + r2[p, 2]
        c3.append(spread(2, p, d, lambda o: r3.at[p, k], lambda o: r3.at[p, k]))
    yield
    c4 = []
    for p in range(3):
        for copy in c3[p]:
            copy.wait_recv()
        rows = pl.ds(base2[p], sixt)
        out[core, rows, :] = ((r3[p, 0] + r3[p, 1]) + r3[p, 2]) + r3[p, 3]
        c4.append(spread(3, p, dims[p][1], lambda o: mine.at[rows], lambda o: mine.at[rows]))
    yield
    c5, c6 = [], []
    for p in range(3):
        for copy in c4[p]:
            copy.wait_recv()
        rows = pl.ds(base1[p], quart)
        c5.append(spread(4, p, dims[p][0], lambda o: mine.at[rows], lambda o: mine.at[rows]))
        c6.append(send(mine.at[rows], mine.at[rows], psem.at[2, p], psem.at[3, p], sib))
    yield
    for p in range(3):
        for i, o in enumerate(offs):
            c5[p][i].wait_recv()
            rows = pl.ds(part * p + lax.rem(coord[dims[p][0]] + 4 - o, 4) * quart, quart)
            c6.append(send(mine.at[rows], mine.at[rows], psem.at[4 + 2 * i, p], psem.at[5 + 2 * i, p], sib))
    yield
    for copy in c6:
        copy.wait_recv()
    yield


def sum_scratch(rows):
    part = rows // 3
    dma = pltpu.SemaphoreType.DMA
    return [
        pltpu.VMEM((rows, 128), F32),
        pltpu.VMEM((3, 3, part // 4, 128), F32),
        pltpu.VMEM((3, 3, part // 16, 128), F32),
        pltpu.VMEM((3, 4, part // 16, 128), F32),
        dma((10, 3)),
        dma((5, 3, 3)),
        dma((5, 3, 3)),
    ]


def home_body(
    temp_ref, bias_ref, img_ref, txt_ref, raw_ref, x_ref, away_ref, away_dt, xt_hbm, wt_hbm,
    img_out, txt_out, scal_out,
    s_scr, h_scr, imgt_scr, di_ref, dt_ref, dw_ref, sums_ref, away_sums, got_ref, xt_ref, wt_ref, rawt_ref, dwt_ref, ai_ref, at_ref, oi_ref, ot_ref, sem, gsem, *bufs,
    total_rows,
):
    step = pl.program_id(0)
    sc_ref = (temp_ref, bias_ref)
    rep, core = lax.axis_index("rep"), lax.axis_index("data")
    coord = [lax.rem(rep, 4), lax.rem(lax.div(rep, 4), 4), lax.div(rep, 16)]
    stride = [1, 4, 16]

    def peer(dim, off):
        if dim == 3:
            return (rep, 1 - core)
        return (rep + (lax.rem(coord[dim] + off, 4) - coord[dim]) * stride[dim], core)

    def remote(src, dst, ssem, rsem, dev):
        return pltpu.make_async_remote_copy(src_ref=src, dst_ref=dst, send_sem=ssem, recv_sem=rsem, device_id=dev, device_id_type=MESH)

    partners = [peer(3, 1)] + [peer(dim, off) for dim in range(3) for off in (1, 2, 3)]
    blocks = xt_ref.shape[0]
    cols = BM // BN
    local = [pltpu.make_async_copy(wt_hbm, wt_ref, sem.at[0])]
    local += [pltpu.make_async_copy(xt_hbm.at[pl.ds(BM * i, BM)], xt_ref.at[i], sem.at[i + 1]) for i in range(blocks)]
    own = got_ref.shape[0]
    local.append(pltpu.make_async_copy(away_dt.at[own, pl.ds(0, 3 * CR)], away_sums, sem.at[blocks + 1]))
    swap = remote(away_dt.at[pl.ds(0, own)], got_ref, gsem.at[0], gsem.at[1], peer(3, 1))

    @pl.when(step == 0)
    def _():
        for dev in partners:
            pl.semaphore_signal(pltpu.get_barrier_semaphore(), inc=1, device_id=dev, device_id_type=MESH)
        for copy in local:
            copy.start()
        sums_ref[...] = jnp.zeros_like(sums_ref)
        dt_ref[...] = jnp.zeros_like(dt_ref)
        dw_ref[...] = jnp.zeros_like(dw_ref)

    @pl.when(step == 1)
    def _():
        pl.semaphore_wait(pltpu.get_barrier_semaphore(), len(partners))
        swap.start()

    pair_terms(sc_ref, img_ref, txt_ref, di_ref, dt_ref, sums_ref, s_scr, h_scr, imgt_scr, total_rows, True, away_ref)
    dw_ref[...] += lax.dot_general(x_ref[...], raw_grad(raw_ref[...], di_ref[...]), TN, preferred_element_type=F32)

    @pl.when(step == pl.num_programs(0) - 1)
    def _():
        started = []

        def send(*args):
            copy = remote(*args)
            copy.start()
            started.append(copy)
            return copy

        feat_i, feat_t = dw_ref.shape[0], dwt_ref.shape[1]
        for l in range(4):
            ai_ref[l // 2, pl.ds(feat_i * (l % 2), feat_i), :] = dw_ref[:, 128 * l:128 * (l + 1)]
        img = all_sum(ai_ref, oi_ref, bufs[:7], peer, coord, core, send)
        txt = all_sum(at_ref, ot_ref, bufs[7:], peer, coord, core, send)
        next(img)
        for copy in local:
            copy.wait()
        swap.wait()
        w_t = wt_ref[...].T

        def product(i):
            rawt_ref[i % 2] = lax.dot_general(w_t, xt_ref[i], NT, preferred_element_type=F32)

        def block(i):
            raw = rawt_ref[i % 2]
            inv = lax.rsqrt(jnp.sum(raw * raw, axis=0, keepdims=True))
            unit = raw * inv
            grad = jnp.concatenate([dt_ref[cols * i + j] + got_ref[cols * i + j] for j in range(cols)], axis=1)
            proj = jnp.sum(unit * grad, axis=0, keepdims=True)
            raw_grad_t = (inv * (grad - unit * proj)).astype(BF16)
            part = jnp.dot(raw_grad_t, xt_ref[i], preferred_element_type=F32)
            dwt_ref[...] = part if i == 0 else dwt_ref[...] + part

        product(0)
        for i in range(blocks):
            if i + 1 < blocks:
                product(i + 1)
            block(i)
            if i == 2:
                next(img)
        for l in range(4):
            at_ref[l // 2, pl.ds(feat_t * (l % 2), feat_t), :] = dwt_ref[128 * l:128 * (l + 1), :].T
        s = scale_of(sc_ref)
        row = lax.broadcasted_iota(jnp.int32, (128, 128), 0)
        both = [jnp.sum(sums_ref[j] + away_sums[CR * j:CR * (j + 1), :]) for j in range(3)]
        loss = both[0] / total_rows
        temp = both[1] * (s * (1.0 / total_rows))
        bias = both[2] / total_rows
        scalars = jnp.where(row == 0, loss, jnp.where(row == 1, temp, jnp.where(row == 2, bias, 0.0)))
        at_ref[0, 2 * feat_t:, :] = scalars
        at_ref[1, 2 * feat_t:, :] = jnp.zeros_like(scalars)
        next(txt)
        next(txt)
        next(img)
        for _ in range(6):
            next(txt, None)
            next(img, None)
        img_out[...] = oi_ref[...]
        txt_out[...] = ot_ref[:, :2 * feat_t, :]
        scal_out[...] = ot_ref[0, 2 * feat_t:2 * feat_t + 8, :]
        for copy in started:
            copy.wait_send()


def home_tile(temp, bias, img, txt, raw, x, away, away_dt, xt, wt, total_rows):
    rows, dim = img.shape
    feat = x.shape[1]
    feat_t = xt.shape[1]
    blocks = txt.shape[0]
    once = dict(pipeline_mode=pl.Buffered(1))
    hbm = pl.BlockSpec(memory_space=pl.ANY)
    img_rows, txt_rows = 2 * feat, 2 * feat_t + 128
    outs = [(2, img_rows, 128), (2, 2 * feat_t, 128), (8, 128)]
    return pl.pallas_call(
        functools.partial(home_body, total_rows=total_rows),
        grid=(rows // BM,),
        in_specs=[
            pl.BlockSpec(memory_space=pltpu.SMEM),
            pl.BlockSpec(memory_space=pltpu.SMEM),
            pl.BlockSpec((BM, dim), lambda i: (i, 0)),
            whole((blocks, BN, dim), **once),
            pl.BlockSpec((BM, dim), lambda i: (i, 0)),
            pl.BlockSpec((BM, feat), lambda i: (i, 0)),
            pl.BlockSpec((BM, dim), lambda i: (i, 0)),
            hbm, hbm, hbm,
        ],
        out_specs=[whole(shape, **once) for shape in outs],
        out_shape=[jax.ShapeDtypeStruct(shape, F32) for shape in outs],
        scratch_shapes=tile_scratch(dim) + [
            pltpu.VMEM((BM, dim), F32),
            pltpu.VMEM((blocks, dim, BN), F32),
            pltpu.VMEM((feat, dim), F32),
            pltpu.VMEM((3, CR, CC), F32),
            pltpu.VMEM((3 * CR, CC), F32),
            pltpu.VMEM((blocks, dim, BN), F32),
            pltpu.VMEM((rows // BM, BM, feat_t), BF16),
            pltpu.VMEM((feat_t, dim), BF16),
            pltpu.VMEM((2, dim, BM), F32),
            pltpu.VMEM((dim, feat_t), F32),
            pltpu.VMEM((2, img_rows, 128), F32),
            pltpu.VMEM((2, txt_rows, 128), F32),
            pltpu.VMEM((2, img_rows, 128), F32),
            pltpu.VMEM((2, txt_rows, 128), F32),
            pltpu.SemaphoreType.DMA((rows // BM + 2,)),
            pltpu.SemaphoreType.DMA((2,)),
        ] + sum_scratch(img_rows) + sum_scratch(txt_rows),
        compiler_params=params(48, collective_id=1, has_side_effects=True),
        cost_estimate=cost(6 * rows * rows * dim, 40 * rows * dim),
        name="home_tile",
    )(temp, bias, img, txt, raw, x, away, away_dt, xt, wt)


def solution(mesh):
    data_n, rep_n = mesh.shape["data"], mesh.shape["rep"]
    row_spec = P(("rep", "data"), None)

    def device_body(img_loc, txt_loc, w_img, w_txt, log_temp, logit_bias):
        rows = img_loc.shape[0]
        dim = w_img.shape[1]
        total_rows = float(rows * rep_n * data_n)
        temp, bias = log_temp.reshape(1), logit_bias.reshape(1)
        emb_t, away_t, emb_i, raw_i = heads(txt_loc, w_txt, img_loc, w_img)
        emb_t = emb_t.reshape(rows // BN, BN, dim)
        away_t = away_t.reshape(rows // BN, BN, dim)
        away_di, away_dt = away_tile(temp, bias, emb_i, away_t, total_rows)
        img_sum, txt_sum, totals = home_tile(temp, bias, emb_i, emb_t, raw_i, img_loc, away_di, away_dt, txt_loc, w_txt, total_rows)
        dw_img = img_sum.reshape(4, -1, 128).transpose(1, 0, 2).reshape(-1, dim)
        dw_txt = txt_sum.reshape(4, -1, 128).transpose(1, 0, 2).reshape(-1, dim)
        return totals[0, 0], totals[1, 0], totals[2, 0], dw_img, dw_txt

    return jax.shard_map(device_body, mesh=mesh, in_specs=(row_spec, row_spec, P(), P(), P(), P()), out_specs=(P(), P(), P(), P(), P()), check_vma=False)
```
